32 devices in a mesh: seq: 8 (over y, x, core), head: 4 (over z).
Axes of the slice: x: 2, y: 2, z: 4, core: 2. Of those that a mesh axis runs over, the one named last changes fastest.
Arguments:
- video_rows: bfloat16 [4096, 5120], P('seq'), may hold values from -6 to 6
- context: bfloat16 [512, 5120], P('seq'), may hold values from -6 to 6
- valid_length: int32 [1], replicated, may hold values from 64 to 512
- timestep: int32 [1], replicated, may hold values from 0 to 999
- query_weight: bfloat16 [5120, 1024], P('seq', 'head'), may hold values from -0.078125 to 0.078125
- key_weight: bfloat16 [5120, 1024], P('seq', 'head'), may hold values from -0.078125 to 0.078125
- value_weight: bfloat16 [5120, 1024], P('seq', 'head'), may hold values from -0.078125 to 0.078125
- out_weight: bfloat16 [1024, 5120], P('head', 'seq'), may hold values from -0.1875 to 0.1875
- query_gain: float32 [1024], P('head'), may hold values from 0.5 to 15
- key_gain: float32 [1024], P('head'), may hold values from 0.5 to 15
- time_weight: bfloat16 [2, 256, 5120], P(None, None, 'head'), may hold values from -0.375 to 0.375
- modulation: float32 [2, 5120], P(None, 'head'), may hold values from -3 to 3
Outputs:
- residual_out: bfloat16 [4096, 5120], P('seq', 'head')
- modulated: bfloat16 [4096, 5120], P('seq', 'head')
The draws below stay inside these ranges and needn't reach their ends.
Inputs may be any that keep to these rules, and one draw needn't show every extreme that they name: `valid_length`: text positions at or beyond it are padding.
All inputs are finite; a program needn't handle non-finite values.
Results may differ from the reference program's by a relative error of at most 0.0065.
The reference program's roundings to bfloat16 on the way (of `normed`, `value_proj`, `query_normed`, `key_normed`, `weights`, `attended` and `act`) count: a program that leaves them out, or rounds other values in their place, can miss the bound.
Values may be sent and summed in bfloat16 or wider, within the bound.
A program may use at most 64 MiB of HBM per device.

```python
import jax
import jax.numpy as jnp
from jax import lax

D = 5120
HD = 128
TEXT = 512
FREQ = 256
HEADS = 8
ATT = 1024
TOKENS = 4096


def head_gains(key):
    base = jax.random.uniform(key, (HEADS, HD), jnp.float32, 0.5, 1.5)
    return base.reshape(HEADS * HD)


def draw_query_gain(key, part):
    return head_gains(jax.random.fold_in(key, 11))


def draw_key_gain(key, part):
    return head_gains(jax.random.fold_in(key, 23))


def shard_levels(rng, shape, cuts, least, top_value):
    def one(axis_at, parts):
        steps = jax.random.uniform(jax.random.fold_in(jax.random.fold_in(rng, 6), axis_at), (parts,), jnp.float32, least / len(cuts), top_value / len(cuts))
        return jnp.repeat(jnp.exp(steps), shape[axis_at] // parts).reshape((-1,) + (1,) * (len(shape) - axis_at - 1))

    loudness = one(*cuts[0])
    for cut in cuts[1:]:
        loudness = loudness * one(*cut)
    return loudness


def centred(own_key, shape, deviation, limit, pieces=(), held_as=jnp.bfloat16):
    loudness = shard_levels(own_key, shape, pieces, -0.22, 0.18) if pieces else 1.0
    entries = jax.random.normal(own_key, shape, jnp.float32) * deviation * loudness
    return jnp.minimum(jnp.maximum(entries, -limit), limit).astype(held_as)


def setup_inputs(seed: int = 0) -> dict:
    arg_keys = jax.random.split(jax.random.key(seed), 13)
    video_rows = centred(arg_keys[0], (TOKENS, D), 1.0, 6.0, ((0, 8),))
    context = centred(arg_keys[1], (TEXT, D), 1.0, 6.0, ((0, 8),))
    valid_length = jax.random.randint(arg_keys[2], (1,), TEXT // 8, TEXT + 1).astype(jnp.int32)
    timestep = jax.random.randint(arg_keys[3], (1,), 0, 1000).astype(jnp.int32)
    query_weight = centred(arg_keys[4], (D, ATT), D ** -0.5, 0.078125, ((0, 8), (1, 4)))
    key_weight = centred(arg_keys[5], (D, ATT), D ** -0.5, 0.078125, ((0, 8), (1, 4)))
    value_weight = centred(arg_keys[6], (D, ATT), D ** -0.5, 0.078125, ((0, 8), (1, 4)))
    out_weight = centred(arg_keys[7], (ATT, D), ATT ** -0.5, 0.1875, ((0, 4), (1, 8)))
    query_gain = draw_query_gain(jax.random.fold_in(arg_keys[12], 71), 0)
    key_gain = draw_key_gain(jax.random.fold_in(arg_keys[12], 71), 0)
    time_weight = centred(arg_keys[10], (2, FREQ, D), FREQ ** -0.5, 0.375, ((2, 4),))
    modulation = centred(arg_keys[11], (2, D), 0.5, 3.0, ((1, 4),), jnp.float32)
    return {"video_rows": video_rows, "context": context, "valid_length": valid_length, "timestep": timestep, "query_weight": query_weight, "key_weight": key_weight, "value_weight": value_weight, "out_weight": out_weight, "query_gain": query_gain, "key_gain": key_gain, "time_weight": time_weight, "modulation": modulation}


def layer_norm(rows):
    mean = lax.optimization_barrier(jnp.mean(rows, axis=-1, keepdims=True))
    spread = lax.optimization_barrier(jnp.mean((rows - mean) ** 2, axis=-1, keepdims=True))
    return (rows - mean) / jnp.sqrt(spread + 1e-06)

def rms_gain(rows, gain):
    return rows / jnp.sqrt(lax.optimization_barrier(jnp.mean(rows * rows, axis=-1, keepdims=True)) + 1e-06) * gain

def reference(video_rows, context, valid_length, timestep, query_weight, key_weight, value_weight, out_weight, query_gain, key_gain, time_weight, modulation):
    normed = layer_norm(video_rows.astype(jnp.float32)).astype(jnp.bfloat16)
    queries = jnp.dot(normed, query_weight, preferred_element_type=jnp.float32)
    key_proj = jnp.dot(context, key_weight, preferred_element_type=jnp.float32)
    value_proj = jnp.dot(context, value_weight, preferred_element_type=jnp.float32).astype(jnp.bfloat16)
    query_normed = rms_gain(queries, query_gain).astype(jnp.bfloat16)
    key_normed = rms_gain(key_proj, key_gain).astype(jnp.bfloat16)
    key_valid = jnp.arange(TEXT, dtype=jnp.int32) < valid_length[0]

    def one_head(head_index):
        offset = (head_index * HD).astype(jnp.int32)
        query_part = lax.dynamic_slice_in_dim(query_normed, offset, HD, 1)
        key_part = lax.dynamic_slice_in_dim(key_normed, offset, HD, 1)
        value_part = lax.dynamic_slice_in_dim(value_proj, offset, HD, 1)
        scores = jnp.dot(query_part, key_part.T, preferred_element_type=jnp.float32) * HD ** (-0.5)
        scores = jnp.where(key_valid[None, :], scores, jnp.float32(-1e+30))
        shifted = jnp.exp(scores - lax.optimization_barrier(jnp.max(scores, axis=-1, keepdims=True)))
        weights = (shifted / lax.optimization_barrier(jnp.sum(shifted, axis=-1, keepdims=True))).astype(jnp.bfloat16)
        return jnp.dot(weights, value_part, preferred_element_type=jnp.float32).astype(jnp.bfloat16)
    per_head = lax.map(one_head, jnp.arange(HEADS, dtype=jnp.int32))
    attended = jnp.transpose(per_head, (1, 0, 2)).reshape(TOKENS, ATT)
    projected = jnp.dot(attended, out_weight, preferred_element_type=jnp.float32)
    residual_out = (video_rows.astype(jnp.float32) + projected).astype(jnp.bfloat16)
    half = FREQ // 2
    freqs = jnp.exp(-jnp.log(10000.0) * jnp.arange(half, dtype=jnp.float32) / half)
    angles = timestep[0].astype(jnp.float32) * freqs
    embedding = jnp.concatenate([jnp.cos(angles), jnp.sin(angles)])
    act = jax.nn.silu(embedding).astype(jnp.bfloat16)[None, :]
    shift = modulation[0] + jnp.dot(act, time_weight[0], preferred_element_type=jnp.float32)[0]
    scale = modulation[1] + jnp.dot(act, time_weight[1], preferred_element_type=jnp.float32)[0]
    resid = residual_out.astype(jnp.float32)
    mean2 = lax.optimization_barrier(jnp.mean(resid, axis=-1, keepdims=True))
    var2 = lax.optimization_barrier(jnp.mean(resid * resid, axis=-1, keepdims=True)) - mean2 * mean2
    modulated = ((resid - mean2) / jnp.sqrt(var2 + 1e-06) * (1.0 + scale) + shift).astype(jnp.bfloat16)
    return (residual_out, modulated)
```

```python
import functools

import jax
import jax.numpy as jnp
from jax import lax
from jax.experimental import pallas as pl
from jax.experimental.pallas import tpu as pltpu
from jax.sharding import PartitionSpec as P

HD = 128
FREQ = 256
LANES = 128
F32 = jnp.float32
BF16 = jnp.bfloat16
MESH_ID = pl.DeviceIdType.MESH


def flip(index, mask):
    bit = 1
    while bit <= mask:
        if mask & bit:
            index = index + bit - 2 * bit * ((index // bit) % 2)
        bit *= 2
    return index


def bits_of(mask):
    return [1 << b for b in range(mask.bit_length()) if mask >> b & 1]


def last_bit(half, mask):
    return bits_of(mask)[-1] if half == 0 else bits_of(mask)[0]


def by_hops(n_seq):
    return sorted(range(2, n_seq, 2), key=lambda k: (len(bits_of(k)), k))


def column_to_row(column):
    tall = column.shape[0]
    wide = -(-tall // LANES) * LANES
    if wide > tall:
        column = jnp.concatenate([column, jnp.zeros((wide - tall, 1), F32)], axis=0)
    return jnp.transpose(jnp.broadcast_to(column, (wide, LANES)))[:1]


def row_to_column(row, tall):
    return jnp.transpose(jnp.broadcast_to(row, (LANES, row.shape[1])))[:tall, :1]


def body(n_seq, n_head, chunks, sliced, *refs):
    if sliced:
        steps(n_seq, n_head, chunks, *refs)
    else:
        steps(n_seq, n_head, chunks, *refs[:12], None, *refs[12:])


def steps(
    n_seq, n_head, chunks,
    valid, video, ctx, qw, kw, vw, ow, qg, kg, act, tw_hbm, mod, vpart,
    resid_out, mod_out,
    vid, normed, ctxv, ctxg, qwg, kvw, cks, ckr, cvs, cvr, kall, vall, spread, owg, attg,
    queries, qsq, ksq, stat, shsc, tw,
    loc_sem, ctx_s, ctx_r, qw_s, qw_r, w_s, w_r, ck_s, ck_r, cv_s, cv_r, k_s, k_r, v_s, v_r,
    sp_s, sp_r, oz_s, oz_r, og_s, og_r, ksq_s, ksq_r, qsq_s, qsq_r, at_s, at_r, st_s, st_r,
):
    s = lax.axis_index("seq")
    z = lax.axis_index("head")
    core = s % 2
    chip = s // 2
    n_chip = n_seq // 2
    ratio = n_seq // n_head
    tok, width = vid.shape
    depth = qw.shape[0]
    att = qw.shape[1]
    text = ctx.shape[0]
    pair = 2 * depth
    sent = []
    masks = by_hops(n_seq)
    chip_bits = [k for k in masks if len(bits_of(k)) == 1]

    def to_seq(k):
        return (flip(s, k), z)

    def to_head(k):
        return (s, flip(z, k))

    def remote(src, dst, ssem, rsem, dev):
        return pltpu.make_async_remote_copy(
            src_ref=src, dst_ref=dst, send_sem=ssem, recv_sem=rsem,
            device_id=dev, device_id_type=MESH_ID,
        )

    def push(src, dst, ssem, rsem, dev):
        copy = remote(src, dst, ssem, rsem, dev)
        copy.start()
        sent.append((None, copy))

    def arrived(dst, ssem, rsem, dev):
        remote(dst, dst, ssem, rsem, dev).wait_recv()

    def gather_own(slot, half, bits, ssem, rsem):
        for b in bits:
            push(slot(half, s), slot(half, s), ssem.at[half, b], rsem.at[half, b], to_seq(b))

    def gather_core(slot, half, ssem, rsem):
        push(slot(half, s), slot(half, s), ssem.at[half, 1], rsem.at[half, 1], to_seq(1))

    def gather_relay(slot, half, k, ssem, rsem):
        here = slot(half, flip(s, k))
        arrived(here, ssem.at[half, k], rsem.at[half, k], to_seq(last_bit(half, k)))
        for b in chip_bits:
            if not k & b and last_bit(half, k | b) == b:
                push(here, here, ssem.at[half, k | b], rsem.at[half, k | b], to_seq(b))
        push(here, here, ssem.at[half, k + 1], rsem.at[half, k + 1], to_seq(1))

    def gather_end(slot, half, k, ssem, rsem):
        here = slot(half, flip(s, k + 1))
        arrived(here, ssem.at[half, k + 1], rsem.at[half, k + 1], to_seq(1))

    barrier = pltpu.get_barrier_semaphore()
    for k in range(1, n_seq):
        pl.semaphore_signal(barrier, inc=1, device_id=to_seq(k), device_id_type=MESH_ID)
    for k in range(1, n_head):
        pl.semaphore_signal(barrier, inc=1, device_id=to_head(k), device_id_type=MESH_ID)

    def half_rows(half, p):
        rows = depth // 2
        return qwg.at[pl.ds(pl.multiple_of(p * depth + half * rows, rows), rows), :]

    def load(src, dst, i):
        copy = pltpu.make_async_copy(src, dst, loc_sem.at[i])
        copy.start()
        return copy

    piece = ow.shape[0] // n_seq

    def ow_piece(p):
        return pl.ds(pl.multiple_of(p * piece, piece), piece)

    own_ctx = load(ctx, ctxv, 0)
    own_qw = load(qw, qwg.at[pl.ds(pl.multiple_of(s * depth, depth), depth), :], 1)
    own_kw = load(kw, kvw.at[core, :, :att], 2)
    own_vw = load(vw, kvw.at[core, :, att:], 3)
    own_vid = load(video, vid, 4)
    own_spread = load(ow.at[ow_piece(s), :], spread.at[s], 5)
    own_tw = load(tw_hbm, tw, 6)
    pl.semaphore_wait(barrier, n_seq + n_head - 2)

    def ctx_cols(p):
        return pl.ds(pl.multiple_of(p * pair, pair), pair)

    own_ctx.wait()
    for k in masks:
        push(
            ctxv.at[:, ctx_cols(flip(chip, k // 2))], ctxg.at[k // 2],
            ctx_s.at[k // 2], ctx_r.at[k // 2], to_seq(k),
        )
    own_kw.wait()
    own_vw.wait()
    push(kvw.at[core], kvw.at[core], w_s, w_r, to_seq(1))
    for k in list(masks) + [k + 1 for k in masks] + [1]:
        push(ow.at[ow_piece(flip(s, k)), :], spread.at[s], sp_s.at[k], sp_r.at[k], to_seq(k))
    own_qw.wait()
    half_slot = half_rows
    gather_own(half_slot, 0, chip_bits[:1], qw_s, qw_r)
    gather_own(half_slot, 1, chip_bits[1:], qw_s, qw_r)
    gather_core(half_slot, 0, qw_s, qw_r)
    gather_core(half_slot, 1, qw_s, qw_r)

    own_vid.wait()
    strip = 16

    with jax.named_scope("norm"):
        @pl.loop(0, tok // strip)
        def _(i):
            at = pl.ds(pl.multiple_of(i * strip, strip), strip)
            rows = vid[at, :].astype(F32)
            mean = jnp.mean(rows, axis=-1, keepdims=True)
            centred = rows - mean
            spread_ = jnp.mean(centred * centred, axis=-1, keepdims=True)
            normed[at, :] = (centred * (1.0 / jnp.sqrt(spread_ + 1e-06))).astype(BF16)

    with jax.named_scope("kv"):
        arrived(kvw.at[1 - core], w_s, w_r, to_seq(1))

        def partial_kv(source):
            return jnp.dot(source, kvw[...].reshape(pair, 2 * att), preferred_element_type=F32)

        mine = partial_kv(ctxv[:, ctx_cols(chip)])
        for k in masks:
            c = k // 2
            arrived(ctxg.at[c], ctx_s.at[c], ctx_r.at[c], to_seq(k))
            block = partial_kv(ctxg[c])
            cks[c] = block[:, :att]
            cvs[c] = block[:, att:].astype(BF16)
            push(cks.at[c], ckr.at[c], ck_s.at[c], ck_r.at[c], to_seq(k))
            push(cvs.at[c], cvr.at[c], cv_s.at[c], cv_r.at[c], to_seq(k))
        cks[0] = mine[:, :att]
        ckr[0] = mine[:, att:]
    gather_own(half_slot, 0, chip_bits[1:], qw_s, qw_r)
    gather_own(half_slot, 1, chip_bits[:1], qw_s, qw_r)

    def chip_queries(p):
        lanes = pl.ds(pl.multiple_of(p * pair, pair), pair)
        return jnp.dot(normed[:, lanes], qwg[lanes, :], preferred_element_type=F32)

    with jax.named_scope("shsc"):
        own_tw.wait()
        for i in range(2):
            shsc[i] = mod[i : i + 1, :] + jnp.dot(act[...], tw[i], preferred_element_type=F32)[:8]

    with jax.named_scope("relay1"):
        first = [(0, b) for b in chip_bits[:1]] + [(1, b) for b in chip_bits[1:]]
        for half, b in first:
            gather_relay(half_slot, half, b, qw_s, qw_r)
        for half in range(2):
            gather_end(half_slot, half, 0, qw_s, qw_r)
    with jax.named_scope("q_own"):
        queries[...] = chip_queries(chip)

    def own_cols(zz):
        return pl.ds(zz * ratio, ratio)

    def ow_slot_z(p):
        return owg.at[:, p, ow_piece(s), :]

    with jax.named_scope("spread"):
        own_spread.wait()
        for k in list(masks) + [k + 1 for k in masks] + [1]:
            arrived(spread.at[flip(s, k)], sp_s.at[k], sp_r.at[k], to_seq(k))
        own_ow = load(spread.at[own_cols(z)], ow_slot_z(z), 7)
        for k in range(1, n_head):
            push(
                spread.at[own_cols(flip(z, k))], ow_slot_z(z), oz_s.at[k], oz_r.at[k], to_head(k)
            )

    with jax.named_scope("kv_sum"):
        key_rows = cks[0]
        value_rows = ckr[0]
        for k in masks:
            c = k // 2
            arrived(ckr.at[c], ck_s.at[c], ck_r.at[c], to_seq(k))
            arrived(cvr.at[c], cv_s.at[c], cv_r.at[c], to_seq(k))
            key_rows = key_rows + ckr[c]
            value_rows = value_rows + cvr[c].astype(F32)
        cks[0] = key_rows
        ksq[0] = column_to_row(jnp.sum(key_rows * key_rows, axis=1, keepdims=True))
        for k in range(1, n_head):
            push(ksq.at[0], ksq.at[k], ksq_s.at[k], ksq_r.at[k], to_head(k))
        vall[s] = value_rows.astype(BF16)
        for k in masks + [1]:
            push(vall.at[s], vall.at[s], v_s.at[k], v_r.at[k], to_seq(k))

    with jax.named_scope("relay2"):
        second = [(0, b) for b in chip_bits[1:]] + [(1, b) for b in chip_bits[:1]]
        for half, b in second:
            gather_relay(half_slot, half, b, qw_s, qw_r)

    with jax.named_scope("k_norm"):
        for k in range(1, n_head):
            arrived(ksq.at[k], ksq_s.at[k], ksq_r.at[k], to_head(k))
        k_mean = row_to_column(jnp.sum(ksq[...], axis=0), text) / (att * n_head)
        kall[s] = (cks[0] / jnp.sqrt(k_mean + 1e-06) * kg[...]).astype(BF16)
        for k in masks + [1]:
            push(kall.at[s], kall.at[s], k_s.at[k], k_r.at[k], to_seq(k))

    with jax.named_scope("q_mid"):
        for b in chip_bits:
            for half in range(2):
                gather_end(half_slot, half, b, qw_s, qw_r)
            queries[...] += chip_queries(flip(chip, b // 2))
    with jax.named_scope("q_far"):
        for k in masks:
            if k not in chip_bits:
                for half in range(2):
                    gather_relay(half_slot, half, k, qw_s, qw_r)
        for k in masks:
            if k not in chip_bits:
                for half in range(2):
                    gather_end(half_slot, half, k, qw_s, qw_r)
                queries[...] += chip_queries(flip(chip, k // 2))
        q = queries[...]
        qsq[0] = column_to_row(jnp.sum(q * q, axis=1, keepdims=True))
        for k in range(1, n_head):
            push(qsq.at[0], qsq.at[k], qsq_s.at[k], qsq_r.at[k], to_head(k))

    def ow_half(half, p):
        rows = piece // 2 if ratio == 1 else piece
        if ratio == 1:
            return owg.at[:, :, pl.ds(pl.multiple_of(p * piece + half * rows, rows), rows), :]
        cut = ratio // 2
        return owg.at[pl.ds(half * cut, cut), :, ow_piece(p), :]

    with jax.named_scope("ow_start"):
        own_ow.wait()
        for k in range(1, n_head):
            arrived(ow_slot_z(flip(z, k)), oz_s.at[k], oz_r.at[k], to_head(k))
        gather_own(ow_half, 0, chip_bits[:1], og_s, og_r)
        gather_own(ow_half, 1, chip_bits[1:], og_s, og_r)
        gather_own(ow_half, 0, chip_bits[1:], og_s, og_r)
        gather_own(ow_half, 1, chip_bits[:1], og_s, og_r)
        for half in range(2):
            gather_core(ow_half, half, og_s, og_r)

    with jax.named_scope("kv_in"):
        for ref, ssem, rsem in ((vall, v_s, v_r), (kall, k_s, k_r)):
            for k in masks:
                here = ref.at[flip(s, k)]
                arrived(here, ssem.at[k], rsem.at[k], to_seq(k))
                push(here, here, ssem.at[k + 1], rsem.at[k + 1], to_seq(1))
        for ref, ssem, rsem in ((vall, v_s, v_r), (kall, k_s, k_r)):
            for k in [0] + masks:
                arrived(ref.at[flip(s, k + 1)], ssem.at[k + 1], rsem.at[k + 1], to_seq(1))

    with jax.named_scope("q_norm"):
        for k in range(1, n_head):
            arrived(qsq.at[k], qsq_s.at[k], qsq_r.at[k], to_head(k))
        q_mean = row_to_column(jnp.sum(qsq[...], axis=0), tok) / (att * n_head)
        q_normed = (queries[...] / jnp.sqrt(q_mean + 1e-06) * qg[...]).astype(BF16)

    step = tok // chunks

    def next_head(way):
        return (s, z + way)

    def held(way, d):
        return attg.at[d % n_head if way > 0 else (n_head - d) % n_head]

    def reach(way, origin_ok, c, d):
        at = slice(c * step, (c + 1) * step)
        side = 0 if way > 0 else 1
        ok = origin_ok & ((z + way >= 0) & (z + way < n_head))
        copy = remote(
            held(way, d - 1).at[at], held(way, d).at[at],
            at_s.at[side, c, d], at_r.at[side, c, d], next_head(way),
        )

        @pl.when(ok)
        def _():
            copy.start()

        sent.append((ok, copy))

    def take(way, c, d):
        at = slice(c * step, (c + 1) * step)
        side = 0 if way > 0 else 1
        origin = z - way * d
        ok = (origin >= 0) & (origin < n_head)

        @pl.when(ok)
        def _():
            arrived(held(way, d).at[at], at_s.at[side, c, d], at_r.at[side, c, d], next_head(-way))

        return ok

    all_text = n_seq * text
    with jax.named_scope("attend"):
        every_k = kall[...].reshape(all_text, att)
        every_v = vall[...].reshape(all_text, att)
        seen = lax.broadcasted_iota(jnp.int32, (1, all_text), 1) < valid[0]
        for c in range(chunks):
            at = slice(c * step, (c + 1) * step)
            for h in range(att // HD):
                lanes = slice(h * HD, (h + 1) * HD)
                scores = lax.dot_general(
                    q_normed[at, lanes], every_k[:, lanes], (((1,), (1,)), ((), ())),
                    preferred_element_type=F32,
                ) * HD ** (-0.5)
                scores = jnp.where(seen, scores, F32(-1e30))
                shifted = jnp.exp(scores - jnp.max(scores, axis=-1, keepdims=True))
                weights = (shifted * (1.0 / jnp.sum(shifted, axis=-1, keepdims=True))).astype(BF16)
                attg[0, at, lanes] = jnp.dot(
                    weights, every_v[:, lanes], preferred_element_type=F32
                ).astype(BF16)
            for way in (1, -1):
                reach(way, z >= 0, c, 1)

    def ow_relays(pairs):
        for half, b in pairs:
            gather_relay(ow_half, half, b, og_s, og_r)

    for d in range(1, n_head - 1):
        for c in range(chunks):
            with jax.named_scope(f"pass{d}_{c}"):
                for way in (1, -1):
                    ok = take(way, c, d)
                    reach(way, ok, c, d + 1)
            if d == 1 and c == 0:
                with jax.named_scope("ow1"):
                    ow_relays(first)
            if d == 1 and c == chunks - 1:
                with jax.named_scope("ow2"):
                    ow_relays(second)
    with jax.named_scope("ow3"):
        for k in masks:
            if k not in chip_bits:
                for half in range(2):
                    gather_relay(ow_half, half, k, og_s, og_r)
        for k in [0] + masks:
            for half in range(2):
                gather_end(ow_half, half, k, og_s, og_r)

    cols = owg.shape[3]
    part_width = mod_out.shape[1]
    for c in range(chunks):
        at = slice(c * step, (c + 1) * step)
        with jax.named_scope(f"last{c}"):
            for way in (1, -1):
                take(way, c, n_head - 1)
        with jax.named_scope(f"project{c}"):
            row_sum = jnp.zeros((step, 1), F32)
            row_sq = jnp.zeros((step, 1), F32)
            for j in range(ratio):
                here = slice(j * cols, (j + 1) * cols)
                projected = jnp.dot(attg[0, at], owg[j, z], preferred_element_type=F32)
                for k in range(1, n_head):
                    projected = projected + jnp.dot(
                        attg[k, at], owg[j, lax.rem(z + n_head - k, n_head)], preferred_element_type=F32
                    )
                if vpart is None:
                    base = vid[at, pl.ds(pl.multiple_of(z * part_width + j * cols, LANES), cols)]
                else:
                    base = vpart[at, here]
                rounded = (base.astype(F32) + projected).astype(BF16)
                resid_out[at, here] = rounded
                wide = rounded.astype(F32)
                row_sum = row_sum + jnp.sum(wide, axis=1, keepdims=True)
                row_sq = row_sq + jnp.sum(wide * wide, axis=1, keepdims=True)
            stat[c, 0, :1] = column_to_row(row_sum)[:, :step]
            stat[c, 0, 1:] = column_to_row(row_sq)[:, :step]
            for k in range(1, n_head):
                push(stat.at[c, 0], stat.at[c, k], st_s.at[c, k], st_r.at[c, k], to_head(k))
    for c in range(chunks):
        at = slice(c * step, (c + 1) * step)
        with jax.named_scope(f"stat{c}"):
            for k in range(1, n_head):
                arrived(stat.at[c, k], st_s.at[c, k], st_r.at[c, k], to_head(k))
        with jax.named_scope(f"modulate{c}"):
            both = jnp.sum(stat[c], axis=0) / (part_width * n_head)
            mean2 = both[:1]
            inverse = 1.0 / jnp.sqrt(both[1:] - mean2 * mean2 + 1e-06)
            mean_col = row_to_column(mean2, step)
            inv_col = row_to_column(inverse, step)
            wide = resid_out[at, :].astype(F32)
            mod_out[at, :] = (
                (wide - mean_col) * inv_col * (1.0 + shsc[1, :1, :]) + shsc[0, :1, :]
            ).astype(BF16)
    for ok, copy in sent:
        if ok is None:
            copy.wait_send()
        else:
            pl.when(ok)(copy.wait_send)


def on_device(
    n_seq,
    n_head,
    video_rows,
    context,
    valid_length,
    timestep,
    query_weight,
    key_weight,
    value_weight,
    out_weight,
    query_gain,
    key_gain,
    time_weight,
    modulation,
):
    tok, width = video_rows.shape
    text = context.shape[0]
    depth, att = query_weight.shape
    cols = out_weight.shape[1]
    part_width = modulation.shape[1]
    ratio = n_seq // n_head
    n_chip = n_seq // 2
    chunks = 4
    piece = out_weight.shape[0] // n_seq
    half = FREQ // 2
    freqs = jnp.exp(-jnp.log(10000.0) * jnp.arange(half, dtype=F32) / half)
    angles = timestep[0].astype(F32) * freqs
    embedding = jnp.concatenate([jnp.cos(angles), jnp.sin(angles)])
    act = jnp.broadcast_to(jax.nn.silu(embedding).astype(BF16)[None, :], (16, FREQ))
    sliced = part_width % LANES != 0 or cols % LANES != 0
    extra = []
    if sliced:
        extra.append(
            lax.dynamic_slice_in_dim(
                video_rows, lax.axis_index("head") * part_width, part_width, 1
            )
        )
    vmem = pl.BlockSpec(memory_space=pltpu.VMEM)
    hbm = pl.BlockSpec(memory_space=pl.ANY)
    dma = pltpu.SemaphoreType.DMA
    return pl.pallas_call(
        functools.partial(body, n_seq, n_head, chunks, sliced),
        out_shape=[jax.ShapeDtypeStruct((tok, part_width), BF16)] * 2,
        in_specs=[pl.BlockSpec(memory_space=pltpu.SMEM)]
        + [hbm] * 6
        + [vmem] * 3
        + [hbm, vmem]
        + [vmem] * len(extra),
        out_specs=[vmem] * 2,
        scratch_shapes=[
            pltpu.VMEM((tok, width), BF16),
            pltpu.VMEM((tok, width), BF16),
            pltpu.VMEM((text, width), BF16),
            pltpu.VMEM((n_chip, text, 2 * depth), BF16),
            pltpu.VMEM((n_seq * depth, att), BF16),
            pltpu.VMEM((2, depth, 2 * att), BF16),
            pltpu.VMEM((n_chip, text, att), F32),
            pltpu.VMEM((n_chip, text, att), F32),
            pltpu.VMEM((n_chip, text, att), BF16),
            pltpu.VMEM((n_chip, text, att), BF16),
            pltpu.VMEM((n_seq, text, att), BF16),
            pltpu.VMEM((n_seq, text, att), BF16),
            pltpu.VMEM((n_seq, piece, cols), BF16),
            pltpu.VMEM((ratio, n_head, out_weight.shape[0], cols), BF16),
            pltpu.VMEM((n_head, tok, att), BF16),
            pltpu.VMEM((tok, att), F32),
            pltpu.VMEM((n_head, 1, tok), F32),
            pltpu.VMEM((n_head, 1, -(-text // LANES) * LANES), F32),
            pltpu.VMEM((chunks, n_head, 2, tok // chunks), F32),
            pltpu.VMEM((2, 8, part_width), F32),
            pltpu.VMEM(time_weight.shape, BF16),
            dma((8,)),
            *[dma((n_chip,))] * 2,
            *[dma((2, n_seq))] * 2,
            *[dma] * 2,
            *[dma((n_chip,))] * 2,
            *[dma((n_chip,))] * 2,
            *[dma((n_seq,))] * 2,
            *[dma((n_seq,))] * 2,
            *[dma((n_seq,))] * 2,
            *[dma((n_head,))] * 2,
            *[dma((2, n_seq))] * 2,
            *[dma((n_head,))] * 2,
            *[dma((n_head,))] * 2,
            *[dma((2, chunks, n_head))] * 2,
            *[dma((chunks, n_head))] * 2,
        ],
        compiler_params=pltpu.CompilerParams(
            collective_id=0, has_side_effects=True, vmem_limit_bytes=60 * 1024 * 1024
        ),
    )(
        valid_length,
        video_rows,
        context,
        query_weight,
        key_weight,
        value_weight,
        out_weight,
        query_gain[None, :],
        key_gain[None, :],
        act,
        time_weight,
        modulation,
        *extra,
    )


def solution(mesh):
    in_specs = (
        P("seq", None),
        P("seq", None),
        P(),
        P(),
        P("seq", "head"),
        P("seq", "head"),
        P("seq", "head"),
        P("head", "seq"),
        P("head"),
        P("head"),
        P(None, None, "head"),
        P(None, "head"),
    )
    out_specs = (P("seq", "head"), P("seq", "head"))
    return jax.shard_map(
        functools.partial(on_device, mesh.shape["seq"], mesh.shape["head"]),
        mesh=mesh, in_specs=in_specs, out_specs=out_specs, check_vma=False,
    )
```

```python
import functools

import jax
import jax.numpy as jnp
import numpy as np
from jax import lax
from jax.experimental import pallas as pl
from jax.experimental.pallas import tpu as pltpu
from jax.sharding import PartitionSpec as P

HD = 128
FREQ = 256
LANES = 128
VMEM_MOST = 67_000_000
NORM_FIRST = 9
F32 = jnp.float32
BF16 = jnp.bfloat16
MESH_ID = pl.DeviceIdType.MESH


def flip(index, mask):
    bit = 1
    while bit <= mask:
        if mask & bit:
            index = index + bit - 2 * bit * ((index // bit) % 2)
        bit *= 2
    return index


def bits_of(mask):
    return [1 << b for b in range(mask.bit_length()) if mask >> b & 1]


def last_bit(half, mask):
    return bits_of(mask)[-1] if half == 0 else bits_of(mask)[0]


def by_hops(n_seq):
    return sorted(range(2, n_seq, 2), key=lambda k: (len(bits_of(k)), k))


def column_to_row(column):
    tall = column.shape[0]
    wide = -(-tall // LANES) * LANES
    if wide > tall:
        column = jnp.concatenate([column, jnp.zeros((wide - tall, 1), F32)], axis=0)
    return jnp.transpose(jnp.broadcast_to(column, (wide, LANES)))[:1]


def row_to_column(row, tall):
    return jnp.transpose(jnp.broadcast_to(row, (LANES, row.shape[1])))[:tall, :1]


def body(n_seq, n_head, cuts, sliced, *refs):
    if sliced:
        steps(n_seq, n_head, cuts, *refs)
    else:
        steps(n_seq, n_head, cuts, *refs[:13], None, *refs[13:])


def steps(
    n_seq, n_head, cuts,
    valid, when, video, ctx, qw, kw, vw, ow, qg_hbm, kg_hbm, freqs_hbm, tw_hbm, mod_hbm, vpart,
    resid_out, mod_out,
    vid, normed, ctxv, ctxg, qwg, kvw, cks, ckr, cvs, cvr, kall, vall, spread, owg, attg,
    queries, qsq, ksq, stat, shsc, tw, qg, kg, freqs, mod,
    loc_sem, send_sem, pass_s, ctx_r, ctz_r, qw_r, qc_r, og_r, oc_r, at_r, st_r, one_r,
):
    s = lax.axis_index("seq")
    z = lax.axis_index("head")
    core = s % 2
    chip = s // 2
    n_chip = n_seq // 2
    ratio = n_seq // n_head
    chunks = len(cuts)
    tok, width = vid.shape
    depth = qw.shape[0]
    att = qw.shape[1]
    text = ctx.shape[0]
    pair = 2 * depth
    masks = by_hops(n_seq)
    chip_bits = [k for k in masks if len(bits_of(k)) == 1]
    far = [k for k in masks if k not in chip_bits]
    (S_CTX, S_CTZ, S_W, S_SP, S_QW, S_CK, S_CV, S_KSQ, S_QSQ, S_V, S_K, S_OZ, S_OG, S_ST) = range(14)
    (R_W, R_SP, R_CK, R_CV, R_KSQ, R_QSQ, R_V, R_VC, R_K, R_KC, R_OZ) = range(11)

    def to_seq(k):
        return (flip(s, k), z)

    def to_head(k):
        return (s, flip(z, k))

    def remote(src, dst, ssem, rsem, dev):
        return pltpu.make_async_remote_copy(
            src_ref=src, dst_ref=dst, send_sem=ssem, recv_sem=rsem,
            device_id=dev, device_id_type=MESH_ID,
        )

    def push(src, dst, group, rsem, dev):
        remote(src, dst, send_sem.at[group], rsem, dev).start()

    def arrived(ref, sem):
        remote(ref, ref, sem, sem, to_seq(1)).wait_recv()

    def left(ref, sem):
        remote(ref, ref, sem, sem, to_seq(1)).wait_send()

    def gather_own(slot, half, bits, group, rsem):
        for b in bits:
            push(slot(half, s), slot(half, s), group, rsem.at[half, b // 2], to_seq(b))

    def gather_core(slot, group, csem):
        for half in range(2):
            push(slot(half, s), slot(half, s), group, csem.at[0], to_seq(1))

    def gather_relay(slot, half, k, group, rsem, csem):
        here = slot(half, flip(s, k))
        arrived(here, rsem.at[half, k // 2])
        for b in chip_bits:
            if not k & b and last_bit(half, k | b) == b:
                push(here, here, group, rsem.at[half, (k | b) // 2], to_seq(b))
        push(here, here, group, csem.at[k // 2], to_seq(1))

    barrier = pltpu.get_barrier_semaphore()
    for k in range(1, n_seq):
        pl.semaphore_signal(barrier, inc=1, device_id=to_seq(k), device_id_type=MESH_ID)
    for k in range(1, n_head):
        pl.semaphore_signal(barrier, inc=1, device_id=to_head(k), device_id_type=MESH_ID)

    def shard_rows(p, count=1):
        return qwg.at[pl.ds(pl.multiple_of(p * depth, depth), count * depth), :]

    def half_rows(half, p):
        rows = depth // 2
        return qwg.at[pl.ds(pl.multiple_of(p * depth + half * rows, rows), rows), :]

    def load(src, dst, i):
        copy = pltpu.make_async_copy(src, dst, loc_sem.at[i])
        copy.start()
        return copy

    piece = ow.shape[0] // n_seq

    def ow_piece(p):
        return pl.ds(pl.multiple_of(p * piece, piece), piece)

    own_ctx = load(ctx, ctxv, 0)
    own_qw = load(qw, shard_rows(s), 1)
    own_kw = load(kw, kvw.at[core, :, :att], 2)
    own_vw = load(vw, kvw.at[core, :, att:], 3)
    own_vid = load(video, vid, 4)
    own_spread = load(ow.at[ow_piece(s), :], spread.at[s], 5)
    own_tw = load(tw_hbm, tw, 6)
    small = [
        load(a, b, 8 + i)
        for i, (a, b) in enumerate(((qg_hbm, qg), (kg_hbm, kg), (freqs_hbm, freqs), (mod_hbm, mod)))
    ]
    with jax.named_scope("barrier"):
        pl.semaphore_wait(barrier, n_seq + n_head - 2)

    def ctx_cols(p):
        return pl.ds(pl.multiple_of(p * pair, pair), pair)

    part = text // 2

    def ctx_rows(q):
        return pl.ds(pl.multiple_of(q * part, part), part)

    mine = z % 2
    own_ctx.wait()
    for k in far + chip_bits:
        push(
            ctxv.at[ctx_rows(mine), ctx_cols(flip(chip, k // 2))], ctxg.at[k // 2, ctx_rows(mine)],
            S_CTX, ctx_r.at[k // 2], to_seq(k),
        )
    own_kw.wait()
    own_vw.wait()
    push(kvw.at[core], kvw.at[core], S_W, one_r.at[R_W], to_seq(1))
    for k in masks + [k + 1 for k in masks] + [1]:
        push(ow.at[ow_piece(flip(s, k)), :], spread.at[s], S_SP, one_r.at[R_SP], to_seq(k))
    own_qw.wait()
    first = [(0, b) for b in chip_bits[:1]] + [(1, b) for b in chip_bits[1:]]
    second = [(0, b) for b in chip_bits[1:]] + [(1, b) for b in chip_bits[:1]]
    for half, b in first + second:
        gather_own(half_rows, half, [b], S_QW, qw_r)
    gather_core(half_rows, S_QW, qc_r)

    own_vid.wait()
    strip = 16
    strips = tok // strip

    def norm(begin, end):
        with jax.named_scope("norm"):
            @pl.loop(begin, end)
            def _(i):
                at = pl.ds(pl.multiple_of(i * strip, strip), strip)
                rows = vid[at, :].astype(F32)
                mean = jnp.mean(rows, axis=-1, keepdims=True)
                centred = rows - mean
                spread_ = jnp.mean(centred * centred, axis=-1, keepdims=True)
                normed[at, :] = (centred * (1.0 / jnp.sqrt(spread_ + 1e-06))).astype(BF16)

    norm(0, strips * NORM_FIRST // 16)
    with jax.named_scope("ctx_share"):
        for k in far + chip_bits:
            here = ctxg.at[k // 2, ctx_rows(mine)]
            arrived(here, ctx_r.at[k // 2])
            push(here, here, S_CTZ, ctz_r.at[k // 2], to_head(1))
    norm(strips * NORM_FIRST // 16, strips)

    with jax.named_scope("kv"):
        arrived(kvw.at[1 - core], one_r.at[R_W])

        def partial_kv(source):
            return jnp.dot(source, kvw[...].reshape(pair, 2 * att), preferred_element_type=F32)

        block = partial_kv(ctxv[:, ctx_cols(chip)])
        cks[0] = block[:, :att]
        ckr[0] = block[:, att:]
        for k in far + chip_bits:
            c = k // 2
            arrived(ctxg.at[c, ctx_rows(1 - mine)], ctz_r.at[c])
            block = partial_kv(ctxg[c])
            cks[c] = block[:, :att]
            cvs[c] = block[:, att:].astype(BF16)
            push(cks.at[c], ckr.at[c], S_CK, one_r.at[R_CK], to_seq(k))
            push(cvs.at[c], cvr.at[c], S_CV, one_r.at[R_CV], to_seq(k))

    def chip_queries(p):
        lanes = pl.ds(pl.multiple_of(p * pair, pair), pair)
        return jnp.dot(normed[:, lanes], qwg[lanes, :], preferred_element_type=F32)

    with jax.named_scope("relay1"):
        for half, b in first:
            gather_relay(half_rows, half, b, S_QW, qw_r, qc_r)

    def own_cols(zz):
        return pl.ds(zz * ratio, ratio)

    def ow_slot_z(p):
        return owg.at[:, p, ow_piece(s), :]

    with jax.named_scope("spread"):
        own_spread.wait()
        arrived(spread.at[pl.ds(0, n_seq - 1)], one_r.at[R_SP])
        own_ow = load(spread.at[own_cols(z)], ow_slot_z(z), 7)
        for k in range(1, n_head):
            push(spread.at[own_cols(flip(z, k))], ow_slot_z(z), S_OZ, one_r.at[R_OZ], to_head(k))

    with jax.named_scope("relay2"):
        for half, b in second:
            gather_relay(half_rows, half, b, S_QW, qw_r, qc_r)
        arrived(shard_rows(flip(s, 1)), qc_r.at[0])
    with jax.named_scope("q_own"):
        queries[...] = chip_queries(chip)
    with jax.named_scope("shsc"):
        own_tw.wait()
        for copy in small:
            copy.wait()
        angles = jnp.broadcast_to(when[0].astype(F32) * freqs[...], (16, freqs.shape[1]))
        embedding = jnp.concatenate([jnp.cos(angles), jnp.sin(angles)], axis=1)
        act = (embedding / (1.0 + jnp.exp(-embedding))).astype(BF16)
        for i in range(2):
            shsc[i] = mod[i : i + 1, :] + jnp.dot(act, tw[i], preferred_element_type=F32)[:8]

    with jax.named_scope("kv_sum"):
        arrived(ckr.at[pl.ds(1, n_chip - 1)], one_r.at[R_CK])
        arrived(cvr.at[pl.ds(1, n_chip - 1)], one_r.at[R_CV])
        key_rows = cks[0]
        value_rows = ckr[0]
        for c in range(1, n_chip):
            key_rows = key_rows + ckr[c]
            value_rows = value_rows + cvr[c].astype(F32)
        cks[0] = key_rows
        ksq[0] = column_to_row(jnp.sum(key_rows * key_rows, axis=1, keepdims=True))
        for k in range(1, n_head):
            push(ksq.at[0], ksq.at[k], S_KSQ, one_r.at[R_KSQ], to_head(k))
        vall[s] = value_rows.astype(BF16)
        for k in masks:
            push(vall.at[s], vall.at[s], S_V, one_r.at[R_V], to_seq(k))
        push(vall.at[s], vall.at[s], S_V, one_r.at[R_VC], to_seq(1))

    with jax.named_scope("q_mid"):
        for b in chip_bits:
            arrived(shard_rows(flip(s, b + 1)), qc_r.at[b // 2])
            queries[...] += chip_queries(flip(chip, b // 2))

    with jax.named_scope("k_norm"):
        arrived(ksq.at[pl.ds(1, n_head - 1)], one_r.at[R_KSQ])
        k_mean = row_to_column(jnp.sum(ksq[...], axis=0), text) / (att * n_head)
        kall[s] = (cks[0] / jnp.sqrt(k_mean + 1e-06) * kg[...]).astype(BF16)
        for k in masks:
            push(kall.at[s], kall.at[s], S_K, one_r.at[R_K], to_seq(k))
        push(kall.at[s], kall.at[s], S_K, one_r.at[R_KC], to_seq(1))

    with jax.named_scope("q_far"):
        for k in far:
            for half in range(2):
                gather_relay(half_rows, half, k, S_QW, qw_r, qc_r)
        for k in far:
            arrived(shard_rows(flip(s, k + 1)), qc_r.at[k // 2])
            queries[...] += chip_queries(flip(chip, k // 2))
        q = queries[...]
        qsq[0] = column_to_row(jnp.sum(q * q, axis=1, keepdims=True))
        for k in range(1, n_head):
            push(qsq.at[0], qsq.at[k], S_QSQ, one_r.at[R_QSQ], to_head(k))

    def ow_half(half, p):
        if ratio == 1:
            rows = piece // 2
            return owg.at[:, :, pl.ds(pl.multiple_of(p * piece + half * rows, rows), rows), :]
        cut = ratio // 2
        return owg.at[pl.ds(half * cut, cut), :, ow_piece(p), :]

    def ow_slot(p):
        return owg.at[:, :, ow_piece(p), :]

    with jax.named_scope("ow_start"):
        own_ow.wait()
        arrived(owg.at[:, pl.ds(0, n_head - 1), ow_piece(s), :], one_r.at[R_OZ])
        for half, b in first + second:
            gather_own(ow_half, half, [b], S_OG, og_r)
        gather_core(ow_half, S_OG, oc_r)

    with jax.named_scope("kv_in"):
        for ref, group, chips in ((vall, S_V, R_V), (kall, S_K, R_K)):
            arrived(ref.at[pl.ds(0, n_chip - 1)], one_r.at[chips])
            for k in masks:
                here = ref.at[flip(s, k)]
                push(here, here, group, one_r.at[chips + 1], to_seq(1))
        for ref, chips in ((vall, R_V), (kall, R_K)):
            arrived(ref.at[pl.ds(0, n_chip)], one_r.at[chips + 1])

    with jax.named_scope("q_norm"):
        arrived(qsq.at[pl.ds(1, n_head - 1)], one_r.at[R_QSQ])
        q_mean = row_to_column(jnp.sum(qsq[...], axis=0), tok) / (att * n_head)
        q_normed = (queries[...] / jnp.sqrt(q_mean + 1e-06) * qg[...]).astype(BF16)

    def held(way, d):
        return d % n_head if way > 0 else (n_head - d) % n_head

    def onward(way, d):
        origin = z - way * (d - 1)
        return (origin >= 0) & (origin < n_head) & (z + way >= 0) & (z + way < n_head)

    def passed(way, d):
        return pass_s.at[0 if way > 0 else 1, d - 1]

    def reach(way, c, d):
        slot = held(way, d)

        @pl.when(onward(way, d))
        def _():
            remote(
                attg.at[held(way, d - 1), cuts[c]], attg.at[slot, cuts[c]],
                passed(way, d), at_r.at[c, slot - 1], (s, z + way),
            ).start()

    def take(way, c, d):
        slot = held(way, d)
        origin = z - way * d

        @pl.when((origin >= 0) & (origin < n_head))
        def _():
            arrived(attg.at[slot, cuts[c]], at_r.at[c, slot - 1])

    all_text = n_seq * text
    with jax.named_scope("attend"):
        every_k = kall[...].reshape(all_text, att)
        every_v = vall[...].reshape(all_text, att)
        seen = lax.broadcasted_iota(jnp.int32, (1, all_text), 1) < valid[0]
        for c in range(chunks):
            at = cuts[c]
            for h in range(att // HD):
                lanes = slice(h * HD, (h + 1) * HD)
                scores = lax.dot_general(
                    q_normed[at, lanes], every_k[:, lanes], (((1,), (1,)), ((), ())),
                    preferred_element_type=F32,
                ) * HD ** (-0.5)
                scores = jnp.where(seen, scores, F32(-1e30))
                shifted = jnp.exp(scores - jnp.max(scores, axis=-1, keepdims=True))
                weights = (shifted * (1.0 / jnp.sum(shifted, axis=-1, keepdims=True))).astype(BF16)
                attg[0, at, lanes] = jnp.dot(
                    weights, every_v[:, lanes], preferred_element_type=F32
                ).astype(BF16)
            for way in (1, -1):
                reach(way, c, 1)

    def ow_relays(pairs):
        for half, b in pairs:
            gather_relay(ow_half, half, b, S_OG, og_r, oc_r)

    for d in range(1, n_head - 1):
        for c in range(chunks):
            with jax.named_scope(f"pass{d}_{c}"):
                for way in (1, -1):
                    take(way, c, d)
                    reach(way, c, d + 1)
            if d == 1 and c == 0:
                with jax.named_scope("ow1"):
                    ow_relays(first)
            if d == 1 and c == chunks - 1:
                with jax.named_scope("ow2"):
                    ow_relays(second)
    with jax.named_scope("left1"):
        few = pl.ds(0, n_chip - 1)
        left(ctxg.at[few, ctx_rows(0)], send_sem.at[S_CTX])
        left(ctxg.at[few, ctx_rows(0)], send_sem.at[S_CTZ])
        left(kvw.at[0], send_sem.at[S_W])
        left(spread.at[pl.ds(0, n_seq - 1)], send_sem.at[S_SP])
        left(shard_rows(0, n_seq - 1), send_sem.at[S_QW])
        left(ckr.at[few], send_sem.at[S_CK])
        left(cvr.at[few], send_sem.at[S_CV])
        left(ksq.at[pl.ds(0, n_head - 1)], send_sem.at[S_KSQ])
        left(qsq.at[pl.ds(0, n_head - 1)], send_sem.at[S_QSQ])
        left(vall.at[pl.ds(0, n_seq - 1)], send_sem.at[S_V])
        left(kall.at[pl.ds(0, n_seq - 1)], send_sem.at[S_K])
        left(owg.at[:, pl.ds(0, n_head - 1), ow_piece(0), :], send_sem.at[S_OZ])
    with jax.named_scope("ow3"):
        for k in far:
            for half in range(2):
                gather_relay(ow_half, half, k, S_OG, og_r, oc_r)
        for k in [0] + masks:
            arrived(ow_slot(flip(s, k + 1)), oc_r.at[k // 2])

    cols = owg.shape[3]
    part_width = mod_out.shape[1]

    def modulate(c):
        at = cuts[c]
        step = at.stop - at.start
        with jax.named_scope(f"stat{c}"):
            arrived(stat.at[c, pl.ds(1, n_head - 1)], st_r.at[c])
        with jax.named_scope(f"modulate{c}"):
            both = jnp.sum(stat[c], axis=0) / (part_width * n_head)
            mean2 = both[:1]
            inverse = 1.0 / jnp.sqrt(both[1:] - mean2 * mean2 + 1e-06)
            mean_col = row_to_column(mean2, step)
            inv_col = row_to_column(inverse, step)
            wide = resid_out[at, :].astype(F32)
            mod_out[at, :] = (
                (wide - mean_col) * inv_col * (1.0 + shsc[1, :1, :]) + shsc[0, :1, :]
            ).astype(BF16)

    for c in range(chunks):
        at = cuts[c]
        step = at.stop - at.start
        with jax.named_scope(f"last{c}"):
            for way in (1, -1):
                take(way, c, n_head - 1)
        with jax.named_scope(f"project{c}"):
            row_sum = jnp.zeros((step, 1), F32)
            row_sq = jnp.zeros((step, 1), F32)
            for j in range(ratio):
                here = slice(j * cols, (j + 1) * cols)
                projected = jnp.dot(attg[0, at], owg[j, z], preferred_element_type=F32)
                for k in range(1, n_head):
                    projected = projected + jnp.dot(
                        attg[k, at], owg[j, lax.rem(z + n_head - k, n_head)],
                        preferred_element_type=F32,
                    )
                if vpart is None:
                    base = vid[at, pl.ds(pl.multiple_of(z * part_width + j * cols, LANES), cols)]
                else:
                    base = vpart[at, here]
                rounded = (base.astype(F32) + projected).astype(BF16)
                resid_out[at, here] = rounded
                wide = rounded.astype(F32)
                row_sum = row_sum + jnp.sum(wide, axis=1, keepdims=True)
                row_sq = row_sq + jnp.sum(wide * wide, axis=1, keepdims=True)
            stat[c, 0, :1] = column_to_row(row_sum)
            stat[c, 0, 1:] = column_to_row(row_sq)
            for k in range(1, n_head):
                push(stat.at[c, 0], stat.at[c, k], S_ST, st_r.at[c], to_head(k))
        if c >= 3:
            modulate(c - 3)
    with jax.named_scope("left2"):
        left(owg.at[:, :, pl.ds(0, piece * (n_seq - 1)), :], send_sem.at[S_OG])
        for way in (1, -1):
            for d in range(1, n_head):
                @pl.when(onward(way, d))
                def _():
                    left(attg.at[0], passed(way, d))
    for c in range(max(chunks - 3, 0), chunks):
        modulate(c)
    left(stat.at[:, pl.ds(0, n_head - 1)], send_sem.at[S_ST])


def put_out(resid, mod, resid_hbm, mod_hbm, sems):
    first = pltpu.make_async_copy(resid, resid_hbm, sems.at[0])
    second = pltpu.make_async_copy(mod, mod_hbm, sems.at[1])
    first.start()
    second.start()
    first.wait()
    second.wait()


def on_device(
    n_seq,
    n_head,
    video_rows,
    context,
    valid_length,
    timestep,
    query_weight,
    key_weight,
    value_weight,
    out_weight,
    query_gain,
    key_gain,
    time_weight,
    modulation,
):
    tok, width = video_rows.shape
    text = context.shape[0]
    depth, att = query_weight.shape
    cols = out_weight.shape[1]
    part_width = modulation.shape[1]
    ratio = n_seq // n_head
    n_chip = n_seq // 2
    quarter = tok // 4
    sizes = [quarter] * 3 + [quarter // 2] * 2
    cuts = [slice(sum(sizes[:c]), sum(sizes[: c + 1])) for c in range(len(sizes))]
    chunks = len(cuts)
    piece = out_weight.shape[0] // n_seq
    half = FREQ // 2
    freqs = np.exp(-np.log(10000.0) * np.arange(half) / half).astype(np.float32)[None, :]
    sliced = part_width % LANES != 0 or cols % LANES != 0
    extra = []
    if sliced:
        extra.append(
            lax.dynamic_slice_in_dim(
                video_rows, lax.axis_index("head") * part_width, part_width, 1
            )
        )
    out_bytes = tok * -(-part_width // LANES) * LANES * 2
    vmem = pl.BlockSpec(memory_space=pltpu.VMEM)
    hbm = pl.BlockSpec(memory_space=pltpu.HBM)
    dma = pltpu.SemaphoreType.DMA
    results = pl.pallas_call(
        functools.partial(body, n_seq, n_head, cuts, sliced),
        out_shape=[pltpu.VMEM((tok, part_width), BF16)] * 2,
        in_specs=[pl.BlockSpec(memory_space=pltpu.SMEM)] * 2
        + [hbm] * 11
        + [vmem] * len(extra),
        out_specs=[vmem] * 2,
        scratch_shapes=[
            pltpu.VMEM((tok, width), BF16),
            pltpu.VMEM((tok, width), BF16),
            pltpu.VMEM((text, width), BF16),
            pltpu.VMEM((n_chip, text, 2 * depth), BF16),
            pltpu.VMEM((n_seq * depth, att), BF16),
            pltpu.VMEM((2, depth, 2 * att), BF16),
            pltpu.VMEM((n_chip, text, att), F32),
            pltpu.VMEM((n_chip, text, att), F32),
            pltpu.VMEM((n_chip, text, att), BF16),
            pltpu.VMEM((n_chip, text, att), BF16),
            pltpu.VMEM((n_seq, text, att), BF16),
            pltpu.VMEM((n_seq, text, att), BF16),
            pltpu.VMEM((n_seq, piece, cols), BF16),
            pltpu.VMEM((ratio, n_head, out_weight.shape[0], cols), BF16),
            pltpu.VMEM((n_head, tok, att), BF16),
            pltpu.VMEM((tok, att), F32),
            pltpu.VMEM((n_head, 1, tok), F32),
            pltpu.VMEM((n_head, 1, -(-text // LANES) * LANES), F32),
            pltpu.VMEM((chunks, n_head, 2, LANES), F32),
            pltpu.VMEM((2, 8, part_width), F32),
            pltpu.VMEM(time_weight.shape, BF16),
            pltpu.VMEM((1, att), F32),
            pltpu.VMEM((1, att), F32),
            pltpu.VMEM((1, half), F32),
            pltpu.VMEM(modulation.shape, F32),
            dma((12,)),
            dma((14,)),
            dma((2, n_head - 1)),
            *[dma((n_chip,))] * 2,
            *[dma((2, n_chip)), dma((n_chip,))] * 2,
            dma((chunks, n_head - 1)),
            dma((chunks,)),
            dma((11,)),
        ],
        compiler_params=pltpu.CompilerParams(
            collective_id=0, has_side_effects=True, vmem_limit_bytes=VMEM_MOST - 2 * out_bytes
        ),
    )(
        valid_length,
        timestep,
        video_rows,
        context,
        query_weight,
        key_weight,
        value_weight,
        out_weight,
        query_gain[None, :],
        key_gain[None, :],
        freqs,
        time_weight,
        modulation,
        *extra,
    )
    return pl.pallas_call(
        put_out,
        out_shape=[jax.ShapeDtypeStruct((tok, part_width), BF16)] * 2,
        in_specs=[vmem] * 2,
        out_specs=[hbm] * 2,
        scratch_shapes=[dma((2,))],
        compiler_params=pltpu.CompilerParams(vmem_limit_bytes=4 * 1024 * 1024),
    )(*results)


def solution(mesh):
    in_specs = (
        P("seq", None),
        P("seq", None),
        P(),
        P(),
        P("seq", "head"),
        P("seq", "head"),
        P("seq", "head"),
        P("head", "seq"),
        P("head"),
        P("head"),
        P(None, None, "head"),
        P(None, "head"),
    )
    out_specs = (P("seq", "head"), P("seq", "head"))
    return jax.shard_map(
        functools.partial(on_device, mesh.shape["seq"], mesh.shape["head"]),
        mesh=mesh, in_specs=in_specs, out_specs=out_specs, check_vma=False,
    )
```

```python
import functools

import jax
import jax.numpy as jnp
import numpy as np
from jax import lax
from jax.experimental import pallas as pl
from jax.experimental.pallas import tpu as pltpu
from jax.sharding import PartitionSpec as P

HD = 128
FREQ = 256
LANES = 128
VMEM_MOST = 67_000_000
NORM_FIRST = 9
OW_FIRST = 3
F32 = jnp.float32
BF16 = jnp.bfloat16
MESH_ID = pl.DeviceIdType.MESH


def flip(index, mask):
    bit = 1
    while bit <= mask:
        if mask & bit:
            index = index + bit - 2 * bit * ((index // bit) % 2)
        bit *= 2
    return index


def bits_of(mask):
    return [1 << b for b in range(mask.bit_length()) if mask >> b & 1]


def last_bit(half, mask):
    return bits_of(mask)[-1] if half == 0 else bits_of(mask)[0]


def by_hops(n_seq):
    return sorted(range(2, n_seq, 2), key=lambda k: (len(bits_of(k)), k))


def column_to_row(column):
    tall = column.shape[0]
    wide = -(-tall // LANES) * LANES
    if wide > tall:
        column = jnp.concatenate([column, jnp.zeros((wide - tall, 1), F32)], axis=0)
    return jnp.transpose(jnp.broadcast_to(column, (wide, LANES)))[:1]


def row_to_column(row, tall):
    return jnp.transpose(jnp.broadcast_to(row, (LANES, row.shape[1])))[:tall, :1]


def body(n_seq, n_head, cuts, sliced, *refs):
    if sliced:
        steps(n_seq, n_head, cuts, *refs)
    else:
        steps(n_seq, n_head, cuts, *refs[:13], None, *refs[13:])


def steps(
    n_seq, n_head, cuts,
    valid_hbm, when_hbm, video, ctx, qw, kw, vw, ow, qg_hbm, kg_hbm, freqs_hbm, tw_hbm, mod_hbm, vpart,
    resid_out, mod_out,
    vid, normed, ctxv, ctxg, qwg, kvw, cks, ckr, cvs, cvr, kall, vall, spread, owg, attg,
    queries, qsq, ksq, stat, shsc, tw, qg, kg, freqs, mod, acc, valid, when,
    loc_sem, send_sem, pass_s, ctx_r, ctz_r, qw_r, qc_r, og_r, oc_r, at_r, st_r, one_r,
):
    s = lax.axis_index("seq")
    z = lax.axis_index("head")
    core = s % 2
    chip = s // 2
    n_chip = n_seq // 2
    ratio = n_seq // n_head
    chunks = len(cuts)
    tok, width = vid.shape
    depth = qw.shape[0]
    att = qw.shape[1]
    text = ctx.shape[0]
    pair = 2 * depth
    masks = by_hops(n_seq)
    chip_bits = [k for k in masks if len(bits_of(k)) == 1]
    far = [k for k in masks if k not in chip_bits]
    (S_CTX, S_CTZ, S_W, S_SP, S_QW, S_CK, S_CV, S_KSQ, S_QSQ, S_V, S_K, S_OZ, S_OG, S_ST) = range(14)
    (R_W, R_SP, R_CK, R_CV, R_KSQ, R_QSQ, R_V, R_VC, R_K, R_KC, R_OZ) = range(11)

    def to_seq(k):
        return (flip(s, k), z)

    def to_head(k):
        return (s, flip(z, k))

    def remote(src, dst, ssem, rsem, dev):
        return pltpu.make_async_remote_copy(
            src_ref=src, dst_ref=dst, send_sem=ssem, recv_sem=rsem,
            device_id=dev, device_id_type=MESH_ID,
        )

    def push(src, dst, group, rsem, dev):
        remote(src, dst, send_sem.at[group], rsem, dev).start()

    def arrived(ref, sem):
        remote(ref, ref, sem, sem, to_seq(1)).wait_recv()

    def left(ref, sem):
        remote(ref, ref, sem, sem, to_seq(1)).wait_send()

    def gather_own(slot, half, bits, group, rsem):
        for b in bits:
            push(slot(half, s), slot(half, s), group, rsem.at[half, b // 2], to_seq(b))

    def gather_core(slot, group, csem):
        for half in range(2):
            push(slot(half, s), slot(half, s), group, csem.at[0], to_seq(1))

    def gather_relay(slot, half, k, group, rsem, csem):
        here = slot(half, flip(s, k))
        arrived(here, rsem.at[half, k // 2])
        for b in chip_bits:
            if not k & b and last_bit(half, k | b) == b:
                push(here, here, group, rsem.at[half, (k | b) // 2], to_seq(b))
        push(here, here, group, csem.at[k // 2], to_seq(1))

    barrier = pltpu.get_barrier_semaphore()
    for k in range(1, n_seq):
        pl.semaphore_signal(barrier, inc=1, device_id=to_seq(k), device_id_type=MESH_ID)
    for k in range(1, n_head):
        pl.semaphore_signal(barrier, inc=1, device_id=to_head(k), device_id_type=MESH_ID)

    def shard_rows(p, count=1):
        return qwg.at[pl.ds(pl.multiple_of(p * depth, depth), count * depth), :]

    def half_rows(half, p):
        rows = depth // 2
        return qwg.at[pl.ds(pl.multiple_of(p * depth + half * rows, rows), rows), :]

    def load(src, dst, i):
        copy = pltpu.make_async_copy(src, dst, loc_sem.at[i])
        copy.start()
        return copy

    piece = ow.shape[0] // n_seq

    def ow_piece(p):
        return pl.ds(pl.multiple_of(p * piece, piece), piece)

    own_ctx = load(ctx, ctxv, 0)
    own_qw = load(qw, shard_rows(s), 1)
    own_kw = load(kw, kvw.at[core, :, :att], 2)
    own_vw = load(vw, kvw.at[core, :, att:], 3)
    own_vid = load(video, vid, 4)
    own_spread = load(ow.at[ow_piece(s), :], spread.at[s], 5)
    own_tw = load(tw_hbm, tw, 6)
    small = [
        load(a, b, 8 + i)
        for i, (a, b) in enumerate(
            (
                (qg_hbm, qg), (kg_hbm, kg), (freqs_hbm, freqs), (mod_hbm, mod),
                (valid_hbm, valid), (when_hbm, when),
            )
        )
    ]
    with jax.named_scope("barrier"):
        pl.semaphore_wait(barrier, n_seq + n_head - 2)

    def ctx_cols(p):
        return pl.ds(pl.multiple_of(p * pair, pair), pair)

    part = text // 2

    def ctx_rows(q):
        return pl.ds(pl.multiple_of(q * part, part), part)

    mine = z % 2
    own_ctx.wait()
    for k in far + chip_bits:
        push(
            ctxv.at[ctx_rows(mine), ctx_cols(flip(chip, k // 2))], ctxg.at[k // 2, ctx_rows(mine)],
            S_CTX, ctx_r.at[k // 2], to_seq(k),
        )
    own_kw.wait()
    own_vw.wait()
    push(kvw.at[core], kvw.at[core], S_W, one_r.at[R_W], to_seq(1))
    for k in masks + [k + 1 for k in masks] + [1]:
        push(ow.at[ow_piece(flip(s, k)), :], spread.at[s], S_SP, one_r.at[R_SP], to_seq(k))
    own_qw.wait()
    first = [(0, b) for b in chip_bits[:1]] + [(1, b) for b in chip_bits[1:]]
    second = [(0, b) for b in chip_bits[1:]] + [(1, b) for b in chip_bits[:1]]
    for half, b in first + second:
        gather_own(half_rows, half, [b], S_QW, qw_r)
    gather_core(half_rows, S_QW, qc_r)

    own_vid.wait()
    strip = 16
    strips = tok // strip

    def norm(begin, end):
        with jax.named_scope("norm"):
            @pl.loop(begin, end)
            def _(i):
                at = pl.ds(pl.multiple_of(i * strip, strip), strip)
                rows = vid[at, :].astype(F32)
                mean = jnp.mean(rows, axis=-1, keepdims=True)
                centred = rows - mean
                spread_ = jnp.mean(centred * centred, axis=-1, keepdims=True)
                normed[at, :] = (centred * (1.0 / jnp.sqrt(spread_ + 1e-06))).astype(BF16)

    norm(0, strips * NORM_FIRST // 16)
    with jax.named_scope("ctx_share"):
        for k in far + chip_bits:
            here = ctxg.at[k // 2, ctx_rows(mine)]
            arrived(here, ctx_r.at[k // 2])
            push(here, here, S_CTZ, ctz_r.at[k // 2], to_head(1))
    norm(strips * NORM_FIRST // 16, strips)

    with jax.named_scope("kv"):
        arrived(kvw.at[1 - core], one_r.at[R_W])

        def partial_kv(source):
            return jnp.dot(source, kvw[...].reshape(pair, 2 * att), preferred_element_type=F32)

        block = partial_kv(ctxv[:, ctx_cols(chip)])
        cks[0] = block[:, :att]
        ckr[0] = block[:, att:]
        for k in far + chip_bits:
            c = k // 2
            arrived(ctxg.at[c, ctx_rows(1 - mine)], ctz_r.at[c])
            block = partial_kv(ctxg[c])
            cks[c] = block[:, :att]
            cvs[c] = block[:, att:].astype(BF16)
            push(cks.at[c], ckr.at[c], S_CK, one_r.at[R_CK], to_seq(k))
        for k in far + chip_bits:
            c = k // 2
            push(cvs.at[c], cvr.at[c], S_CV, one_r.at[R_CV], to_seq(k))

    def chip_queries(p):
        lanes = pl.ds(pl.multiple_of(p * pair, pair), pair)
        return jnp.dot(normed[:, lanes], qwg[lanes, :], preferred_element_type=F32)

    with jax.named_scope("relay1"):
        for half, b in first:
            gather_relay(half_rows, half, b, S_QW, qw_r, qc_r)

    def own_cols(zz):
        return pl.ds(zz * ratio, ratio)

    def ow_slot_z(p):
        return owg.at[:, p, ow_piece(s), :]

    with jax.named_scope("spread"):
        own_spread.wait()
        arrived(spread.at[pl.ds(0, n_seq - 1)], one_r.at[R_SP])
        own_ow = load(spread.at[own_cols(z)], ow_slot_z(z), 7)
        for k in range(1, n_head):
            push(spread.at[own_cols(flip(z, k))], ow_slot_z(z), S_OZ, one_r.at[R_OZ], to_head(k))

    with jax.named_scope("relay2"):
        for half, b in second:
            gather_relay(half_rows, half, b, S_QW, qw_r, qc_r)
        arrived(shard_rows(flip(s, 1)), qc_r.at[0])
    with jax.named_scope("q_own"):
        queries[...] = chip_queries(chip)
    with jax.named_scope("shsc"):
        own_tw.wait()
        for copy in small:
            copy.wait()
        angles = jnp.broadcast_to(when[0].astype(F32) * freqs[...], (16, freqs.shape[1]))
        embedding = jnp.concatenate([jnp.cos(angles), jnp.sin(angles)], axis=1)
        act = (embedding / (1.0 + jnp.exp(-embedding))).astype(BF16)
        for i in range(2):
            shsc[i] = mod[i : i + 1, :] + jnp.dot(act, tw[i], preferred_element_type=F32)[:8]

    with jax.named_scope("kv_sum"):
        arrived(ckr.at[pl.ds(1, n_chip - 1)], one_r.at[R_CK])
        key_rows = cks[0]
        for c in range(1, n_chip):
            key_rows = key_rows + ckr[c]
        cks[0] = key_rows
        ksq[0] = column_to_row(jnp.sum(key_rows * key_rows, axis=1, keepdims=True))
        for k in range(1, n_head):
            push(ksq.at[0], ksq.at[k], S_KSQ, one_r.at[R_KSQ], to_head(k))
        arrived(cvr.at[pl.ds(1, n_chip - 1)], one_r.at[R_CV])
        value_rows = ckr[0]
        for c in range(1, n_chip):
            value_rows = value_rows + cvr[c].astype(F32)
        vall[s] = value_rows.astype(BF16)
        for k in masks:
            push(vall.at[s], vall.at[s], S_V, one_r.at[R_V], to_seq(k))
        push(vall.at[s], vall.at[s], S_V, one_r.at[R_VC], to_seq(1))

    with jax.named_scope("q_mid"):
        for b in chip_bits:
            arrived(shard_rows(flip(s, b + 1)), qc_r.at[b // 2])
            queries[...] += chip_queries(flip(chip, b // 2))

    with jax.named_scope("k_norm"):
        arrived(ksq.at[pl.ds(1, n_head - 1)], one_r.at[R_KSQ])
        k_mean = row_to_column(jnp.sum(ksq[...], axis=0), text) / (att * n_head)
        kall[s] = (cks[0] / jnp.sqrt(k_mean + 1e-06) * kg[...]).astype(BF16)
        for k in masks:
            push(kall.at[s], kall.at[s], S_K, one_r.at[R_K], to_seq(k))
        push(kall.at[s], kall.at[s], S_K, one_r.at[R_KC], to_seq(1))

    def ow_half(half, p):
        if ratio == 1:
            rows = piece // 2
            return owg.at[:, :, pl.ds(pl.multiple_of(p * piece + half * rows, rows), rows), :]
        cut = ratio // 2
        return owg.at[pl.ds(half * cut, cut), :, ow_piece(p), :]

    def ow_slot(p):
        return owg.at[:, :, ow_piece(p), :]

    with jax.named_scope("ow_start"):
        own_ow.wait()
        arrived(owg.at[:, pl.ds(0, n_head - 1), ow_piece(s), :], one_r.at[R_OZ])
        for half, b in first + second:
            gather_own(ow_half, half, [b], S_OG, og_r)
        gather_core(ow_half, S_OG, oc_r)

    with jax.named_scope("q_far"):
        for k in far:
            for half in range(2):
                gather_relay(half_rows, half, k, S_QW, qw_r, qc_r)
        for k in far:
            arrived(shard_rows(flip(s, k + 1)), qc_r.at[k // 2])
            queries[...] += chip_queries(flip(chip, k // 2))
        q = queries[...]
        qsq[0] = column_to_row(jnp.sum(q * q, axis=1, keepdims=True))
        for k in range(1, n_head):
            push(qsq.at[0], qsq.at[k], S_QSQ, one_r.at[R_QSQ], to_head(k))

    with jax.named_scope("kv_in"):
        for ref, group, chips in ((vall, S_V, R_V), (kall, S_K, R_K)):
            arrived(ref.at[pl.ds(0, n_chip - 1)], one_r.at[chips])
            for k in masks:
                here = ref.at[flip(s, k)]
                push(here, here, group, one_r.at[chips + 1], to_seq(1))
        for ref, chips in ((vall, R_V), (kall, R_K)):
            arrived(ref.at[pl.ds(0, n_chip)], one_r.at[chips + 1])

    with jax.named_scope("q_norm"):
        arrived(qsq.at[pl.ds(1, n_head - 1)], one_r.at[R_QSQ])
        q_mean = row_to_column(jnp.sum(qsq[...], axis=0), tok) / (att * n_head)
        q_normed = (queries[...] / jnp.sqrt(q_mean + 1e-06) * qg[...]).astype(BF16)

    def held(way, d):
        return d % n_head if way > 0 else (n_head - d) % n_head

    def onward(way, d):
        origin = z - way * (d - 1)
        return (origin >= 0) & (origin < n_head) & (z + way >= 0) & (z + way < n_head)

    def passed(way, d):
        return pass_s.at[0 if way > 0 else 1, d - 1]

    def reach(way, c, d):
        slot = held(way, d)

        @pl.when(onward(way, d))
        def _():
            remote(
                attg.at[held(way, d - 1), cuts[c]], attg.at[slot, cuts[c]],
                passed(way, d), at_r.at[c, slot - 1], (s, z + way),
            ).start()

    def take(way, c, d):
        slot = held(way, d)
        origin = z - way * d

        @pl.when((origin >= 0) & (origin < n_head))
        def _():
            arrived(attg.at[slot, cuts[c]], at_r.at[c, slot - 1])

    def ow_relays(pairs):
        for half, b in pairs:
            gather_relay(ow_half, half, b, S_OG, og_r, oc_r)

    all_text = n_seq * text
    with jax.named_scope("attend"):
        every_k = kall[...].reshape(all_text, att)
        every_v = vall[...].reshape(all_text, att)
        seen = lax.broadcasted_iota(jnp.int32, (1, all_text), 1) < valid[0]
        for c in range(chunks):
            at = cuts[c]
            for h in range(att // HD):
                lanes = slice(h * HD, (h + 1) * HD)
                scores = lax.dot_general(
                    q_normed[at, lanes], every_k[:, lanes], (((1,), (1,)), ((), ())),
                    preferred_element_type=F32,
                ) * HD ** (-0.5)
                scores = jnp.where(seen, scores, F32(-1e30))
                shifted = jnp.exp(scores - jnp.max(scores, axis=-1, keepdims=True))
                weights = (shifted * (1.0 / jnp.sum(shifted, axis=-1, keepdims=True))).astype(BF16)
                attg[0, at, lanes] = jnp.dot(
                    weights, every_v[:, lanes], preferred_element_type=F32
                ).astype(BF16)
            for way in (1, -1):
                reach(way, c, 1)
            if c == OW_FIRST:
                ow_relays(first)

    cols = owg.shape[3]
    part_width = mod_out.shape[1]
    last = z + 1 - (2 * z) // n_head

    def projection(at, j, slot):
        return jnp.dot(
            attg[slot, at], owg[j, lax.rem(z + n_head - slot, n_head)], preferred_element_type=F32
        )

    def accumulate(c):
        at = cuts[c]
        with jax.named_scope(f"accumulate{c}"):
            for j in range(ratio):
                here = slice(j * cols, (j + 1) * cols)
                if vpart is None:
                    base = vid[at, pl.ds(pl.multiple_of(z * part_width + j * cols, LANES), cols)]
                else:
                    base = vpart[at, here]
                projected = projection(at, j, 0)
                for i in range(1, n_head - 1):
                    projected = projected + projection(at, j, lax.rem(last - 1 + i, n_head - 1) + 1)
                acc[at, here] = base.astype(F32) + projected

    for d in range(1, n_head - 1):
        for c in range(chunks):
            with jax.named_scope(f"pass{d}_{c}"):
                for way in (1, -1):
                    take(way, c, d)
                    reach(way, c, d + 1)
            if d == 1 and c == 1:
                with jax.named_scope("ow2"):
                    ow_relays(second)
            if d == n_head - 2 and c == 0:
                with jax.named_scope("ow3"):
                    for k in far:
                        for half in range(2):
                            gather_relay(ow_half, half, k, S_OG, og_r, oc_r)
            if d == n_head - 2 and c == 1:
                with jax.named_scope("ow4"):
                    for k in [0] + masks:
                        arrived(ow_slot(flip(s, k + 1)), oc_r.at[k // 2])
            if d == n_head - 2 and c >= 1:
                accumulate(c - 1)
    accumulate(chunks - 1)
    with jax.named_scope("left1"):
        few = pl.ds(0, n_chip - 1)
        left(ctxg.at[few, ctx_rows(0)], send_sem.at[S_CTX])
        left(ctxg.at[few, ctx_rows(0)], send_sem.at[S_CTZ])
        left(kvw.at[0], send_sem.at[S_W])
        left(spread.at[pl.ds(0, n_seq - 1)], send_sem.at[S_SP])
        left(shard_rows(0, n_seq - 1), send_sem.at[S_QW])
        left(ckr.at[few], send_sem.at[S_CK])
        left(cvr.at[few], send_sem.at[S_CV])
        left(ksq.at[pl.ds(0, n_head - 1)], send_sem.at[S_KSQ])
        left(qsq.at[pl.ds(0, n_head - 1)], send_sem.at[S_QSQ])
        left(vall.at[pl.ds(0, n_seq - 1)], send_sem.at[S_V])
        left(kall.at[pl.ds(0, n_seq - 1)], send_sem.at[S_K])
        left(owg.at[:, pl.ds(0, n_head - 1), ow_piece(0), :], send_sem.at[S_OZ])
    def modulate(c):
        at = cuts[c]
        step = at.stop - at.start
        with jax.named_scope(f"stat{c}"):
            arrived(stat.at[c, pl.ds(1, n_head - 1)], st_r.at[c])
        with jax.named_scope(f"modulate{c}"):
            both = jnp.sum(stat[c], axis=0) / (part_width * n_head)
            mean2 = both[:1]
            inverse = 1.0 / jnp.sqrt(both[1:] - mean2 * mean2 + 1e-06)
            mean_col = row_to_column(mean2, step)
            inv_col = row_to_column(inverse, step)
            wide = resid_out[at, :].astype(F32)
            mod_out[at, :] = (
                (wide - mean_col) * inv_col * (1.0 + shsc[1, :1, :]) + shsc[0, :1, :]
            ).astype(BF16)

    for c in range(chunks):
        at = cuts[c]
        step = at.stop - at.start
        with jax.named_scope(f"last{c}"):
            for way in (1, -1):
                take(way, c, n_head - 1)
        with jax.named_scope(f"project{c}"):
            row_sum = jnp.zeros((step, 1), F32)
            row_sq = jnp.zeros((step, 1), F32)
            for j in range(ratio):
                here = slice(j * cols, (j + 1) * cols)
                rounded = (acc[at, here] + projection(at, j, last)).astype(BF16)
                resid_out[at, here] = rounded
                wide = rounded.astype(F32)
                row_sum = row_sum + jnp.sum(wide, axis=1, keepdims=True)
                row_sq = row_sq + jnp.sum(wide * wide, axis=1, keepdims=True)
            stat[c, 0, :1] = column_to_row(row_sum)
            stat[c, 0, 1:] = column_to_row(row_sq)
            for k in range(1, n_head):
                push(stat.at[c, 0], stat.at[c, k], S_ST, st_r.at[c], to_head(k))
        if c >= 3:
            modulate(c - 3)
    with jax.named_scope("left2"):
        left(owg.at[:, :, pl.ds(0, piece * (n_seq - 1)), :], send_sem.at[S_OG])
        for way in (1, -1):
            for d in range(1, n_head):
                @pl.when(onward(way, d))
                def _():
                    left(attg.at[0], passed(way, d))
    for c in range(max(chunks - 3, 0), chunks):
        modulate(c)
    left(stat.at[:, pl.ds(0, n_head - 1)], send_sem.at[S_ST])


def put_out(resid, mod, resid_hbm, mod_hbm, sems):
    pieces = sems.shape[1]
    rows = resid.shape[0] // pieces
    copies = [
        pltpu.make_async_copy(src.at[at], dst.at[at], sems.at[i, p])
        for p, at in enumerate(pl.ds(p * rows, rows) for p in range(pieces))
        for i, (src, dst) in enumerate(((resid, resid_hbm), (mod, mod_hbm)))
    ]
    for copy in copies:
        copy.start()
    for copy in copies:
        copy.wait()


def on_device(
    n_seq,
    n_head,
    video_rows,
    context,
    valid_length,
    timestep,
    query_weight,
    key_weight,
    value_weight,
    out_weight,
    query_gain,
    key_gain,
    time_weight,
    modulation,
):
    tok, width = video_rows.shape
    text = context.shape[0]
    depth, att = query_weight.shape
    cols = out_weight.shape[1]
    part_width = modulation.shape[1]
    ratio = n_seq // n_head
    n_chip = n_seq // 2
    quarter = tok // 4
    sizes = [quarter // 2] + [quarter] * 3 + [quarter // 2]
    cuts = [slice(sum(sizes[:c]), sum(sizes[: c + 1])) for c in range(len(sizes))]
    chunks = len(cuts)
    piece = out_weight.shape[0] // n_seq
    half = FREQ // 2
    freqs = np.exp(-np.log(10000.0) * np.arange(half) / half).astype(np.float32)[None, :]
    sliced = part_width % LANES != 0 or cols % LANES != 0
    extra = []
    if sliced:
        extra.append(
            lax.dynamic_slice_in_dim(
                video_rows, lax.axis_index("head") * part_width, part_width, 1
            )
        )
    out_bytes = tok * -(-part_width // LANES) * LANES * 2
    vmem = pl.BlockSpec(memory_space=pltpu.VMEM)
    hbm = pl.BlockSpec(memory_space=pltpu.HBM)
    dma = pltpu.SemaphoreType.DMA
    results = pl.pallas_call(
        functools.partial(body, n_seq, n_head, cuts, sliced),
        out_shape=[pltpu.VMEM((tok, part_width), BF16)] * 2,
        in_specs=[hbm] * 13 + [vmem] * len(extra),
        out_specs=[vmem] * 2,
        scratch_shapes=[
            pltpu.VMEM((tok, width), BF16),
            pltpu.VMEM((tok, width), BF16),
            pltpu.VMEM((text, width), BF16),
            pltpu.VMEM((n_chip, text, 2 * depth), BF16),
            pltpu.VMEM((n_seq * depth, att), BF16),
            pltpu.VMEM((2, depth, 2 * att), BF16),
            pltpu.VMEM((n_chip, text, att), F32),
            pltpu.VMEM((n_chip, text, att), F32),
            pltpu.VMEM((n_chip, text, att), BF16),
            pltpu.VMEM((n_chip, text, att), BF16),
            pltpu.VMEM((n_seq, text, att), BF16),
            pltpu.VMEM((n_seq, text, att), BF16),
            pltpu.VMEM((n_seq, piece, cols), BF16),
            pltpu.VMEM((ratio, n_head, out_weight.shape[0], cols), BF16),
            pltpu.VMEM((n_head, tok, att), BF16),
            pltpu.VMEM((tok, att), F32),
            pltpu.VMEM((n_head, 1, tok), F32),
            pltpu.VMEM((n_head, 1, -(-text // LANES) * LANES), F32),
            pltpu.VMEM((chunks, n_head, 2, -(-max(sizes) // LANES) * LANES), F32),
            pltpu.VMEM((2, 8, part_width), F32),
            pltpu.VMEM(time_weight.shape, BF16),
            pltpu.VMEM((1, att), F32),
            pltpu.VMEM((1, att), F32),
            pltpu.VMEM((1, half), F32),
            pltpu.VMEM(modulation.shape, F32),
            pltpu.VMEM((tok, part_width), F32),
            pltpu.SMEM((1,), jnp.int32),
            pltpu.SMEM((1,), jnp.int32),
            dma((14,)),
            dma((14,)),
            dma((2, n_head - 1)),
            *[dma((n_chip,))] * 2,
            *[dma((2, n_chip)), dma((n_chip,))] * 2,
            dma((chunks, n_head - 1)),
            dma((chunks,)),
            dma((11,)),
        ],
        compiler_params=pltpu.CompilerParams(
            collective_id=0, has_side_effects=True, vmem_limit_bytes=VMEM_MOST - 2 * out_bytes
        ),
    )(
        valid_length,
        timestep,
        video_rows,
        context,
        query_weight,
        key_weight,
        value_weight,
        out_weight,
        query_gain[None, :],
        key_gain[None, :],
        freqs,
        time_weight,
        modulation,
        *extra,
    )
    return pl.pallas_call(
        put_out,
        out_shape=[jax.ShapeDtypeStruct((tok, part_width), BF16)] * 2,
        in_specs=[vmem] * 2,
        out_specs=[hbm] * 2,
        scratch_shapes=[dma((2, 4))],
        compiler_params=pltpu.CompilerParams(vmem_limit_bytes=4 * 1024 * 1024),
    )(*results)


def solution(mesh):
    in_specs = (
        P("seq", None),
        P("seq", None),
        P(),
        P(),
        P("seq", "head"),
        P("seq", "head"),
        P("seq", "head"),
        P("head", "seq"),
        P("head"),
        P("head"),
        P(None, None, "head"),
        P(None, "head"),
    )
    out_specs = (P("seq", "head"), P("seq", "head"))
    return jax.shard_map(
        functools.partial(on_device, mesh.shape["seq"], mesh.shape["head"]),
        mesh=mesh, in_specs=in_specs, out_specs=out_specs, check_vma=False,
    )
```

```python
import functools

import jax
import jax.numpy as jnp
import numpy as np
from jax import lax
from jax.experimental import pallas as pl
from jax.experimental.pallas import tpu as pltpu
from jax.sharding import PartitionSpec as P

HD = 128
FREQ = 256
LANES = 128
VMEM_MOST = 67_000_000
NORM_AT = (5, 8)
OW_FIRST = 3
F32 = jnp.float32
BF16 = jnp.bfloat16
MESH_ID = pl.DeviceIdType.MESH


def flip(index, mask):
    bit = 1
    while bit <= mask:
        if mask & bit:
            index = index + bit - 2 * bit * ((index // bit) % 2)
        bit *= 2
    return index


def bits_of(mask):
    return [1 << b for b in range(mask.bit_length()) if mask >> b & 1]


def last_bit(half, mask):
    return bits_of(mask)[-1] if half == 0 else bits_of(mask)[0]


def by_hops(n_seq):
    return sorted(range(2, n_seq, 2), key=lambda k: (len(bits_of(k)), k))


def column_to_row(column):
    tall = column.shape[0]
    wide = -(-tall // LANES) * LANES
    if wide > tall:
        column = jnp.concatenate([column, jnp.zeros((wide - tall, 1), F32)], axis=0)
    return jnp.transpose(jnp.broadcast_to(column, (wide, LANES)))[:1]


def row_to_column(row, tall):
    return jnp.transpose(jnp.broadcast_to(row, (LANES, row.shape[1])))[:tall, :1]


def body(n_seq, n_head, cuts, sliced, *refs):
    if sliced:
        steps(n_seq, n_head, cuts, *refs)
    else:
        steps(n_seq, n_head, cuts, *refs[:13], None, *refs[13:])


def steps(
    n_seq, n_head, cuts,
    valid_hbm, when_hbm, video, ctx, qw, kw, vw, ow, qg_hbm, kg_hbm, freqs_hbm, tw_hbm, mod_hbm, vpart,
    resid_out, mod_out,
    vid, normed, ctxv, ctxg, qwg, kvw, cks, ckr, cvs, cvr, kall, vall, spread, owg, attg,
    queries, qsq, ksq, stat, shsc, tw, qg, kg, freqs, mod, acc, valid, when,
    loc_sem, send_sem, pass_s, ctx_r, ctz_r, qw_r, qc_r, og_r, oc_r, at_r, st_r, one_r,
):
    s = lax.axis_index("seq")
    z = lax.axis_index("head")
    core = s % 2
    chip = s // 2
    n_chip = n_seq // 2
    ratio = n_seq // n_head
    chunks = len(cuts)
    tok, width = vid.shape
    depth = qw.shape[0]
    att = qw.shape[1]
    text = ctx.shape[0]
    pair = 2 * depth
    masks = by_hops(n_seq)
    chip_bits = [k for k in masks if len(bits_of(k)) == 1]
    far = [k for k in masks if k not in chip_bits]
    (S_CTX, S_CTZ, S_W, S_SP, S_QW, S_CK, S_CV, S_KSQ, S_QSQ, S_V, S_K, S_OZ, S_OG, S_ST) = range(14)
    (R_W, R_SP, R_CK, R_CV, R_KSQ, R_QSQ, R_V, R_VC, R_K, R_KC, R_OZ) = range(11)

    def to_seq(k):
        return (flip(s, k), z)

    def to_head(k):
        return (s, flip(z, k))

    def remote(src, dst, ssem, rsem, dev):
        return pltpu.make_async_remote_copy(
            src_ref=src, dst_ref=dst, send_sem=ssem, recv_sem=rsem,
            device_id=dev, device_id_type=MESH_ID,
        )

    def push(src, dst, group, rsem, dev):
        remote(src, dst, send_sem.at[group], rsem, dev).start()

    def arrived(ref, sem):
        remote(ref, ref, sem, sem, to_seq(1)).wait_recv()

    def left(ref, sem):
        remote(ref, ref, sem, sem, to_seq(1)).wait_send()

    def gather_own(slot, half, bits, group, rsem):
        for b in bits:
            push(slot(half, s), slot(half, s), group, rsem.at[half, b // 2], to_seq(b))

    def gather_core(slot, group, csem):
        for half in range(2):
            push(slot(half, s), slot(half, s), group, csem.at[0], to_seq(1))

    def gather_relay(slot, half, k, group, rsem, csem):
        here = slot(half, flip(s, k))
        arrived(here, rsem.at[half, k // 2])
        for b in chip_bits:
            if not k & b and last_bit(half, k | b) == b:
                push(here, here, group, rsem.at[half, (k | b) // 2], to_seq(b))
        push(here, here, group, csem.at[k // 2], to_seq(1))

    barrier = pltpu.get_barrier_semaphore()
    for k in range(1, n_seq):
        pl.semaphore_signal(barrier, inc=1, device_id=to_seq(k), device_id_type=MESH_ID)
    for k in range(1, n_head):
        pl.semaphore_signal(barrier, inc=1, device_id=to_head(k), device_id_type=MESH_ID)

    def shard_rows(p, count=1):
        return qwg.at[pl.ds(pl.multiple_of(p * depth, depth), count * depth), :]

    def half_rows(half, p):
        rows = depth // 2
        return qwg.at[pl.ds(pl.multiple_of(p * depth + half * rows, rows), rows), :]

    def load(src, dst, i):
        copy = pltpu.make_async_copy(src, dst, loc_sem.at[i])
        copy.start()
        return copy

    piece = ow.shape[0] // n_seq

    def ow_piece(p):
        return pl.ds(pl.multiple_of(p * piece, piece), piece)

    own_ctx = load(ctx, ctxv, 0)
    own_qw = load(qw, shard_rows(s), 1)
    own_kw = load(kw, kvw.at[core, :, :att], 2)
    own_vw = load(vw, kvw.at[core, :, att:], 3)
    own_vid = load(video, vid, 4)
    own_spread = load(ow.at[ow_piece(s), :], spread.at[s], 5)
    own_tw = load(tw_hbm, tw, 6)
    small = [
        load(a, b, 8 + i)
        for i, (a, b) in enumerate(
            (
                (qg_hbm, qg), (kg_hbm, kg), (freqs_hbm, freqs), (mod_hbm, mod),
                (valid_hbm, valid), (when_hbm, when),
            )
        )
    ]
    with jax.named_scope("barrier"):
        pl.semaphore_wait(barrier, n_seq + n_head - 2)

    def ctx_cols(p):
        return pl.ds(pl.multiple_of(p * pair, pair), pair)

    part = text // 2

    def ctx_rows(q):
        return pl.ds(pl.multiple_of(q * part, part), part)

    mine = z % 2
    own_ctx.wait()
    for k in masks:
        push(
            ctxv.at[ctx_rows(mine), ctx_cols(flip(chip, k // 2))], ctxg.at[k // 2, ctx_rows(mine)],
            S_CTX, ctx_r.at[k // 2], to_seq(k),
        )
    own_kw.wait()
    own_vw.wait()
    push(kvw.at[core], kvw.at[core], S_W, one_r.at[R_W], to_seq(1))
    for k in masks + [k + 1 for k in masks] + [1]:
        push(ow.at[ow_piece(flip(s, k)), :], spread.at[s], S_SP, one_r.at[R_SP], to_seq(k))
    own_qw.wait()
    first = [(0, b) for b in chip_bits[:1]] + [(1, b) for b in chip_bits[1:]]
    second = [(0, b) for b in chip_bits[1:]] + [(1, b) for b in chip_bits[:1]]
    for half, b in first + second:
        gather_own(half_rows, half, [b], S_QW, qw_r)
    gather_core(half_rows, S_QW, qc_r)

    own_vid.wait()
    strip = 16
    strips = tok // strip

    def norm(begin, end):
        with jax.named_scope("norm"):
            @pl.loop(begin, end)
            def _(i):
                at = pl.ds(pl.multiple_of(i * strip, strip), strip)
                rows = vid[at, :].astype(F32)
                mean = jnp.mean(rows, axis=-1, keepdims=True)
                centred = rows - mean
                spread_ = jnp.mean(centred * centred, axis=-1, keepdims=True)
                normed[at, :] = (centred * (1.0 / jnp.sqrt(spread_ + 1e-06))).astype(BF16)

    def share(ks):
        with jax.named_scope("share%d" % len(ks)):
            for k in ks:
                here = ctxg.at[k // 2, ctx_rows(mine)]
                arrived(here, ctx_r.at[k // 2])
                push(here, here, S_CTZ, ctz_r.at[k // 2], to_head(1))

    done = [strips * n // 16 for n in NORM_AT]
    norm(0, done[0])
    share(chip_bits)
    norm(done[0], done[1])
    share(far)
    norm(done[1], strips)

    with jax.named_scope("kv"):
        arrived(kvw.at[1 - core], one_r.at[R_W])

        def partial_kv(source):
            return jnp.dot(source, kvw[...].reshape(pair, 2 * att), preferred_element_type=F32)

        block = partial_kv(ctxv[:, ctx_cols(chip)])
        cks[0] = block[:, :att]
        ckr[0] = block[:, att:]
        for k in masks:
            c = k // 2
            arrived(ctxg.at[c, ctx_rows(1 - mine)], ctz_r.at[c])
            block = partial_kv(ctxg[c])
            cks[c] = block[:, :att]
            cvs[c] = block[:, att:].astype(BF16)
            push(cks.at[c], ckr.at[c], S_CK, one_r.at[R_CK], to_seq(k))

    def shard_queries(p, rows):
        lanes = pl.ds(pl.multiple_of(p * rows, rows), rows)
        return jnp.dot(normed[:, lanes], qwg[lanes, :], preferred_element_type=F32)

    def chip_queries(p):
        return shard_queries(p, pair)

    with jax.named_scope("relay1"):
        for half, b in first:
            gather_relay(half_rows, half, b, S_QW, qw_r, qc_r)
        for k in masks:
            c = k // 2
            push(cvs.at[c], cvr.at[c], S_CV, one_r.at[R_CV], to_seq(k))

    def own_cols(zz):
        return pl.ds(zz * ratio, ratio)

    def ow_slot_z(p):
        return owg.at[:, p, ow_piece(s), :]

    with jax.named_scope("spread"):
        own_spread.wait()
        arrived(spread.at[pl.ds(0, n_seq - 1)], one_r.at[R_SP])
        own_ow = load(spread.at[own_cols(z)], ow_slot_z(z), 7)
        for k in range(1, n_head):
            push(spread.at[own_cols(flip(z, k))], ow_slot_z(z), S_OZ, one_r.at[R_OZ], to_head(k))

    with jax.named_scope("relay2"):
        for half, b in second:
            gather_relay(half_rows, half, b, S_QW, qw_r, qc_r)
        arrived(shard_rows(flip(s, 1)), qc_r.at[0])
    with jax.named_scope("q_own"):
        queries[...] = chip_queries(chip)
    with jax.named_scope("shsc"):
        own_tw.wait()
        for copy in small:
            copy.wait()
        angles = jnp.broadcast_to(when[...].astype(F32) * freqs[...], (16, freqs.shape[1]))
        embedding = jnp.concatenate([jnp.cos(angles), jnp.sin(angles)], axis=1)
        act = (embedding / (1.0 + jnp.exp(-embedding))).astype(BF16)
        for i in range(2):
            shsc[i] = mod[i : i + 1, :] + jnp.dot(act, tw[i], preferred_element_type=F32)[:8]

    with jax.named_scope("kv_sum"):
        arrived(ckr.at[pl.ds(1, n_chip - 1)], one_r.at[R_CK])
        key_rows = cks[0]
        for c in range(1, n_chip):
            key_rows = key_rows + ckr[c]
        cks[0] = key_rows
        ksq[0] = column_to_row(jnp.sum(key_rows * key_rows, axis=1, keepdims=True))
        for k in range(1, n_head):
            push(ksq.at[0], ksq.at[k], S_KSQ, one_r.at[R_KSQ], to_head(k))

    with jax.named_scope("q_mid"):
        for b in chip_bits:
            arrived(shard_rows(flip(s, b + 1)), qc_r.at[b // 2])
            queries[...] += chip_queries(flip(chip, b // 2))

    with jax.named_scope("far_relay"):
        for k in far:
            for half in range(2):
                gather_relay(half_rows, half, k, S_QW, qw_r, qc_r)

    with jax.named_scope("k_norm"):
        arrived(ksq.at[pl.ds(1, n_head - 1)], one_r.at[R_KSQ])
        k_mean = row_to_column(jnp.sum(ksq[...], axis=0), text) / (att * n_head)
        kall[s] = (cks[0] / jnp.sqrt(k_mean + 1e-06) * kg[...]).astype(BF16)
        for k in masks:
            push(kall.at[s], kall.at[s], S_K, one_r.at[R_K], to_seq(k))
        push(kall.at[s], kall.at[s], S_K, one_r.at[R_KC], to_seq(1))

    with jax.named_scope("v_sum"):
        arrived(cvr.at[pl.ds(1, n_chip - 1)], one_r.at[R_CV])
        value_rows = ckr[0]
        for c in range(1, n_chip):
            value_rows = value_rows + cvr[c].astype(F32)
        vall[s] = value_rows.astype(BF16)
        for k in masks:
            push(vall.at[s], vall.at[s], S_V, one_r.at[R_V], to_seq(k))
        push(vall.at[s], vall.at[s], S_V, one_r.at[R_VC], to_seq(1))

    def ow_half(half, p):
        if ratio == 1:
            rows = piece // 2
            return owg.at[:, :, pl.ds(pl.multiple_of(p * piece + half * rows, rows), rows), :]
        cut = ratio // 2
        return owg.at[pl.ds(half * cut, cut), :, ow_piece(p), :]

    def ow_slot(p):
        return owg.at[:, :, ow_piece(p), :]

    with jax.named_scope("q_far"):
        for k in far:
            if depth % LANES == 0:
                queries[...] += shard_queries(flip(s, k), depth)
            arrived(shard_rows(flip(s, k + 1)), qc_r.at[k // 2])
            if depth % LANES == 0:
                queries[...] += shard_queries(flip(s, k + 1), depth)
            else:
                queries[...] += chip_queries(flip(chip, k // 2))
        q = queries[...]
        qsq[0] = column_to_row(jnp.sum(q * q, axis=1, keepdims=True))
        for k in range(1, n_head):
            push(qsq.at[0], qsq.at[k], S_QSQ, one_r.at[R_QSQ], to_head(k))

    with jax.named_scope("kv_in"):
        for ref, group, chips in ((kall, S_K, R_K), (vall, S_V, R_V)):
            arrived(ref.at[pl.ds(0, n_chip - 1)], one_r.at[chips])
            for k in masks:
                here = ref.at[flip(s, k)]
                push(here, here, group, one_r.at[chips + 1], to_seq(1))
    with jax.named_scope("ow_start"):
        own_ow.wait()
        arrived(owg.at[:, pl.ds(0, n_head - 1), ow_piece(s), :], one_r.at[R_OZ])
        for half, b in first + second:
            gather_own(ow_half, half, [b], S_OG, og_r)
        gather_core(ow_half, S_OG, oc_r)
    with jax.named_scope("kv_end"):
        for ref, chips in ((vall, R_V), (kall, R_K)):
            arrived(ref.at[pl.ds(0, n_chip)], one_r.at[chips + 1])

    with jax.named_scope("q_norm"):
        arrived(qsq.at[pl.ds(1, n_head - 1)], one_r.at[R_QSQ])
        q_mean = row_to_column(jnp.sum(qsq[...], axis=0), tok) / (att * n_head)
        q_root = jnp.sqrt(q_mean + 1e-06)

    def held(way, d):
        return d % n_head if way > 0 else (n_head - d) % n_head

    def onward(way, d):
        origin = z - way * (d - 1)
        return (origin >= 0) & (origin < n_head) & (z + way >= 0) & (z + way < n_head)

    def passed(way, d):
        return pass_s.at[0 if way > 0 else 1, d - 1]

    def reach(way, c, d):
        slot = held(way, d)

        @pl.when(onward(way, d))
        def _():
            remote(
                attg.at[held(way, d - 1), cuts[c]], attg.at[slot, cuts[c]],
                passed(way, d), at_r.at[c, slot - 1], (s, z + way),
            ).start()

    def take(way, c, d):
        slot = held(way, d)
        origin = z - way * d

        @pl.when((origin >= 0) & (origin < n_head))
        def _():
            arrived(attg.at[slot, cuts[c]], at_r.at[c, slot - 1])

    def ow_relays(pairs):
        for half, b in pairs:
            gather_relay(ow_half, half, b, S_OG, og_r, oc_r)

    all_text = n_seq * text
    with jax.named_scope("attend"):
        every_k = kall[...].reshape(all_text, att)
        every_v = vall[...].reshape(all_text, att)
        seen = lax.broadcasted_iota(jnp.int32, (1, all_text), 1) < valid[...]
        for c in range(chunks):
            at = cuts[c]
            q_normed = (queries[at, :] / q_root[at] * qg[...]).astype(BF16)
            for h in range(att // HD):
                lanes = slice(h * HD, (h + 1) * HD)
                scores = lax.dot_general(
                    q_normed[:, lanes], every_k[:, lanes], (((1,), (1,)), ((), ())),
                    preferred_element_type=F32,
                ) * HD ** (-0.5)
                scores = jnp.where(seen, scores, F32(-1e30))
                shifted = jnp.exp(scores - jnp.max(scores, axis=-1, keepdims=True))
                weights = (shifted * (1.0 / jnp.sum(shifted, axis=-1, keepdims=True))).astype(BF16)
                attg[0, at, lanes] = jnp.dot(
                    weights, every_v[:, lanes], preferred_element_type=F32
                ).astype(BF16)
            for way in (1, -1):
                reach(way, c, 1)
            if c == OW_FIRST:
                ow_relays(first)

    cols = owg.shape[3]
    part_width = mod_out.shape[1]
    last = z + 1 - (2 * z) // n_head

    def projection(at, j, slot):
        return jnp.dot(
            attg[slot, at], owg[j, lax.rem(z + n_head - slot, n_head)], preferred_element_type=F32
        )

    def accumulate(c):
        at = cuts[c]
        with jax.named_scope(f"accumulate{c}"):
            for j in range(ratio):
                here = slice(j * cols, (j + 1) * cols)
                if vpart is None:
                    base = vid[at, pl.ds(pl.multiple_of(z * part_width + j * cols, LANES), cols)]
                else:
                    base = vpart[at, here]
                projected = projection(at, j, 0)
                for i in range(1, n_head - 1):
                    projected = projected + projection(at, j, lax.rem(last - 1 + i, n_head - 1) + 1)
                acc[at, here] = base.astype(F32) + projected

    for d in range(1, n_head - 1):
        for c in range(chunks):
            with jax.named_scope(f"pass{d}_{c}"):
                for way in (1, -1):
                    take(way, c, d)
                    reach(way, c, d + 1)
            if d == 1 and c == 1:
                with jax.named_scope("ow2"):
                    ow_relays(second)
            if d == n_head - 2 and c == 0:
                with jax.named_scope("ow3"):
                    for k in far:
                        for half in range(2):
                            gather_relay(ow_half, half, k, S_OG, og_r, oc_r)
            if d == n_head - 2 and c == 1:
                with jax.named_scope("ow4"):
                    for k in [0] + masks:
                        arrived(ow_slot(flip(s, k + 1)), oc_r.at[k // 2])
            if d == n_head - 2 and c >= 1:
                accumulate(c - 1)
    accumulate(chunks - 1)
    with jax.named_scope("left1"):
        few = pl.ds(0, n_chip - 1)
        left(ctxg.at[few, ctx_rows(0)], send_sem.at[S_CTX])
        left(ctxg.at[few, ctx_rows(0)], send_sem.at[S_CTZ])
        left(kvw.at[0], send_sem.at[S_W])
        left(spread.at[pl.ds(0, n_seq - 1)], send_sem.at[S_SP])
        left(shard_rows(0, n_seq - 1), send_sem.at[S_QW])
        left(ckr.at[few], send_sem.at[S_CK])
        left(cvr.at[few], send_sem.at[S_CV])
        left(ksq.at[pl.ds(0, n_head - 1)], send_sem.at[S_KSQ])
        left(qsq.at[pl.ds(0, n_head - 1)], send_sem.at[S_QSQ])
        left(vall.at[pl.ds(0, n_seq - 1)], send_sem.at[S_V])
        left(kall.at[pl.ds(0, n_seq - 1)], send_sem.at[S_K])
        left(owg.at[:, pl.ds(0, n_head - 1), ow_piece(0), :], send_sem.at[S_OZ])
    def modulate(c):
        at = cuts[c]
        step = at.stop - at.start
        with jax.named_scope(f"stat{c}"):
            arrived(stat.at[c, pl.ds(1, n_head - 1)], st_r.at[c])
        with jax.named_scope(f"modulate{c}"):
            both = jnp.sum(stat[c], axis=0) / (part_width * n_head)
            mean2 = both[:1]
            inverse = 1.0 / jnp.sqrt(both[1:] - mean2 * mean2 + 1e-06)
            mean_col = row_to_column(mean2, step)
            inv_col = row_to_column(inverse, step)
            wide = resid_out[at, :].astype(F32)
            mod_out[at, :] = (
                (wide - mean_col) * inv_col * (1.0 + shsc[1, :1, :]) + shsc[0, :1, :]
            ).astype(BF16)

    for c in range(chunks):
        at = cuts[c]
        step = at.stop - at.start
        with jax.named_scope(f"last{c}"):
            for way in (1, -1):
                take(way, c, n_head - 1)
        with jax.named_scope(f"project{c}"):
            row_sum = jnp.zeros((step, 1), F32)
            row_sq = jnp.zeros((step, 1), F32)
            for j in range(ratio):
                here = slice(j * cols, (j + 1) * cols)
                rounded = (acc[at, here] + projection(at, j, last)).astype(BF16)
                resid_out[at, here] = rounded
                wide = rounded.astype(F32)
                row_sum = row_sum + jnp.sum(wide, axis=1, keepdims=True)
                row_sq = row_sq + jnp.sum(wide * wide, axis=1, keepdims=True)
            stat[c, 0, :1] = column_to_row(row_sum)
            stat[c, 0, 1:] = column_to_row(row_sq)
            for k in range(1, n_head):
                push(stat.at[c, 0], stat.at[c, k], S_ST, st_r.at[c], to_head(k))
        if c >= 3:
            modulate(c - 3)
    with jax.named_scope("left2"):
        left(owg.at[:, :, pl.ds(0, piece * (n_seq - 1)), :], send_sem.at[S_OG])
        for way in (1, -1):
            for d in range(1, n_head):
                @pl.when(onward(way, d))
                def _():
                    left(attg.at[0], passed(way, d))
    for c in range(max(chunks - 3, 0), chunks):
        modulate(c)
    left(stat.at[:, pl.ds(0, n_head - 1)], send_sem.at[S_ST])


def put_out(resid, mod, resid_hbm, mod_hbm, sems):
    pieces = sems.shape[1]
    rows = resid.shape[0] // pieces
    copies = [
        pltpu.make_async_copy(src.at[at], dst.at[at], sems.at[i, p])
        for p, at in enumerate(pl.ds(p * rows, rows) for p in range(pieces))
        for i, (src, dst) in enumerate(((resid, resid_hbm), (mod, mod_hbm)))
    ]
    for copy in copies:
        copy.start()
    for copy in copies:
        copy.wait()


def on_device(
    n_seq,
    n_head,
    video_rows,
    context,
    valid_length,
    timestep,
    query_weight,
    key_weight,
    value_weight,
    out_weight,
    query_gain,
    key_gain,
    time_weight,
    modulation,
):
    tok, width = video_rows.shape
    text = context.shape[0]
    depth, att = query_weight.shape
    cols = out_weight.shape[1]
    part_width = modulation.shape[1]
    ratio = n_seq // n_head
    n_chip = n_seq // 2
    quarter = tok // 4
    sizes = [quarter // 2] + [quarter] * 3 + [quarter // 2]
    cuts = [slice(sum(sizes[:c]), sum(sizes[: c + 1])) for c in range(len(sizes))]
    chunks = len(cuts)
    piece = out_weight.shape[0] // n_seq
    half = FREQ // 2
    freqs = np.exp(-np.log(10000.0) * np.arange(half) / half).astype(np.float32)[None, :]
    sliced = part_width % LANES != 0 or cols % LANES != 0
    extra = []
    if sliced:
        extra.append(
            lax.dynamic_slice_in_dim(
                video_rows, lax.axis_index("head") * part_width, part_width, 1
            )
        )
    out_bytes = tok * -(-part_width // LANES) * LANES * 2
    vmem = pl.BlockSpec(memory_space=pltpu.VMEM)
    hbm = pl.BlockSpec(memory_space=pltpu.HBM)
    dma = pltpu.SemaphoreType.DMA
    results = pl.pallas_call(
        functools.partial(body, n_seq, n_head, cuts, sliced),
        out_shape=[pltpu.VMEM((tok, part_width), BF16)] * 2,
        in_specs=[hbm] * 13 + [vmem] * len(extra),
        out_specs=[vmem] * 2,
        scratch_shapes=[
            pltpu.VMEM((tok, width), BF16),
            pltpu.VMEM((tok, width), BF16),
            pltpu.VMEM((text, width), BF16),
            pltpu.VMEM((n_chip, text, 2 * depth), BF16),
            pltpu.VMEM((n_seq * depth, att), BF16),
            pltpu.VMEM((2, depth, 2 * att), BF16),
            pltpu.VMEM((n_chip, text, att), F32),
            pltpu.VMEM((n_chip, text, att), F32),
            pltpu.VMEM((n_chip, text, att), BF16),
            pltpu.VMEM((n_chip, text, att), BF16),
            pltpu.VMEM((n_seq, text, att), BF16),
            pltpu.VMEM((n_seq, text, att), BF16),
            pltpu.VMEM((n_seq, piece, cols), BF16),
            pltpu.VMEM((ratio, n_head, out_weight.shape[0], cols), BF16),
            pltpu.VMEM((n_head, tok, att), BF16),
            pltpu.VMEM((tok, att), F32),
            pltpu.VMEM((n_head, 1, tok), F32),
            pltpu.VMEM((n_head, 1, -(-text // LANES) * LANES), F32),
            pltpu.VMEM((chunks, n_head, 2, -(-max(sizes) // LANES) * LANES), F32),
            pltpu.VMEM((2, 8, part_width), F32),
            pltpu.VMEM(time_weight.shape, BF16),
            pltpu.VMEM((1, att), F32),
            pltpu.VMEM((1, att), F32),
            pltpu.VMEM((1, half), F32),
            pltpu.VMEM(modulation.shape, F32),
            pltpu.VMEM((tok, part_width), F32),
            pltpu.VMEM((1, 1), jnp.int32),
            pltpu.VMEM((1, 1), jnp.int32),
            dma((14,)),
            dma((14,)),
            dma((2, n_head - 1)),
            *[dma((n_chip,))] * 2,
            *[dma((2, n_chip)), dma((n_chip,))] * 2,
            dma((chunks, n_head - 1)),
            dma((chunks,)),
            dma((11,)),
        ],
        compiler_params=pltpu.CompilerParams(
            collective_id=0, has_side_effects=True, vmem_limit_bytes=VMEM_MOST - 2 * out_bytes
        ),
    )(
        valid_length[None, :],
        timestep[None, :],
        video_rows,
        context,
        query_weight,
        key_weight,
        value_weight,
        out_weight,
        query_gain[None, :],
        key_gain[None, :],
        freqs,
        time_weight,
        modulation,
        *extra,
    )
    return pl.pallas_call(
        put_out,
        out_shape=[jax.ShapeDtypeStruct((tok, part_width), BF16)] * 2,
        in_specs=[vmem] * 2,
        out_specs=[hbm] * 2,
        scratch_shapes=[dma((2, 4))],
        compiler_params=pltpu.CompilerParams(vmem_limit_bytes=4 * 1024 * 1024),
    )(*results)


def solution(mesh):
    in_specs = (
        P("seq", None),
        P("seq", None),
        P(),
        P(),
        P("seq", "head"),
        P("seq", "head"),
        P("seq", "head"),
        P("head", "seq"),
        P("head"),
        P("head"),
        P(None, None, "head"),
        P(None, "head"),
    )
    out_specs = (P("seq", "head"), P("seq", "head"))
    return jax.shard_map(
        functools.partial(on_device, mesh.shape["seq"], mesh.shape["head"]),
        mesh=mesh, in_specs=in_specs, out_specs=out_specs, check_vma=False,
    )
```

```python
import functools

import jax
import jax.numpy as jnp
import numpy as np
from jax import lax
from jax.experimental import pallas as pl
from jax.experimental.pallas import tpu as pltpu
from jax.sharding import PartitionSpec as P

HD = 128
FREQ = 256
LANES = 128
VMEM_MOST = 67_000_000
NORM_AT = (5, 8)
F32 = jnp.float32
BF16 = jnp.bfloat16
MESH_ID = pl.DeviceIdType.MESH


def flip(index, mask):
    bit = 1
    while bit <= mask:
        if mask & bit:
            index = index + bit - 2 * bit * ((index // bit) % 2)
        bit *= 2
    return index


def bits_of(mask):
    return [1 << b for b in range(mask.bit_length()) if mask >> b & 1]


def last_bit(half, mask):
    return bits_of(mask)[-1] if half == 0 else bits_of(mask)[0]


def by_hops(n_seq):
    return sorted(range(2, n_seq, 2), key=lambda k: (len(bits_of(k)), k))


def column_to_row(column):
    tall = column.shape[0]
    wide = -(-tall // LANES) * LANES
    if wide > tall:
        column = jnp.concatenate([column, jnp.zeros((wide - tall, 1), F32)], axis=0)
    return jnp.transpose(jnp.broadcast_to(column, (wide, LANES)))[:1]


def row_to_column(row, tall):
    return jnp.transpose(jnp.broadcast_to(row, (LANES, row.shape[1])))[:tall, :1]


def body(n_seq, n_head, cuts, sliced, *refs):
    if sliced:
        steps(n_seq, n_head, cuts, *refs)
    else:
        steps(n_seq, n_head, cuts, *refs[:13], None, *refs[13:])


def steps(
    n_seq, n_head, cuts,
    valid_hbm, when_hbm, video, ctx, qw, kw, vw, ow, qg_hbm, kg_hbm, freqs_hbm, tw_hbm, mod_hbm, vpart,
    resid_out, mod_out,
    vid, normed, ctxv, ctxg, qwg, kvw, cks, ckr, cvs, cvr, own_v, key_sum, kall, vall, spread, owg, attg,
    queries, qsq, ksq, stat, shsc, tw, qg, kg, freqs, mod, acc, valid, when,
    loc_sem, send_sem, pass_s, ctx_r, ctz_r, qw_r, qc_r, og_r, oc_r, at_r, st_r, one_r,
):
    s = lax.axis_index("seq")
    z = lax.axis_index("head")
    core = s % 2
    chip = s // 2
    n_chip = n_seq // 2
    ratio = n_seq // n_head
    chunks = len(cuts)
    tok, width = vid.shape
    depth = qw.shape[0]
    att = qw.shape[1]
    text = ctx.shape[0]
    pair = 2 * depth
    masks = by_hops(n_seq)
    chip_bits = [k for k in masks if len(bits_of(k)) == 1]
    far = [k for k in masks if k not in chip_bits]
    (S_CTX, S_CTZ, S_W, S_SP, S_QW, S_CK, S_CV, S_KSQ, S_QSQ, S_V, S_K, S_OZ, S_OG, S_ST) = range(14)
    (R_W, R_SP, R_CK, R_CV, R_KSQ, R_QSQ, R_V, R_VC, R_K, R_KC, R_OZ) = range(11)

    def to_seq(k):
        return (flip(s, k), z)

    def to_head(k):
        return (s, flip(z, k))

    def remote(src, dst, ssem, rsem, dev):
        return pltpu.make_async_remote_copy(
            src_ref=src, dst_ref=dst, send_sem=ssem, recv_sem=rsem,
            device_id=dev, device_id_type=MESH_ID,
        )

    def push(src, dst, group, rsem, dev):
        remote(src, dst, send_sem.at[group], rsem, dev).start()

    def arrived(ref, sem):
        remote(ref, ref, sem, sem, to_seq(1)).wait_recv()

    def left(ref, sem):
        remote(ref, ref, sem, sem, to_seq(1)).wait_send()

    def gather_own(slot, half, bits, group, rsem):
        for b in bits:
            push(slot(half, s), slot(half, s), group, rsem.at[half, b // 2], to_seq(b))

    def gather_core(slot, group, csem):
        for half in range(2):
            push(slot(half, s), slot(half, s), group, csem.at[0], to_seq(1))

    def gather_relay(slot, half, k, group, rsem, csem):
        here = slot(half, flip(s, k))
        arrived(here, rsem.at[half, k // 2])
        for b in chip_bits:
            if not k & b and last_bit(half, k | b) == b:
                push(here, here, group, rsem.at[half, (k | b) // 2], to_seq(b))
        push(here, here, group, csem.at[k // 2], to_seq(1))

    barrier = pltpu.get_barrier_semaphore()
    for k in range(1, n_seq):
        pl.semaphore_signal(barrier, inc=1, device_id=to_seq(k), device_id_type=MESH_ID)
    for k in range(1, n_head):
        pl.semaphore_signal(barrier, inc=1, device_id=to_head(k), device_id_type=MESH_ID)

    def shard_rows(p, count=1):
        return qwg.at[pl.ds(pl.multiple_of(p * depth, depth), count * depth), :]

    def half_rows(half, p):
        rows = depth // 2
        return qwg.at[pl.ds(pl.multiple_of(p * depth + half * rows, rows), rows), :]

    def load(src, dst, i):
        copy = pltpu.make_async_copy(src, dst, loc_sem.at[i])
        copy.start()
        return copy

    piece = ow.shape[0] // n_seq

    def ow_piece(p):
        return pl.ds(pl.multiple_of(p * piece, piece), piece)

    own_ctx = load(ctx, ctxv, 0)
    own_qw = load(qw, shard_rows(s), 1)
    own_kw = load(kw, kvw.at[core, :, :att], 2)
    own_vw = load(vw, kvw.at[core, :, att:], 3)
    own_vid = load(video, vid, 4)
    own_spread = load(ow.at[ow_piece(s), :], spread.at[s], 5)
    own_tw = load(tw_hbm, tw, 6)
    small = [
        load(a, b, 8 + i)
        for i, (a, b) in enumerate(
            (
                (qg_hbm, qg), (kg_hbm, kg), (freqs_hbm, freqs), (mod_hbm, mod),
                (valid_hbm, valid), (when_hbm, when),
            )
        )
    ]
    with jax.named_scope("barrier"):
        pl.semaphore_wait(barrier, n_seq + n_head - 2)

    def ctx_cols(p):
        return pl.ds(pl.multiple_of(p * pair, pair), pair)

    part = text // 2

    def ctx_rows(q):
        return pl.ds(pl.multiple_of(q * part, part), part)

    mine = z % 2
    own_ctx.wait()
    for k in masks:
        push(
            ctxv.at[ctx_rows(mine), ctx_cols(flip(chip, k // 2))], ctxg.at[k // 2, ctx_rows(mine)],
            S_CTX, ctx_r.at[k // 2], to_seq(k),
        )
    own_kw.wait()
    own_vw.wait()
    push(kvw.at[core], kvw.at[core], S_W, one_r.at[R_W], to_seq(1))
    for k in masks + [k + 1 for k in masks] + [1]:
        push(ow.at[ow_piece(flip(s, k)), :], spread.at[s], S_SP, one_r.at[R_SP], to_seq(k))
    own_qw.wait()
    first = [(0, b) for b in chip_bits[:1]] + [(1, b) for b in chip_bits[1:]]
    second = [(0, b) for b in chip_bits[1:]] + [(1, b) for b in chip_bits[:1]]
    for half, b in first + second:
        gather_own(half_rows, half, [b], S_QW, qw_r)
    gather_core(half_rows, S_QW, qc_r)

    own_vid.wait()
    strip = 16
    strips = tok // strip

    def norm(begin, end):
        with jax.named_scope("norm"):
            @pl.loop(begin, end)
            def _(i):
                at = pl.ds(pl.multiple_of(i * strip, strip), strip)
                rows = vid[at, :].astype(F32)
                mean = jnp.mean(rows, axis=-1, keepdims=True)
                centred = rows - mean
                spread_ = jnp.mean(centred * centred, axis=-1, keepdims=True)
                normed[at, :] = (centred * (1.0 / jnp.sqrt(spread_ + 1e-06))).astype(BF16)

    def share(ks):
        with jax.named_scope("share%d" % len(ks)):
            for k in ks:
                here = ctxg.at[k // 2, ctx_rows(mine)]
                arrived(here, ctx_r.at[k // 2])
                push(here, here, S_CTZ, ctz_r.at[k // 2], to_head(1))

    done = [strips * n // 16 for n in NORM_AT]
    norm(0, done[0])
    share(chip_bits)
    norm(done[0], done[1])
    share(far)
    norm(done[1], strips)

    def keeper(k):
        return (flip(s, k) // 2 * 2 + 1, z)

    def chip_slot(ref, p):
        return ref.at[pl.ds(2 * p, 2)]

    def spread_text(ref, group, chips):
        here = chip_slot(ref, chip)
        for k in masks:
            push(here, here, group, one_r.at[chips], to_seq(k))
        push(here, here, group, one_r.at[chips + 1], to_seq(1))

    with jax.named_scope("kv"):
        arrived(kvw.at[1 - core], one_r.at[R_W])

        def partial_kv(source):
            return jnp.dot(source, kvw[...].reshape(pair, 2 * att), preferred_element_type=F32)

        block = partial_kv(ctxv[:, ctx_cols(chip)])
        cks[0] = block[:, :att]
        own_v[...] = block[:, att:]
        cvs[0] = block[:, att:].astype(BF16)
        for k in masks:
            c = k // 2
            arrived(ctxg.at[c, ctx_rows(1 - mine)], ctz_r.at[c])
            block = partial_kv(ctxg[c])
            cks[c] = block[:, :att]
            cvs[c] = block[:, att:].astype(BF16)
            push(cks.at[c], ckr.at[core * n_chip + c], S_CK, one_r.at[R_CK], keeper(k))

        @pl.when(core == 0)
        def _():
            push(cks.at[0], ckr.at[0], S_CK, one_r.at[R_CK], to_seq(1))

    def shard_queries(p, rows):
        lanes = pl.ds(pl.multiple_of(p * rows, rows), rows)
        return jnp.dot(normed[:, lanes], qwg[lanes, :], preferred_element_type=F32)

    def chip_queries(p):
        return shard_queries(p, pair)

    with jax.named_scope("relay1"):
        for half, b in first:
            gather_relay(half_rows, half, b, S_QW, qw_r, qc_r)
        for k in masks:
            c = k // 2
            push(cvs.at[c], cvr.at[core * n_chip + c], S_CV, one_r.at[R_CV], keeper(k))

        @pl.when(core == 0)
        def _():
            push(cvs.at[0], cvr.at[0], S_CV, one_r.at[R_CV], to_seq(1))

    def own_cols(zz):
        return pl.ds(zz * ratio, ratio)

    def ow_slot_z(p):
        return owg.at[:, p, ow_piece(s), :]

    with jax.named_scope("spread"):
        own_spread.wait()
        arrived(spread.at[pl.ds(0, n_seq - 1)], one_r.at[R_SP])
        own_ow = load(spread.at[own_cols(z)], ow_slot_z(z), 7)
        for k in range(1, n_head):
            push(spread.at[own_cols(flip(z, k))], ow_slot_z(z), S_OZ, one_r.at[R_OZ], to_head(k))

    with jax.named_scope("relay2"):
        for half, b in second:
            gather_relay(half_rows, half, b, S_QW, qw_r, qc_r)
        arrived(shard_rows(flip(s, 1)), qc_r.at[0])
    with jax.named_scope("q_own"):
        queries[...] = chip_queries(chip)
    with jax.named_scope("shsc"):
        own_tw.wait()
        for copy in small:
            copy.wait()
        angles = jnp.broadcast_to(when[...].astype(F32) * freqs[...], (16, freqs.shape[1]))
        embedding = jnp.concatenate([jnp.cos(angles), jnp.sin(angles)], axis=1)
        act = (embedding / (1.0 + jnp.exp(-embedding))).astype(BF16)
        for i in range(2):
            shsc[i] = mod[i : i + 1, :] + jnp.dot(act, tw[i], preferred_element_type=F32)[:8]

    @pl.when(core == 1)
    def _():
        with jax.named_scope("kv_sum"):
            arrived(ckr.at[pl.ds(0, n_seq - 1)], one_r.at[R_CK])
            both = [ckr[0], cks[0]]
            for q in range(2):
                for c in range(1, n_chip):
                    both[q] = both[q] + ckr[q * n_chip + c]
            key_rows = jnp.concatenate(both, axis=0)
            key_sum[...] = key_rows
            ksq[0] = column_to_row(jnp.sum(key_rows * key_rows, axis=1, keepdims=True))
            for k in range(1, n_head):
                push(ksq.at[0], ksq.at[k], S_KSQ, one_r.at[R_KSQ], to_head(k))

    with jax.named_scope("q_mid"):
        for b in chip_bits:
            arrived(shard_rows(flip(s, b + 1)), qc_r.at[b // 2])
            queries[...] += chip_queries(flip(chip, b // 2))

    with jax.named_scope("far_relay"):
        for k in far:
            for half in range(2):
                gather_relay(half_rows, half, k, S_QW, qw_r, qc_r)

    @pl.when(core == 1)
    def _():
        with jax.named_scope("k_norm"):
            arrived(ksq.at[pl.ds(1, n_head - 1)], one_r.at[R_KSQ])
            k_mean = row_to_column(jnp.sum(ksq[...], axis=0), 2 * text) / (att * n_head)
            key_normed = (key_sum[...] / jnp.sqrt(k_mean + 1e-06) * kg[...]).astype(BF16)
            for q in range(2):
                kall[2 * chip + q] = key_normed[q * text : (q + 1) * text]
            spread_text(kall, S_K, R_K)
        with jax.named_scope("v_sum"):
            arrived(cvr.at[pl.ds(0, n_seq - 1)], one_r.at[R_CV])
            both = [cvr[0].astype(F32), own_v[...]]
            for q in range(2):
                for c in range(1, n_chip):
                    both[q] = both[q] + cvr[q * n_chip + c].astype(F32)
                vall[2 * chip + q] = both[q].astype(BF16)
            spread_text(vall, S_V, R_V)

    def ow_half(half, p):
        if ratio == 1:
            rows = piece // 2
            return owg.at[:, :, pl.ds(pl.multiple_of(p * piece + half * rows, rows), rows), :]
        cut = ratio // 2
        return owg.at[pl.ds(half * cut, cut), :, ow_piece(p), :]

    def ow_slot(p):
        return owg.at[:, :, ow_piece(p), :]

    with jax.named_scope("q_far"):
        for k in far:
            if depth % LANES == 0:
                queries[...] += shard_queries(flip(s, k), depth)
            arrived(shard_rows(flip(s, k + 1)), qc_r.at[k // 2])
            if depth % LANES == 0:
                queries[...] += shard_queries(flip(s, k + 1), depth)
            else:
                queries[...] += chip_queries(flip(chip, k // 2))
        q = queries[...]
        qsq[0] = column_to_row(jnp.sum(q * q, axis=1, keepdims=True))
        for k in range(1, n_head):
            push(qsq.at[0], qsq.at[k], S_QSQ, one_r.at[R_QSQ], to_head(k))

    @pl.when(core == 1)
    def _():
        with jax.named_scope("kv_in"):
            for ref, group, chips in ((kall, S_K, R_K), (vall, S_V, R_V)):
                arrived(ref.at[pl.ds(0, n_seq - 2)], one_r.at[chips])
                for k in masks:
                    here = chip_slot(ref, flip(chip, k // 2))
                    push(here, here, group, one_r.at[chips + 1], to_seq(1))

    @pl.when(core == 0)
    def _():
        with jax.named_scope("kv_end"):
            for ref, chips in ((kall, R_K), (vall, R_V)):
                arrived(ref, one_r.at[chips + 1])

    with jax.named_scope("ow_start"):
        own_ow.wait()
        arrived(owg.at[:, pl.ds(0, n_head - 1), ow_piece(s), :], one_r.at[R_OZ])
        for half, b in first + second:
            gather_own(ow_half, half, [b], S_OG, og_r)
        gather_core(ow_half, S_OG, oc_r)

    with jax.named_scope("q_norm"):
        arrived(qsq.at[pl.ds(1, n_head - 1)], one_r.at[R_QSQ])
        q_mean = row_to_column(jnp.sum(qsq[...], axis=0), tok) / (att * n_head)
        q_root = jnp.sqrt(q_mean + 1e-06)

    def held(way, d):
        return d % n_head if way > 0 else (n_head - d) % n_head

    def onward(way, d):
        origin = z - way * (d - 1)
        return (origin >= 0) & (origin < n_head) & (z + way >= 0) & (z + way < n_head)

    def passed(way, d):
        return pass_s.at[0 if way > 0 else 1, d - 1]

    def reach(way, c, d):
        slot = held(way, d)

        @pl.when(onward(way, d))
        def _():
            remote(
                attg.at[held(way, d - 1), cuts[c]], attg.at[slot, cuts[c]],
                passed(way, d), at_r.at[c, slot - 1], (s, z + way),
            ).start()

    def take(way, c, d):
        slot = held(way, d)
        origin = z - way * d

        @pl.when((origin >= 0) & (origin < n_head))
        def _():
            arrived(attg.at[slot, cuts[c]], at_r.at[c, slot - 1])

    def ow_relays(pairs):
        for half, b in pairs:
            gather_relay(ow_half, half, b, S_OG, og_r, oc_r)

    all_text = n_seq * text
    with jax.named_scope("attend"):
        every_k = kall[...].reshape(all_text, att)
        every_v = vall[...].reshape(all_text, att)
        seen = lax.broadcasted_iota(jnp.int32, (1, all_text), 1) < valid[...]
        for c in range(chunks):
            at = cuts[c]
            q_normed = (queries[at, :] / q_root[at] * qg[...]).astype(BF16)
            for h in range(att // HD):
                lanes = slice(h * HD, (h + 1) * HD)
                scores = lax.dot_general(
                    q_normed[:, lanes], every_k[:, lanes], (((1,), (1,)), ((), ())),
                    preferred_element_type=F32,
                ) * HD ** (-0.5)
                scores = jnp.where(seen, scores, F32(-1e30))
                shifted = jnp.exp(scores - jnp.max(scores, axis=-1, keepdims=True))
                weights = (shifted * (1.0 / jnp.sum(shifted, axis=-1, keepdims=True))).astype(BF16)
                attg[0, at, lanes] = jnp.dot(
                    weights, every_v[:, lanes], preferred_element_type=F32
                ).astype(BF16)
            for way in (1, -1):
                reach(way, c, 1)

    cols = owg.shape[3]
    part_width = mod_out.shape[1]
    last = z + 1 - (2 * z) // n_head

    def projection(at, j, slot):
        return jnp.dot(
            attg[slot, at], owg[j, lax.rem(z + n_head - slot, n_head)], preferred_element_type=F32
        )

    def accumulate(begin, end):
        at = slice(cuts[begin].start, cuts[end - 1].stop)
        with jax.named_scope(f"accumulate{begin}"):
            for j in range(ratio):
                here = slice(j * cols, (j + 1) * cols)
                if vpart is None:
                    base = vid[at, pl.ds(pl.multiple_of(z * part_width + j * cols, LANES), cols)]
                else:
                    base = vpart[at, here]
                projected = projection(at, j, 0)
                for i in range(1, n_head - 1):
                    projected = projected + projection(at, j, lax.rem(last - 1 + i, n_head - 1) + 1)
                acc[at, here] = base.astype(F32) + projected

    for d in range(1, n_head - 1):
        for c in range(chunks):
            with jax.named_scope(f"pass{d}_{c}"):
                for way in (1, -1):
                    take(way, c, d)
                    reach(way, c, d + 1)
            if d == 1 and c == 1:
                with jax.named_scope("ow1"):
                    ow_relays(first)
            if d == 1 and c == chunks - 1:
                with jax.named_scope("ow2"):
                    ow_relays(second)
            if d == n_head - 2 and c == 1:
                with jax.named_scope("ow3"):
                    for k in far:
                        for half in range(2):
                            gather_relay(ow_half, half, k, S_OG, og_r, oc_r)
            if d == n_head - 2 and c == 2:
                with jax.named_scope("ow4"):
                    for k in [0] + masks:
                        arrived(ow_slot(flip(s, k + 1)), oc_r.at[k // 2])
                accumulate(0, 3)
    accumulate(3, chunks)
    with jax.named_scope("left1"):
        few = pl.ds(0, n_chip - 1)
        left(ctxg.at[few, ctx_rows(0)], send_sem.at[S_CTX])
        left(ctxg.at[few, ctx_rows(0)], send_sem.at[S_CTZ])
        left(kvw.at[0], send_sem.at[S_W])
        left(spread.at[pl.ds(0, n_seq - 1)], send_sem.at[S_SP])
        left(shard_rows(0, n_seq - 1), send_sem.at[S_QW])
        left(qsq.at[pl.ds(0, n_head - 1)], send_sem.at[S_QSQ])
        left(owg.at[:, pl.ds(0, n_head - 1), ow_piece(0), :], send_sem.at[S_OZ])

        @pl.when(core == 0)
        def _():
            left(ckr.at[pl.ds(0, n_chip)], send_sem.at[S_CK])
            left(cvr.at[pl.ds(0, n_chip)], send_sem.at[S_CV])

        @pl.when(core == 1)
        def _():
            left(ckr.at[few], send_sem.at[S_CK])
            left(cvr.at[few], send_sem.at[S_CV])
            left(ksq.at[pl.ds(0, n_head - 1)], send_sem.at[S_KSQ])
            for group in (S_V, S_K):
                left(qwg.at[pl.ds(0, 2 * (n_seq - 1) * text)], send_sem.at[group])

    def modulate(c):
        at = cuts[c]
        step = at.stop - at.start
        with jax.named_scope(f"stat{c}"):
            arrived(stat.at[c, pl.ds(1, n_head - 1)], st_r.at[c])
        with jax.named_scope(f"modulate{c}"):
            both = jnp.sum(stat[c], axis=0) / (part_width * n_head)
            mean2 = both[:1]
            inverse = 1.0 / jnp.sqrt(both[1:] - mean2 * mean2 + 1e-06)
            mean_col = row_to_column(mean2, step)
            inv_col = row_to_column(inverse, step)
            wide = resid_out[at, :].astype(F32)
            mod_out[at, :] = (
                (wide - mean_col) * inv_col * (1.0 + shsc[1, :1, :]) + shsc[0, :1, :]
            ).astype(BF16)

    for c in range(chunks):
        at = cuts[c]
        step = at.stop - at.start
        with jax.named_scope(f"last{c}"):
            for way in (1, -1):
                take(way, c, n_head - 1)
        with jax.named_scope(f"project{c}"):
            row_sum = jnp.zeros((step, 1), F32)
            row_sq = jnp.zeros((step, 1), F32)
            for j in range(ratio):
                here = slice(j * cols, (j + 1) * cols)
                rounded = (acc[at, here] + projection(at, j, last)).astype(BF16)
                resid_out[at, here] = rounded
                wide = rounded.astype(F32)
                row_sum = row_sum + jnp.sum(wide, axis=1, keepdims=True)
                row_sq = row_sq + jnp.sum(wide * wide, axis=1, keepdims=True)
            stat[c, 0, :1] = column_to_row(row_sum)
            stat[c, 0, 1:] = column_to_row(row_sq)
            for k in range(1, n_head):
                push(stat.at[c, 0], stat.at[c, k], S_ST, st_r.at[c], to_head(k))
    with jax.named_scope("left2"):
        left(owg.at[:, :, pl.ds(0, piece * (n_seq - 1)), :], send_sem.at[S_OG])
        for way in (1, -1):
            for d in range(1, n_head):
                @pl.when(onward(way, d))
                def _():
                    left(attg.at[0], passed(way, d))
    for c in range(chunks):
        modulate(c)
    left(stat.at[:, pl.ds(0, n_head - 1)], send_sem.at[S_ST])


def put_out(resid, mod, resid_hbm, mod_hbm, sems):
    pieces = sems.shape[1]
    rows = resid.shape[0] // pieces
    copies = [
        pltpu.make_async_copy(src.at[at], dst.at[at], sems.at[i, p])
        for p, at in enumerate(pl.ds(p * rows, rows) for p in range(pieces))
        for i, (src, dst) in enumerate(((resid, resid_hbm), (mod, mod_hbm)))
    ]
    for copy in copies:
        copy.start()
    for copy in copies:
        copy.wait()


def on_device(
    n_seq,
    n_head,
    video_rows,
    context,
    valid_length,
    timestep,
    query_weight,
    key_weight,
    value_weight,
    out_weight,
    query_gain,
    key_gain,
    time_weight,
    modulation,
):
    tok, width = video_rows.shape
    text = context.shape[0]
    depth, att = query_weight.shape
    cols = out_weight.shape[1]
    part_width = modulation.shape[1]
    ratio = n_seq // n_head
    n_chip = n_seq // 2
    quarter = tok // 4
    sizes = [quarter // 2] + [quarter] * 3 + [quarter // 2]
    cuts = [slice(sum(sizes[:c]), sum(sizes[: c + 1])) for c in range(len(sizes))]
    chunks = len(cuts)
    piece = out_weight.shape[0] // n_seq
    half = FREQ // 2
    freqs = np.exp(-np.log(10000.0) * np.arange(half) / half).astype(np.float32)[None, :]
    sliced = part_width % LANES != 0 or cols % LANES != 0
    extra = []
    if sliced:
        extra.append(
            lax.dynamic_slice_in_dim(
                video_rows, lax.axis_index("head") * part_width, part_width, 1
            )
        )
    out_bytes = tok * -(-part_width // LANES) * LANES * 2
    vmem = pl.BlockSpec(memory_space=pltpu.VMEM)
    hbm = pl.BlockSpec(memory_space=pltpu.HBM)
    dma = pltpu.SemaphoreType.DMA
    results = pl.pallas_call(
        functools.partial(body, n_seq, n_head, cuts, sliced),
        out_shape=[pltpu.VMEM((tok, part_width), BF16)] * 2,
        in_specs=[hbm] * 13 + [vmem] * len(extra),
        out_specs=[vmem] * 2,
        scratch_shapes=[
            pltpu.VMEM((tok, width), BF16),
            pltpu.VMEM((tok, width), BF16),
            pltpu.VMEM((text, width), BF16),
            pltpu.VMEM((n_chip, text, 2 * depth), BF16),
            pltpu.VMEM((n_seq * depth, att), BF16),
            pltpu.VMEM((2, depth, 2 * att), BF16),
            pltpu.VMEM((n_chip, text, att), F32),
            pltpu.VMEM((n_seq, text, att), F32),
            pltpu.VMEM((n_chip, text, att), BF16),
            pltpu.VMEM((n_seq, text, att), BF16),
            pltpu.VMEM((text, att), F32),
            pltpu.VMEM((2 * text, att), F32),
            pltpu.VMEM((n_seq, text, att), BF16),
            pltpu.VMEM((n_seq, text, att), BF16),
            pltpu.VMEM((n_seq, piece, cols), BF16),
            pltpu.VMEM((ratio, n_head, out_weight.shape[0], cols), BF16),
            pltpu.VMEM((n_head, tok, att), BF16),
            pltpu.VMEM((tok, att), F32),
            pltpu.VMEM((n_head, 1, tok), F32),
            pltpu.VMEM((n_head, 1, -(-2 * text // LANES) * LANES), F32),
            pltpu.VMEM((chunks, n_head, 2, -(-max(sizes) // LANES) * LANES), F32),
            pltpu.VMEM((2, 8, part_width), F32),
            pltpu.VMEM(time_weight.shape, BF16),
            pltpu.VMEM((1, att), F32),
            pltpu.VMEM((1, att), F32),
            pltpu.VMEM((1, half), F32),
            pltpu.VMEM(modulation.shape, F32),
            pltpu.VMEM((tok, part_width), F32),
            pltpu.VMEM((1, 1), jnp.int32),
            pltpu.VMEM((1, 1), jnp.int32),
            dma((14,)),
            dma((14,)),
            dma((2, n_head - 1)),
            *[dma((n_chip,))] * 2,
            *[dma((2, n_chip)), dma((n_chip,))] * 2,
            dma((chunks, n_head - 1)),
            dma((chunks,)),
            dma((11,)),
        ],
        compiler_params=pltpu.CompilerParams(
            collective_id=0, has_side_effects=True, vmem_limit_bytes=VMEM_MOST - 2 * out_bytes
        ),
    )(
        valid_length[None, :],
        timestep[None, :],
        video_rows,
        context,
        query_weight,
        key_weight,
        value_weight,
        out_weight,
        query_gain[None, :],
        key_gain[None, :],
        freqs,
        time_weight,
        modulation,
        *extra,
    )
    return pl.pallas_call(
        put_out,
        out_shape=[jax.ShapeDtypeStruct((tok, part_width), BF16)] * 2,
        in_specs=[vmem] * 2,
        out_specs=[hbm] * 2,
        scratch_shapes=[dma((2, 4))],
        compiler_params=pltpu.CompilerParams(vmem_limit_bytes=4 * 1024 * 1024),
    )(*results)


def solution(mesh):
    in_specs = (
        P("seq", None),
        P("seq", None),
        P(),
        P(),
        P("seq", "head"),
        P("seq", "head"),
        P("seq", "head"),
        P("head", "seq"),
        P("head"),
        P("head"),
        P(None, None, "head"),
        P(None, "head"),
    )
    out_specs = (P("seq", "head"), P("seq", "head"))
    return jax.shard_map(
        functools.partial(on_device, mesh.shape["seq"], mesh.shape["head"]),
        mesh=mesh, in_specs=in_specs, out_specs=out_specs, check_vma=False,
    )
```

```python
import functools

import jax
import jax.numpy as jnp
import numpy as np
from jax import lax
from jax.experimental import pallas as pl
from jax.experimental.pallas import tpu as pltpu
from jax.sharding import PartitionSpec as P

HD = 128
FREQ = 256
LANES = 128
VMEM_MOST = 67_000_000
NORM_AT = (6, 8, 9)
F32 = jnp.float32
BF16 = jnp.bfloat16
MESH_ID = pl.DeviceIdType.MESH


def flip(index, mask):
    bit = 1
    while bit <= mask:
        if mask & bit:
            index = index + bit - 2 * bit * ((index // bit) % 2)
        bit *= 2
    return index


def bits_of(mask):
    return [1 << b for b in range(mask.bit_length()) if mask >> b & 1]


def last_bit(half, mask):
    return bits_of(mask)[-1] if half == 0 else bits_of(mask)[0]


def by_hops(n_seq):
    return sorted(range(2, n_seq, 2), key=lambda k: (len(bits_of(k)), k))


def column_to_row(column):
    tall = column.shape[0]
    wide = -(-tall // LANES) * LANES
    if wide > tall:
        column = jnp.concatenate([column, jnp.zeros((wide - tall, 1), F32)], axis=0)
    return jnp.transpose(jnp.broadcast_to(column, (wide, LANES)))[:1]


def row_to_column(row, tall):
    return jnp.transpose(jnp.broadcast_to(row, (LANES, row.shape[1])))[:tall, :1]


def body(n_seq, n_head, cuts, sliced, *refs):
    if sliced:
        steps(n_seq, n_head, cuts, *refs)
    else:
        steps(n_seq, n_head, cuts, *refs[:13], None, *refs[13:])


def steps(
    n_seq, n_head, cuts,
    valid_hbm, when_hbm, video, ctx, qw, kw, vw, ow, qg_hbm, kg_hbm, freqs_hbm, tw_hbm, mod_hbm, vpart,
    resid_out, mod_out,
    vid, normed, ctxv, ctxg, qwg, kvw, cks, ckr, cvs, cvr, own_v, key_sum, kall, vall, spread, owg, attg,
    queries, qsq, ksq, stat, shsc, tw, qg, kg, freqs, mod, acc, valid, when,
    loc_sem, send_sem, pass_s, ctx_r, ctz_r, qw_r, qc_r, og_r, oc_r, at_r, st_r, one_r,
):
    s = lax.axis_index("seq")
    z = lax.axis_index("head")
    core = s % 2
    chip = s // 2
    n_chip = n_seq // 2
    ratio = n_seq // n_head
    chunks = len(cuts)
    tok, width = vid.shape
    depth = qw.shape[0]
    att = qw.shape[1]
    text = ctx.shape[0]
    pair = 2 * depth
    masks = by_hops(n_seq)
    chip_bits = [k for k in masks if len(bits_of(k)) == 1]
    far = [k for k in masks if k not in chip_bits]
    (S_CTX, S_W, S_SP, S_QW, S_CK, S_CV, S_KSQ, S_QSQ, S_KV, S_OZ, S_OG, S_ST) = range(12)
    (R_W, R_SP, R_CK, R_CV, R_KSQ, R_QSQ, R_V, R_VC, R_K, R_KC, R_OZ, R_SPL) = range(12)

    def to_seq(k):
        return (flip(s, k), z)

    def to_head(k):
        return (s, flip(z, k))

    def remote(src, dst, ssem, rsem, dev):
        return pltpu.make_async_remote_copy(
            src_ref=src, dst_ref=dst, send_sem=ssem, recv_sem=rsem,
            device_id=dev, device_id_type=MESH_ID,
        )

    def push(src, dst, group, rsem, dev):
        remote(src, dst, send_sem.at[group], rsem, dev).start()

    def arrived(ref, sem):
        remote(ref, ref, sem, sem, to_seq(1)).wait_recv()

    def left(ref, sem):
        remote(ref, ref, sem, sem, to_seq(1)).wait_send()

    def gather_own(slot, half, bits, group, rsem):
        for b in bits:
            push(slot(half, s), slot(half, s), group, rsem.at[half, b // 2 - 1], to_seq(b))

    def gather_core(slot, group, csem):
        for half in range(2):
            push(slot(half, s), slot(half, s), group, csem.at[0], to_seq(1))

    def gather_relay(slot, half, k, group, rsem, csem):
        here = slot(half, flip(s, k))
        arrived(here, rsem.at[half, k // 2 - 1])
        for b in chip_bits:
            if not k & b and last_bit(half, k | b) == b:
                push(here, here, group, rsem.at[half, (k | b) // 2 - 1], to_seq(b))
        push(here, here, group, csem.at[k // 2], to_seq(1))

    barrier = pltpu.get_barrier_semaphore()
    for k in range(1, n_seq):
        pl.semaphore_signal(barrier, inc=1, device_id=to_seq(k), device_id_type=MESH_ID)
    for k in range(1, n_head):
        pl.semaphore_signal(barrier, inc=1, device_id=to_head(k), device_id_type=MESH_ID)

    def shard_rows(p, count=1):
        return qwg.at[pl.ds(pl.multiple_of(p * depth, depth), count * depth), :]

    def half_rows(half, p):
        rows = depth // 2
        return qwg.at[pl.ds(pl.multiple_of(p * depth + half * rows, rows), rows), :]

    def load(src, dst, i):
        copy = pltpu.make_async_copy(src, dst, loc_sem.at[i])
        copy.start()
        return copy

    piece = ow.shape[0] // n_seq

    def ow_piece(p):
        return pl.ds(pl.multiple_of(p * piece, piece), piece)

    own_ctx = load(ctx, ctxv, 0)
    own_qw = load(qw, shard_rows(s), 1)
    load(kw, kvw.at[core, :, :att], 2)
    load(vw, kvw.at[core, :, att:], 2)
    own_vid = load(video, vid, 4)
    own_spread = load(ow.at[ow_piece(s), :], spread.at[s], 5)
    own_tw = load(tw_hbm, tw, 6)
    small = [
        load(a, b, 7 + i)
        for i, (a, b) in enumerate(
            (
                (qg_hbm, qg), (kg_hbm, kg), (freqs_hbm, freqs), (mod_hbm, mod),
                (valid_hbm, valid), (when_hbm, when),
            )
        )
    ]
    with jax.named_scope("barrier"):
        pl.semaphore_wait(barrier, n_seq + n_head - 2)

    def ctx_cols(p):
        return pl.ds(pl.multiple_of(p * pair, pair), pair)

    part = text // 2

    def ctx_rows(q):
        return pl.ds(pl.multiple_of(q * part, part), part)

    mine = z % 2
    own_ctx.wait()
    for k in masks:
        push(
            ctxv.at[ctx_rows(mine), ctx_cols(flip(chip, k // 2))], ctxg.at[k // 2, ctx_rows(mine)],
            S_CTX, ctx_r.at[k // 2 - 1], to_seq(k),
        )
    pltpu.make_async_copy(kvw.at[core], kvw.at[core], loc_sem.at[2]).wait()
    push(kvw.at[core], kvw.at[core], S_W, one_r.at[R_W], to_seq(1))

    def spread_rows(ks, rsem):
        for k in ks:
            push(ow.at[ow_piece(flip(s, k)), :], spread.at[s], S_SP, one_r.at[rsem], to_seq(k))

    spread_rows(masks, R_SP)
    own_qw.wait()
    first = [(0, b) for b in chip_bits[:1]] + [(1, b) for b in chip_bits[1:]]
    second = [(0, b) for b in chip_bits[1:]] + [(1, b) for b in chip_bits[:1]]
    for half, b in first + second:
        gather_own(half_rows, half, [b], S_QW, qw_r)
    gather_core(half_rows, S_QW, qc_r)

    own_vid.wait()
    strip = 16
    strips = tok // strip

    def norm(begin, end):
        with jax.named_scope("norm"):
            @pl.loop(begin, end)
            def _(i):
                at = pl.ds(pl.multiple_of(i * strip, strip), strip)
                rows = vid[at, :].astype(F32)
                mean = jnp.mean(rows, axis=-1, keepdims=True)
                centred = rows - mean
                spread_ = jnp.mean(centred * centred, axis=-1, keepdims=True)
                normed[at, :] = (centred * (1.0 / jnp.sqrt(spread_ + 1e-06))).astype(BF16)

    def share(ks):
        with jax.named_scope("share%d" % len(ks)):
            for k in ks:
                here = ctxg.at[k // 2, ctx_rows(mine)]
                arrived(here, ctx_r.at[k // 2 - 1])
                push(here, here, S_CTX, ctz_r.at[k // 2 - 1], to_head(1))

    done = [strips * n // 16 for n in NORM_AT]
    norm(0, done[0])
    share(chip_bits)
    norm(done[0], done[1])
    share(far)
    norm(done[1], done[2])

    def keeper(k):
        return (flip(s, k) // 2 * 2 + 1, z)

    def chip_slot(ref, p):
        return ref.at[pl.ds(2 * p, 2)]

    def spread_text(ref, chips):
        here = chip_slot(ref, chip)
        for k in masks:
            push(here, here, S_KV, one_r.at[chips], to_seq(k))
        push(here, here, S_KV, one_r.at[chips + 1], to_seq(1))

    with jax.named_scope("kv"):
        arrived(kvw.at[1 - core], one_r.at[R_W])

        def partial_kv(source):
            return jnp.dot(source, kvw[...].reshape(pair, 2 * att), preferred_element_type=F32)

        block = partial_kv(ctxv[:, ctx_cols(chip)])
        cks[0] = block[:, :att]
        own_v[...] = block[:, att:]
        cvs[0] = block[:, att:].astype(BF16)
        for k in masks:
            c = k // 2
            arrived(ctxg.at[c, ctx_rows(1 - mine)], ctz_r.at[c - 1])
            block = partial_kv(ctxg[c])
            cks[c] = block[:, :att]
            cvs[c] = block[:, att:].astype(BF16)
            push(cks.at[c], ckr.at[core * n_chip + c], S_CK, one_r.at[R_CK], keeper(k))

        @pl.when(core == 0)
        def _():
            push(cks.at[0], ckr.at[0], S_CK, one_r.at[R_CK], to_seq(1))

    def shard_queries(p, rows):
        lanes = pl.ds(pl.multiple_of(p * rows, rows), rows)
        return jnp.dot(normed[:, lanes], qwg[lanes, :], preferred_element_type=F32)

    def chip_queries(p):
        return shard_queries(p, pair)

    with jax.named_scope("relay1"):
        for half, b in first:
            gather_relay(half_rows, half, b, S_QW, qw_r, qc_r)
        for k in masks:
            c = k // 2
            push(cvs.at[c], cvr.at[core * n_chip + c], S_CV, one_r.at[R_CV], keeper(k))

        @pl.when(core == 0)
        def _():
            push(cvs.at[0], cvr.at[0], S_CV, one_r.at[R_CV], to_seq(1))

    spread_rows([k + 1 for k in masks] + [1], R_SPL)
    norm(done[2], strips)

    def own_cols(zz):
        return pl.ds(zz * ratio, ratio)

    def ow_slot_z(p):
        return owg.at[:, p, ow_piece(s), :]

    def hand_over(k, j):
        zz = flip(z, k)
        push(
            spread.at[zz * ratio + j], owg.at[j, z, ow_piece(s), :], S_OZ, one_r.at[R_OZ], to_head(k)
        )

    with jax.named_scope("spread"):
        own_spread.wait()
        arrived(spread.at[pl.ds(0, n_chip - 1)], one_r.at[R_SP])
        if ratio > 1:
            for j in range(0, ratio, 2):
                for k in range(1, n_head):
                    hand_over(k, j + core)

    with jax.named_scope("relay2"):
        for half, b in second:
            gather_relay(half_rows, half, b, S_QW, qw_r, qc_r)
        arrived(shard_rows(flip(s, 1)), qc_r.at[0])
    with jax.named_scope("q_own"):
        queries[...] = chip_queries(chip)
    with jax.named_scope("shsc"):
        own_tw.wait()
        for copy in small:
            copy.wait()
        angles = jnp.broadcast_to(when[...].astype(F32) * freqs[...], (16, freqs.shape[1]))
        embedding = jnp.concatenate([jnp.cos(angles), jnp.sin(angles)], axis=1)
        act = (embedding / (1.0 + jnp.exp(-embedding))).astype(BF16)
        for i in range(2):
            shsc[i] = mod[i : i + 1, :] + jnp.dot(act, tw[i], preferred_element_type=F32)[:8]

    @pl.when(core == 1)
    def _():
        with jax.named_scope("kv_sum"):
            arrived(ckr.at[pl.ds(0, n_seq - 1)], one_r.at[R_CK])
            both = [ckr[0], cks[0]]
            for q in range(2):
                for c in range(1, n_chip):
                    both[q] = both[q] + ckr[q * n_chip + c]
            key_rows = jnp.concatenate(both, axis=0)
            key_sum[...] = key_rows
            ksq[0] = column_to_row(jnp.sum(key_rows * key_rows, axis=1, keepdims=True))
            for k in range(1, n_head):
                push(ksq.at[0], ksq.at[k], S_KSQ, one_r.at[R_KSQ], to_head(k))

    with jax.named_scope("q_mid"):
        for b in chip_bits:
            arrived(shard_rows(flip(s, b + 1)), qc_r.at[b // 2])
            queries[...] += chip_queries(flip(chip, b // 2))

    with jax.named_scope("far_relay"):
        for k in far:
            for half in range(2):
                gather_relay(half_rows, half, k, S_QW, qw_r, qc_r)
        if depth % LANES == 0:
            for k in far:
                queries[...] += shard_queries(flip(s, k), depth)

    @pl.when(core == 1)
    def _():
        with jax.named_scope("k_norm"):
            arrived(ksq.at[pl.ds(1, n_head - 1)], one_r.at[R_KSQ])
            k_mean = row_to_column(jnp.sum(ksq[...], axis=0), 2 * text) / (att * n_head)
            key_normed = (key_sum[...] / jnp.sqrt(k_mean + 1e-06) * kg[...]).astype(BF16)
            for q in range(2):
                kall[2 * chip + q] = key_normed[q * text : (q + 1) * text]
            spread_text(kall, R_K)
        with jax.named_scope("v_sum"):
            arrived(cvr.at[pl.ds(0, n_seq - 1)], one_r.at[R_CV])
            both = [cvr[0].astype(F32), own_v[...]]
            for q in range(2):
                for c in range(1, n_chip):
                    both[q] = both[q] + cvr[q * n_chip + c].astype(F32)
                vall[2 * chip + q] = both[q].astype(BF16)
            spread_text(vall, R_V)

    def ow_half(half, p):
        if ratio == 1:
            rows = piece // 2
            return owg.at[:, :, pl.ds(pl.multiple_of(p * piece + half * rows, rows), rows), :]
        cut = ratio // 2
        return owg.at[pl.ds(half * cut, cut), :, ow_piece(p), :]

    def ow_slot(p):
        return owg.at[:, :, ow_piece(p), :]

    with jax.named_scope("q_far"):
        for k in far:
            arrived(shard_rows(flip(s, k + 1)), qc_r.at[k // 2])
            if depth % LANES == 0:
                queries[...] += shard_queries(flip(s, k + 1), depth)
            else:
                queries[...] += chip_queries(flip(chip, k // 2))
        q = queries[...]
        qsq[0] = column_to_row(jnp.sum(q * q, axis=1, keepdims=True))
        for k in range(1, n_head):
            push(qsq.at[0], qsq.at[k], S_QSQ, one_r.at[R_QSQ], to_head(k))

    with jax.named_scope("spread_late"):
        arrived(spread.at[pl.ds(0, n_chip)], one_r.at[R_SPL])
        own_ow = load(spread.at[own_cols(z)], ow_slot_z(z), 3)
        for k in range(1, n_head):
            if ratio > 1:
                for j in range(0, ratio, 2):
                    hand_over(k, j + 1 - core)
            else:
                hand_over(k, 0)

    @pl.when(core == 1)
    def _():
        with jax.named_scope("kv_in"):
            for ref, chips in ((kall, R_K), (vall, R_V)):
                arrived(ref.at[pl.ds(0, n_seq - 2)], one_r.at[chips])
                for k in masks:
                    here = chip_slot(ref, flip(chip, k // 2))
                    push(here, here, S_KV, one_r.at[chips + 1], to_seq(1))

    @pl.when(core == 0)
    def _():
        with jax.named_scope("kv_end"):
            for ref, chips in ((kall, R_K), (vall, R_V)):
                arrived(ref, one_r.at[chips + 1])

    with jax.named_scope("q_norm"):
        arrived(qsq.at[pl.ds(1, n_head - 1)], one_r.at[R_QSQ])
        q_mean = row_to_column(jnp.sum(qsq[...], axis=0), tok) / (att * n_head)
        q_root = jnp.sqrt(q_mean + 1e-06)

    def held(way, d):
        return d % n_head if way > 0 else (n_head - d) % n_head

    def onward(way, d):
        origin = z - way * (d - 1)
        return (origin >= 0) & (origin < n_head) & (z + way >= 0) & (z + way < n_head)

    def passed(way, d):
        return pass_s.at[0 if way > 0 else 1, d - 1]

    def reach(way, c, d):
        slot = held(way, d)

        @pl.when(onward(way, d))
        def _():
            remote(
                attg.at[held(way, d - 1), cuts[c]], attg.at[slot, cuts[c]],
                passed(way, d), at_r.at[c, slot - 1], (s, z + way),
            ).start()

    def take(way, c, d):
        slot = held(way, d)
        origin = z - way * d

        @pl.when((origin >= 0) & (origin < n_head))
        def _():
            arrived(attg.at[slot, cuts[c]], at_r.at[c, slot - 1])

    def ow_relays(pairs):
        for half, b in pairs:
            gather_relay(ow_half, half, b, S_OG, og_r, oc_r)

    def ow_begin():
        with jax.named_scope("ow_start"):
            own_ow.wait()
            arrived(owg.at[:, pl.ds(0, n_head - 1), ow_piece(s), :], one_r.at[R_OZ])
            for half, b in first + second:
                gather_own(ow_half, half, [b], S_OG, og_r)
            gather_core(ow_half, S_OG, oc_r)

    all_text = n_seq * text
    with jax.named_scope("attend"):
        every_k = kall[...].reshape(all_text, att)
        every_v = vall[...].reshape(all_text, att)
        seen = lax.broadcasted_iota(jnp.int32, (1, all_text), 1) < valid[...]
        for c in range(chunks):
            at = cuts[c]
            q_normed = (queries[at, :] / q_root[at] * qg[...]).astype(BF16)
            for h in range(att // HD):
                lanes = slice(h * HD, (h + 1) * HD)
                scores = lax.dot_general(
                    q_normed[:, lanes], every_k[:, lanes], (((1,), (1,)), ((), ())),
                    preferred_element_type=F32,
                ) * HD ** (-0.5)
                scores = jnp.where(seen, scores, F32(-1e30))
                shifted = jnp.exp(scores - jnp.max(scores, axis=-1, keepdims=True))
                weights = (shifted * (1.0 / jnp.sum(shifted, axis=-1, keepdims=True))).astype(BF16)
                attg[0, at, lanes] = jnp.dot(
                    weights, every_v[:, lanes], preferred_element_type=F32
                ).astype(BF16)
            for way in (1, -1):
                reach(way, c, 1)
            if c == 1:
                ow_begin()

    cols = owg.shape[3]
    part_width = mod_out.shape[1]
    last = z + 1 - (2 * z) // n_head

    def projection(at, j, slot):
        return jnp.dot(
            attg[slot, at], owg[j, lax.rem(z + n_head - slot, n_head)], preferred_element_type=F32
        )

    def accumulate(begin, end):
        at = slice(cuts[begin].start, cuts[end - 1].stop)
        with jax.named_scope(f"accumulate{begin}"):
            for j in range(ratio):
                here = slice(j * cols, (j + 1) * cols)
                if vpart is None:
                    base = vid[at, pl.ds(pl.multiple_of(z * part_width + j * cols, LANES), cols)]
                else:
                    base = vpart[at, here]
                projected = projection(at, j, 0)
                for i in range(1, n_head - 1):
                    projected = projected + projection(at, j, lax.rem(last - 1 + i, n_head - 1) + 1)
                acc[at, here] = base.astype(F32) + projected

    for d in range(1, n_head - 1):
        for c in range(chunks):
            with jax.named_scope(f"pass{d}_{c}"):
                for way in (1, -1):
                    take(way, c, d)
                    reach(way, c, d + 1)
            if d == 1 and c == 1:
                with jax.named_scope("ow1"):
                    ow_relays(first)
            if d == 1 and c == chunks - 1:
                with jax.named_scope("ow2"):
                    ow_relays(second)
            if d == n_head - 2 and c == 1:
                with jax.named_scope("ow3"):
                    for k in far:
                        for half in range(2):
                            gather_relay(ow_half, half, k, S_OG, og_r, oc_r)
            if d == n_head - 2 and c == 2:
                with jax.named_scope("ow4"):
                    for k in [0] + masks:
                        arrived(ow_slot(flip(s, k + 1)), oc_r.at[k // 2])
                accumulate(0, 3)
    accumulate(3, chunks)
    with jax.named_scope("left1"):
        few = pl.ds(0, n_chip - 1)
        left(ctxg.at[few], send_sem.at[S_CTX])
        left(kvw.at[0], send_sem.at[S_W])
        left(spread.at[pl.ds(0, n_seq - 1)], send_sem.at[S_SP])
        left(shard_rows(0, n_seq - 1), send_sem.at[S_QW])
        left(qsq.at[pl.ds(0, n_head - 1)], send_sem.at[S_QSQ])
        left(owg.at[:, pl.ds(0, n_head - 1), ow_piece(0), :], send_sem.at[S_OZ])

        @pl.when(core == 0)
        def _():
            left(ckr.at[pl.ds(0, n_chip)], send_sem.at[S_CK])
            left(cvr.at[pl.ds(0, n_chip)], send_sem.at[S_CV])

        @pl.when(core == 1)
        def _():
            left(ckr.at[few], send_sem.at[S_CK])
            left(cvr.at[few], send_sem.at[S_CV])
            left(ksq.at[pl.ds(0, n_head - 1)], send_sem.at[S_KSQ])
            left(qwg.at[pl.ds(0, 4 * (n_seq - 1) * text)], send_sem.at[S_KV])

    def modulate(c):
        at = cuts[c]
        step = at.stop - at.start
        with jax.named_scope(f"stat{c}"):
            arrived(stat.at[c, pl.ds(1, n_head - 1)], st_r.at[c])
        with jax.named_scope(f"modulate{c}"):
            wide_row = -(-2 * step // LANES) * LANES
            both = jnp.sum(stat[c, :, :, :wide_row], axis=0) / (part_width * n_head)
            both_col = row_to_column(both, 2 * step)
            mean_col = both_col[:step]
            inv_col = 1.0 / jnp.sqrt(both_col[step:] - mean_col * mean_col + 1e-06)
            wide = resid_out[at, :].astype(F32)
            mod_out[at, :] = (
                (wide - mean_col) * inv_col * (1.0 + shsc[1, :1, :]) + shsc[0, :1, :]
            ).astype(BF16)

    for c in range(chunks):
        at = cuts[c]
        step = at.stop - at.start
        with jax.named_scope(f"last{c}"):
            for way in (1, -1):
                take(way, c, n_head - 1)
        with jax.named_scope(f"project{c}"):
            row_sum = jnp.zeros((step, 1), F32)
            row_sq = jnp.zeros((step, 1), F32)
            for j in range(ratio):
                here = slice(j * cols, (j + 1) * cols)
                rounded = (acc[at, here] + projection(at, j, last)).astype(BF16)
                resid_out[at, here] = rounded
                wide = rounded.astype(F32)
                row_sum = row_sum + jnp.sum(wide, axis=1, keepdims=True)
                row_sq = row_sq + jnp.sum(wide * wide, axis=1, keepdims=True)
            moments = column_to_row(jnp.concatenate([row_sum, row_sq], axis=0))
            stat[c, 0, :, : moments.shape[1]] = moments
            for k in range(1, n_head):
                push(stat.at[c, 0], stat.at[c, k], S_ST, st_r.at[c], to_head(k))
    with jax.named_scope("left2"):
        left(owg.at[:, :, pl.ds(0, piece * (n_seq - 1)), :], send_sem.at[S_OG])
        for way in (1, -1):
            for d in range(1, n_head):
                @pl.when(onward(way, d))
                def _():
                    left(attg.at[0], passed(way, d))
    for c in range(chunks):
        modulate(c)
    left(stat.at[:, pl.ds(0, n_head - 1)], send_sem.at[S_ST])


def put_out(resid, mod, resid_hbm, mod_hbm, sems):
    pieces = sems.shape[1]
    rows = resid.shape[0] // pieces
    copies = [
        pltpu.make_async_copy(src.at[at], dst.at[at], sems.at[i, p])
        for p, at in enumerate(pl.ds(p * rows, rows) for p in range(pieces))
        for i, (src, dst) in enumerate(((resid, resid_hbm), (mod, mod_hbm)))
    ]
    for copy in copies:
        copy.start()
    for copy in copies:
        copy.wait()


def on_device(
    n_seq,
    n_head,
    video_rows,
    context,
    valid_length,
    timestep,
    query_weight,
    key_weight,
    value_weight,
    out_weight,
    query_gain,
    key_gain,
    time_weight,
    modulation,
):
    tok, width = video_rows.shape
    text = context.shape[0]
    depth, att = query_weight.shape
    cols = out_weight.shape[1]
    part_width = modulation.shape[1]
    ratio = n_seq // n_head
    n_chip = n_seq // 2
    quarter = tok // 4
    sizes = [quarter // 2] + [quarter] * 3 + [quarter // 2]
    cuts = [slice(sum(sizes[:c]), sum(sizes[: c + 1])) for c in range(len(sizes))]
    chunks = len(cuts)
    piece = out_weight.shape[0] // n_seq
    half = FREQ // 2
    freqs = np.exp(-np.log(10000.0) * np.arange(half) / half).astype(np.float32)[None, :]
    sliced = part_width % LANES != 0 or cols % LANES != 0
    extra = []
    if sliced:
        extra.append(
            lax.dynamic_slice_in_dim(
                video_rows, lax.axis_index("head") * part_width, part_width, 1
            )
        )
    out_bytes = tok * -(-part_width // LANES) * LANES * 2
    vmem = pl.BlockSpec(memory_space=pltpu.VMEM)
    hbm = pl.BlockSpec(memory_space=pltpu.HBM)
    dma = pltpu.SemaphoreType.DMA
    results = pl.pallas_call(
        functools.partial(body, n_seq, n_head, cuts, sliced),
        out_shape=[pltpu.VMEM((tok, part_width), BF16)] * 2,
        in_specs=[hbm] * 13 + [vmem] * len(extra),
        out_specs=[vmem] * 2,
        scratch_shapes=[
            pltpu.VMEM((tok, width), BF16),
            pltpu.VMEM((tok, width), BF16),
            pltpu.VMEM((text, width), BF16),
            pltpu.VMEM((n_chip, text, 2 * depth), BF16),
            pltpu.VMEM((n_seq * depth, att), BF16),
            pltpu.VMEM((2, depth, 2 * att), BF16),
            pltpu.VMEM((n_chip, text, att), F32),
            pltpu.VMEM((n_seq, text, att), F32),
            pltpu.VMEM((n_chip, text, att), BF16),
            pltpu.VMEM((n_seq, text, att), BF16),
            pltpu.VMEM((text, att), F32),
            pltpu.VMEM((2 * text, att), F32),
            pltpu.VMEM((n_seq, text, att), BF16),
            pltpu.VMEM((n_seq, text, att), BF16),
            pltpu.VMEM((n_seq, piece, cols), BF16),
            pltpu.VMEM((ratio, n_head, out_weight.shape[0], cols), BF16),
            pltpu.VMEM((n_head, tok, att), BF16),
            pltpu.VMEM((tok, att), F32),
            pltpu.VMEM((n_head, 1, tok), F32),
            pltpu.VMEM((n_head, 1, -(-2 * text // LANES) * LANES), F32),
            pltpu.VMEM((chunks, n_head, 1, -(-2 * max(sizes) // LANES) * LANES), F32),
            pltpu.VMEM((2, 8, part_width), F32),
            pltpu.VMEM(time_weight.shape, BF16),
            pltpu.VMEM((1, att), F32),
            pltpu.VMEM((1, att), F32),
            pltpu.VMEM((1, half), F32),
            pltpu.VMEM(modulation.shape, F32),
            pltpu.VMEM((tok, part_width), F32),
            pltpu.VMEM((1, 1), jnp.int32),
            pltpu.VMEM((1, 1), jnp.int32),
            dma((13,)),
            dma((12,)),
            dma((2, n_head - 1)),
            *[dma((n_chip - 1,))] * 2,
            *[dma((2, n_chip - 1)), dma((n_chip,))] * 2,
            dma((chunks, n_head - 1)),
            dma((chunks,)),
            dma((12,)),
        ],
        compiler_params=pltpu.CompilerParams(
            collective_id=0, has_side_effects=True, vmem_limit_bytes=VMEM_MOST - 2 * out_bytes
        ),
    )(
        valid_length[None, :],
        timestep[None, :],
        video_rows,
        context,
        query_weight,
        key_weight,
        value_weight,
        out_weight,
        query_gain[None, :],
        key_gain[None, :],
        freqs,
        time_weight,
        modulation,
        *extra,
    )
    return pl.pallas_call(
        put_out,
        out_shape=[jax.ShapeDtypeStruct((tok, part_width), BF16)] * 2,
        in_specs=[vmem] * 2,
        out_specs=[hbm] * 2,
        scratch_shapes=[dma((2, 4))],
        compiler_params=pltpu.CompilerParams(vmem_limit_bytes=4 * 1024 * 1024),
    )(*results)


def solution(mesh):
    in_specs = (
        P("seq", None),
        P("seq", None),
        P(),
        P(),
        P("seq", "head"),
        P("seq", "head"),
        P("seq", "head"),
        P("head", "seq"),
        P("head"),
        P("head"),
        P(None, None, "head"),
        P(None, "head"),
    )
    out_specs = (P("seq", "head"), P("seq", "head"))
    return jax.shard_map(
        functools.partial(on_device, mesh.shape["seq"], mesh.shape["head"]),
        mesh=mesh, in_specs=in_specs, out_specs=out_specs, check_vma=False,
    )
```

```python
import functools

import jax
import jax.numpy as jnp
import numpy as np
from jax import lax
from jax.experimental import pallas as pl
from jax.experimental.pallas import tpu as pltpu
from jax.sharding import PartitionSpec as P

HD = 128
FREQ = 256
LANES = 128
VMEM_MOST = 67_000_000
NORM_AT = (6, 8, 9)
F32 = jnp.float32
BF16 = jnp.bfloat16
MESH_ID = pl.DeviceIdType.MESH


def flip(index, mask):
    bit = 1
    while bit <= mask:
        if mask & bit:
            index = index + bit - 2 * bit * ((index // bit) % 2)
        bit *= 2
    return index


def bits_of(mask):
    return [1 << b for b in range(mask.bit_length()) if mask >> b & 1]


def last_bit(half, mask):
    return bits_of(mask)[-1] if half == 0 else bits_of(mask)[0]


def by_hops(n_seq):
    return sorted(range(2, n_seq, 2), key=lambda k: (len(bits_of(k)), k))


def column_to_row(column):
    tall = column.shape[0]
    wide = -(-tall // LANES) * LANES
    if wide > tall:
        column = jnp.concatenate([column, jnp.zeros((wide - tall, 1), F32)], axis=0)
    return jnp.transpose(jnp.broadcast_to(column, (wide, LANES)))[:1]


def row_to_column(row, tall):
    return jnp.transpose(jnp.broadcast_to(row, (LANES, row.shape[1])))[:tall, :1]


def body(n_seq, n_head, cuts, sliced, *refs):
    if sliced:
        steps(n_seq, n_head, cuts, *refs)
    else:
        steps(n_seq, n_head, cuts, *refs[:13], None, *refs[13:])


def steps(
    n_seq, n_head, cuts,
    valid_hbm, when_hbm, video, ctx, qw, kw, vw, ow, qg_hbm, kg_hbm, freqs_hbm, tw_hbm, mod_hbm, vpart,
    resid_out, mod_out,
    vid, normed, ctxv, ctxg, qwg, kvw, cks, ckr, cvs, cvr, own_v, key_sum, kall, vall, spread, owg, attg,
    queries, qsq, ksq, stat, shsc, tw, qg, kg, freqs, mod, acc, valid, when,
    loc_sem, send_sem, pass_s, ctx_r, ctz_r, qw_r, qc_r, og_r, oc_r, at_r, st_r, one_r,
):
    s = lax.axis_index("seq")
    z = lax.axis_index("head")
    core = s % 2
    chip = s // 2
    n_chip = n_seq // 2
    ratio = n_seq // n_head
    chunks = len(cuts)
    tok, width = vid.shape
    depth = qw.shape[0]
    att = qw.shape[1]
    text = ctx.shape[0]
    pair = 2 * depth
    masks = by_hops(n_seq)
    chip_bits = [k for k in masks if len(bits_of(k)) == 1]
    far = [k for k in masks if k not in chip_bits]
    (S_CTX, S_W, S_SP, S_QW, S_CK, S_CV, S_KSQ, S_QSQ, S_KV, S_OZ, S_OG, S_ST) = range(12)
    (R_W, R_SP, R_CK, R_CV, R_KSQ, R_QSQ, R_V, R_VC, R_K, R_KC, R_OZ, R_SPL) = range(12)

    def to_seq(k):
        return (flip(s, k), z)

    def to_head(k):
        return (s, flip(z, k))

    def remote(src, dst, ssem, rsem, dev):
        return pltpu.make_async_remote_copy(
            src_ref=src, dst_ref=dst, send_sem=ssem, recv_sem=rsem,
            device_id=dev, device_id_type=MESH_ID,
        )

    def push(src, dst, group, rsem, dev):
        remote(src, dst, send_sem.at[group], rsem, dev).start()

    def arrived(ref, sem):
        remote(ref, ref, sem, sem, to_seq(1)).wait_recv()

    def left(ref, sem):
        remote(ref, ref, sem, sem, to_seq(1)).wait_send()

    def gather_own(slot, half, bits, group, rsem):
        for b in bits:
            push(slot(half, s), slot(half, s), group, rsem.at[half, b // 2 - 1], to_seq(b))

    def gather_core(slot, group, csem):
        for half in range(2):
            push(slot(half, s), slot(half, s), group, csem.at[0], to_seq(1))

    def gather_relay(slot, half, k, group, rsem, csem):
        here = slot(half, flip(s, k))
        arrived(here, rsem.at[half, k // 2 - 1])
        for b in chip_bits:
            if not k & b and last_bit(half, k | b) == b:
                push(here, here, group, rsem.at[half, (k | b) // 2 - 1], to_seq(b))
        push(here, here, group, csem.at[k // 2], to_seq(1))

    barrier = pltpu.get_barrier_semaphore()
    for k in range(1, n_seq):
        pl.semaphore_signal(barrier, inc=1, device_id=to_seq(k), device_id_type=MESH_ID)
    for k in range(1, n_head):
        pl.semaphore_signal(barrier, inc=1, device_id=to_head(k), device_id_type=MESH_ID)

    def shard_rows(p, count=1):
        return qwg.at[pl.ds(pl.multiple_of(p * depth, depth), count * depth), :]

    def half_rows(half, p):
        rows = depth // 2
        return qwg.at[pl.ds(pl.multiple_of(p * depth + half * rows, rows), rows), :]

    def load(src, dst, i):
        copy = pltpu.make_async_copy(src, dst, loc_sem.at[i])
        copy.start()
        return copy

    piece = ow.shape[0] // n_seq

    def ow_piece(p):
        return pl.ds(pl.multiple_of(p * piece, piece), piece)

    own_ctx = load(ctx, ctxv, 0)
    own_qw = load(qw, shard_rows(s), 1)
    load(kw, kvw.at[core, :, :att], 2)
    load(vw, kvw.at[core, :, att:], 2)
    own_vid = load(video, vid, 4)
    own_spread = load(ow.at[ow_piece(s), :], spread.at[s], 5)
    own_tw = load(tw_hbm, tw, 6)
    small = [
        load(a, b, 7 + i)
        for i, (a, b) in enumerate(
            (
                (qg_hbm, qg), (kg_hbm, kg), (freqs_hbm, freqs), (mod_hbm, mod),
                (valid_hbm, valid), (when_hbm, when),
            )
        )
    ]
    with jax.named_scope("barrier"):
        pl.semaphore_wait(barrier, n_seq + n_head - 2)

    def ctx_cols(p):
        return pl.ds(pl.multiple_of(p * pair, pair), pair)

    part = text // 2

    def ctx_rows(q):
        return pl.ds(pl.multiple_of(q * part, part), part)

    mine = z % 2
    own_ctx.wait()
    for k in masks:
        push(
            ctxv.at[ctx_rows(mine), ctx_cols(flip(chip, k // 2))], ctxg.at[k // 2, ctx_rows(mine)],
            S_CTX, ctx_r.at[k // 2 - 1], to_seq(k),
        )
    pltpu.make_async_copy(kvw.at[core], kvw.at[core], loc_sem.at[2]).wait()
    push(kvw.at[core], kvw.at[core], S_W, one_r.at[R_W], to_seq(1))

    def spread_rows(ks, rsem):
        for k in ks:
            push(ow.at[ow_piece(flip(s, k)), :], spread.at[s], S_SP, one_r.at[rsem], to_seq(k))

    spread_rows(masks, R_SP)
    own_qw.wait()
    first = [(0, b) for b in chip_bits[:1]] + [(1, b) for b in chip_bits[1:]]
    second = [(0, b) for b in chip_bits[1:]] + [(1, b) for b in chip_bits[:1]]
    for half, b in first + second:
        gather_own(half_rows, half, [b], S_QW, qw_r)
    gather_core(half_rows, S_QW, qc_r)

    own_vid.wait()
    strip = 16
    strips = tok // strip

    def norm(begin, end):
        with jax.named_scope("norm"):
            @pl.loop(begin, end)
            def _(i):
                at = pl.ds(pl.multiple_of(i * strip, strip), strip)
                rows = vid[at, :].astype(F32)
                mean = jnp.mean(rows, axis=-1, keepdims=True)
                centred = rows - mean
                spread_ = jnp.mean(centred * centred, axis=-1, keepdims=True)
                normed[at, :] = (centred * (1.0 / jnp.sqrt(spread_ + 1e-06))).astype(BF16)

    def share(ks):
        with jax.named_scope("share%d" % len(ks)):
            for k in ks:
                here = ctxg.at[k // 2, ctx_rows(mine)]
                arrived(here, ctx_r.at[k // 2 - 1])
                push(here, here, S_CTX, ctz_r.at[k // 2 - 1], to_head(1))

    done = [strips * n // 16 for n in NORM_AT]
    norm(0, done[0])
    share(chip_bits)
    norm(done[0], done[1])
    share(far)
    norm(done[1], done[2])

    def keeper(k):
        return (flip(s, k) // 2 * 2 + 1, z)

    def chip_slot(ref, p):
        return ref.at[pl.ds(2 * p, 2)]

    def spread_text(ref, chips):
        here = chip_slot(ref, chip)
        for k in masks:
            push(here, here, S_KV, one_r.at[chips], to_seq(k))
        push(here, here, S_KV, one_r.at[chips + 1], to_seq(1))

    with jax.named_scope("kv"):
        arrived(kvw.at[1 - core], one_r.at[R_W])

        def partial_kv(source):
            return jnp.dot(source, kvw[...].reshape(pair, 2 * att), preferred_element_type=F32)

        block = partial_kv(ctxv[:, ctx_cols(chip)])
        cks[0] = block[:, :att]
        own_v[...] = block[:, att:]
        cvs[0] = block[:, att:].astype(BF16)
        for k in masks:
            c = k // 2
            arrived(ctxg.at[c, ctx_rows(1 - mine)], ctz_r.at[c - 1])
            block = partial_kv(ctxg[c])
            cks[c] = block[:, :att]
            cvs[c] = block[:, att:].astype(BF16)
            push(cks.at[c], ckr.at[core * n_chip + c], S_CK, one_r.at[R_CK], keeper(k))

        @pl.when(core == 0)
        def _():
            push(cks.at[0], ckr.at[0], S_CK, one_r.at[R_CK], to_seq(1))

    def shard_queries(p, rows):
        lanes = pl.ds(pl.multiple_of(p * rows, rows), rows)
        return jnp.dot(normed[:, lanes], qwg[lanes, :], preferred_element_type=F32)

    def chip_queries(p):
        return shard_queries(p, pair)

    with jax.named_scope("relay1"):
        for half, b in first:
            gather_relay(half_rows, half, b, S_QW, qw_r, qc_r)
        for k in masks:
            c = k // 2
            push(cvs.at[c], cvr.at[core * n_chip + c], S_CV, one_r.at[R_CV], keeper(k))

        @pl.when(core == 0)
        def _():
            push(cvs.at[0], cvr.at[0], S_CV, one_r.at[R_CV], to_seq(1))

    spread_rows([k + 1 for k in masks] + [1], R_SPL)
    norm(done[2], strips)

    def own_cols(zz):
        return pl.ds(zz * ratio, ratio)

    def ow_slot_z(p):
        return owg.at[:, p, ow_piece(s), :]

    def hand_over(k, j):
        zz = flip(z, k)
        push(
            spread.at[zz * ratio + j], owg.at[j, z, ow_piece(s), :], S_OZ, one_r.at[R_OZ], to_head(k)
        )

    with jax.named_scope("spread"):
        own_spread.wait()
        arrived(spread.at[pl.ds(0, n_chip - 1)], one_r.at[R_SP])
        if ratio > 1:
            for j in range(0, ratio, 2):
                for k in range(1, n_head):
                    hand_over(k, j + core)

    with jax.named_scope("relay2"):
        for half, b in second:
            gather_relay(half_rows, half, b, S_QW, qw_r, qc_r)
        arrived(shard_rows(flip(s, 1)), qc_r.at[0])
    with jax.named_scope("q_own"):
        queries[...] = chip_queries(chip)
    with jax.named_scope("shsc"):
        own_tw.wait()
        for copy in small:
            copy.wait()
        angles = jnp.broadcast_to(when[...].astype(F32) * freqs[...], (16, freqs.shape[1]))
        embedding = jnp.concatenate([jnp.cos(angles), jnp.sin(angles)], axis=1)
        act = (embedding / (1.0 + jnp.exp(-embedding))).astype(BF16)
        for i in range(2):
            shsc[i] = mod[i : i + 1, :] + jnp.dot(act, tw[i], preferred_element_type=F32)[:8]

    @pl.when(core == 1)
    def _():
        with jax.named_scope("kv_sum"):
            arrived(ckr.at[pl.ds(0, n_seq - 1)], one_r.at[R_CK])
            both = [ckr[0], cks[0]]
            for q in range(2):
                for c in range(1, n_chip):
                    both[q] = both[q] + ckr[q * n_chip + c]
            key_rows = jnp.concatenate(both, axis=0)
            key_sum[...] = key_rows
            ksq[0] = column_to_row(jnp.sum(key_rows * key_rows, axis=1, keepdims=True))
            for k in range(1, n_head):
                push(ksq.at[0], ksq.at[k], S_KSQ, one_r.at[R_KSQ], to_head(k))

    with jax.named_scope("q_mid"):
        for b in chip_bits:
            arrived(shard_rows(flip(s, b + 1)), qc_r.at[b // 2])
            queries[...] += chip_queries(flip(chip, b // 2))

    with jax.named_scope("far_relay"):
        for k in far:
            for half in range(2):
                gather_relay(half_rows, half, k, S_QW, qw_r, qc_r)
        if depth % LANES == 0:
            for k in far:
                queries[...] += shard_queries(flip(s, k), depth)

    @pl.when(core == 1)
    def _():
        with jax.named_scope("k_norm"):
            arrived(ksq.at[pl.ds(1, n_head - 1)], one_r.at[R_KSQ])
            k_mean = row_to_column(jnp.sum(ksq[...], axis=0), 2 * text) / (att * n_head)
            key_normed = (key_sum[...] / jnp.sqrt(k_mean + 1e-06) * kg[...]).astype(BF16)
            for q in range(2):
                kall[2 * chip + q] = key_normed[q * text : (q + 1) * text]
            spread_text(kall, R_K)
        with jax.named_scope("v_sum"):
            arrived(cvr.at[pl.ds(0, n_seq - 1)], one_r.at[R_CV])
            both = [cvr[0].astype(F32), own_v[...]]
            for q in range(2):
                for c in range(1, n_chip):
                    both[q] = both[q] + cvr[q * n_chip + c].astype(F32)
                vall[2 * chip + q] = both[q].astype(BF16)
            spread_text(vall, R_V)

    def ow_half(half, p):
        if ratio == 1:
            rows = piece // 2
            return owg.at[:, :, pl.ds(pl.multiple_of(p * piece + half * rows, rows), rows), :]
        cut = ratio // 2
        return owg.at[pl.ds(half * cut, cut), :, ow_piece(p), :]

    def ow_slot(p):
        return owg.at[:, :, ow_piece(p), :]

    with jax.named_scope("q_far"):
        for k in far:
            arrived(shard_rows(flip(s, k + 1)), qc_r.at[k // 2])
            if depth % LANES == 0:
                queries[...] += shard_queries(flip(s, k + 1), depth)
            else:
                queries[...] += chip_queries(flip(chip, k // 2))
        q = queries[...]
        qsq[0] = column_to_row(jnp.sum(q * q, axis=1, keepdims=True))
        for k in range(1, n_head):
            push(qsq.at[0], qsq.at[k], S_QSQ, one_r.at[R_QSQ], to_head(k))

    with jax.named_scope("spread_late"):
        arrived(spread.at[pl.ds(0, n_chip)], one_r.at[R_SPL])
        own_ow = load(spread.at[own_cols(z)], ow_slot_z(z), 3)
        for k in range(1, n_head):
            if ratio > 1:
                for j in range(0, ratio, 2):
                    hand_over(k, j + 1 - core)
            else:
                hand_over(k, 0)

    @pl.when(core == 1)
    def _():
        with jax.named_scope("kv_in"):
            for ref, chips in ((kall, R_K), (vall, R_V)):
                arrived(ref.at[pl.ds(0, n_seq - 2)], one_r.at[chips])
                for k in masks:
                    here = chip_slot(ref, flip(chip, k // 2))
                    push(here, here, S_KV, one_r.at[chips + 1], to_seq(1))

    @pl.when(core == 0)
    def _():
        with jax.named_scope("kv_end"):
            for ref, chips in ((kall, R_K), (vall, R_V)):
                arrived(ref, one_r.at[chips + 1])

    with jax.named_scope("q_norm"):
        arrived(qsq.at[pl.ds(1, n_head - 1)], one_r.at[R_QSQ])
        q_mean = row_to_column(jnp.sum(qsq[...], axis=0), tok) / (att * n_head)
        q_root = jnp.sqrt(q_mean + 1e-06)

    def held(way, d):
        return d % n_head if way > 0 else (n_head - d) % n_head

    def onward(way, d):
        origin = z - way * (d - 1)
        return (origin >= 0) & (origin < n_head) & (z + way >= 0) & (z + way < n_head)

    def passed(way, d):
        return pass_s.at[0 if way > 0 else 1, d - 1]

    def reach(way, c, d):
        slot = held(way, d)

        @pl.when(onward(way, d))
        def _():
            remote(
                attg.at[held(way, d - 1), cuts[c]], attg.at[slot, cuts[c]],
                passed(way, d), at_r.at[c, slot - 1], (s, z + way),
            ).start()

    def take(way, c, d):
        slot = held(way, d)
        origin = z - way * d

        @pl.when((origin >= 0) & (origin < n_head))
        def _():
            arrived(attg.at[slot, cuts[c]], at_r.at[c, slot - 1])

    def ow_relays(pairs):
        for half, b in pairs:
            gather_relay(ow_half, half, b, S_OG, og_r, oc_r)

    def ow_begin():
        with jax.named_scope("ow_start"):
            own_ow.wait()
            arrived(owg.at[:, pl.ds(0, n_head - 1), ow_piece(s), :], one_r.at[R_OZ])
            for half, b in first + second:
                gather_own(ow_half, half, [b], S_OG, og_r)
            gather_core(ow_half, S_OG, oc_r)

    all_text = n_seq * text
    with jax.named_scope("attend"):
        every_k = kall[...].reshape(all_text, att)
        every_v = vall[...].reshape(all_text, att)
        seen = lax.broadcasted_iota(jnp.int32, (1, all_text), 1) < valid[...]
        for c in range(chunks):
            at = cuts[c]
            q_normed = (queries[at, :] / q_root[at] * qg[...]).astype(BF16)
            for h in range(att // HD):
                lanes = slice(h * HD, (h + 1) * HD)
                scores = lax.dot_general(
                    q_normed[:, lanes], every_k[:, lanes], (((1,), (1,)), ((), ())),
                    preferred_element_type=F32,
                ) * HD ** (-0.5)
                scores = jnp.where(seen, scores, F32(-1e30))
                shifted = jnp.exp(scores - jnp.max(scores, axis=-1, keepdims=True))
                weights = (shifted * (1.0 / jnp.sum(shifted, axis=-1, keepdims=True))).astype(BF16)
                attg[0, at, lanes] = jnp.dot(
                    weights, every_v[:, lanes], preferred_element_type=F32
                ).astype(BF16)
            for way in (1, -1):
                reach(way, c, 1)
            if c < 2:
                pl.when(core == c)(ow_begin)

    cols = owg.shape[3]
    part_width = mod_out.shape[1]
    last = z + 1 - (2 * z) // n_head

    def projection(at, j, slot):
        return jnp.dot(
            attg[slot, at], owg[j, lax.rem(z + n_head - slot, n_head)], preferred_element_type=F32
        )

    def accumulate(begin, end):
        at = slice(cuts[begin].start, cuts[end - 1].stop)
        with jax.named_scope(f"accumulate{begin}"):
            for j in range(ratio):
                here = slice(j * cols, (j + 1) * cols)
                if vpart is None:
                    base = vid[at, pl.ds(pl.multiple_of(z * part_width + j * cols, LANES), cols)]
                else:
                    base = vpart[at, here]
                projected = projection(at, j, 0)
                for i in range(1, n_head - 1):
                    projected = projected + projection(at, j, lax.rem(last - 1 + i, n_head - 1) + 1)
                acc[at, here] = base.astype(F32) + projected

    for d in range(1, n_head - 1):
        for c in range(chunks):
            with jax.named_scope(f"pass{d}_{c}"):
                for way in (1, -1):
                    take(way, c, d)
                    reach(way, c, d + 1)
            if d == 1 and c == 1:
                with jax.named_scope("ow1"):
                    ow_relays(first)
            if d == 1 and c == chunks - 1:
                with jax.named_scope("ow2"):
                    ow_relays(second)
            if d == n_head - 2 and c == 1:
                with jax.named_scope("ow3"):
                    for k in far:
                        for half in range(2):
                            gather_relay(ow_half, half, k, S_OG, og_r, oc_r)
            if d == n_head - 2 and c == 2:
                with jax.named_scope("ow4"):
                    for k in [0] + masks:
                        arrived(ow_slot(flip(s, k + 1)), oc_r.at[k // 2])
                accumulate(0, 3)
    accumulate(3, chunks)
    with jax.named_scope("left1"):
        few = pl.ds(0, n_chip - 1)
        left(ctxg.at[few], send_sem.at[S_CTX])
        left(kvw.at[0], send_sem.at[S_W])
        left(spread.at[pl.ds(0, n_seq - 1)], send_sem.at[S_SP])
        left(shard_rows(0, n_seq - 1), send_sem.at[S_QW])
        left(qsq.at[pl.ds(0, n_head - 1)], send_sem.at[S_QSQ])
        left(owg.at[:, pl.ds(0, n_head - 1), ow_piece(0), :], send_sem.at[S_OZ])

        @pl.when(core == 0)
        def _():
            left(ckr.at[pl.ds(0, n_chip)], send_sem.at[S_CK])
            left(cvr.at[pl.ds(0, n_chip)], send_sem.at[S_CV])

        @pl.when(core == 1)
        def _():
            left(ckr.at[few], send_sem.at[S_CK])
            left(cvr.at[few], send_sem.at[S_CV])
            left(ksq.at[pl.ds(0, n_head - 1)], send_sem.at[S_KSQ])
            left(qwg.at[pl.ds(0, 4 * (n_seq - 1) * text)], send_sem.at[S_KV])

    def modulate(c):
        at = cuts[c]
        step = at.stop - at.start
        with jax.named_scope(f"stat{c}"):
            arrived(stat.at[c, pl.ds(1, n_head - 1)], st_r.at[c])
        with jax.named_scope(f"modulate{c}"):
            wide_row = -(-2 * step // LANES) * LANES
            both = jnp.sum(stat[c, :, :, :wide_row], axis=0) / (part_width * n_head)
            both_col = row_to_column(both, 2 * step)
            mean_col = both_col[:step]
            inv_col = 1.0 / jnp.sqrt(both_col[step:] - mean_col * mean_col + 1e-06)
            wide = resid_out[at, :].astype(F32)
            mod_out[at, :] = (
                (wide - mean_col) * inv_col * (1.0 + shsc[1, :1, :]) + shsc[0, :1, :]
            ).astype(BF16)

    for c in range(chunks):
        at = cuts[c]
        step = at.stop - at.start
        with jax.named_scope(f"last{c}"):
            for way in (1, -1):
                take(way, c, n_head - 1)
        with jax.named_scope(f"project{c}"):
            row_sum = jnp.zeros((step, 1), F32)
            row_sq = jnp.zeros((step, 1), F32)
            for j in range(ratio):
                here = slice(j * cols, (j + 1) * cols)
                rounded = (acc[at, here] + projection(at, j, last)).astype(BF16)
                resid_out[at, here] = rounded
                wide = rounded.astype(F32)
                row_sum = row_sum + jnp.sum(wide, axis=1, keepdims=True)
                row_sq = row_sq + jnp.sum(wide * wide, axis=1, keepdims=True)
            moments = column_to_row(jnp.concatenate([row_sum, row_sq], axis=0))
            stat[c, 0, :, : moments.shape[1]] = moments
            for k in range(1, n_head):
                push(stat.at[c, 0], stat.at[c, k], S_ST, st_r.at[c], to_head(k))
    with jax.named_scope("left2"):
        left(owg.at[:, :, pl.ds(0, piece * (n_seq - 1)), :], send_sem.at[S_OG])
        for way in (1, -1):
            for d in range(1, n_head):
                @pl.when(onward(way, d))
                def _():
                    left(attg.at[0], passed(way, d))
    for c in range(chunks):
        modulate(c)
    left(stat.at[:, pl.ds(0, n_head - 1)], send_sem.at[S_ST])


def put_out(resid, mod, resid_hbm, mod_hbm, sems):
    pieces = sems.shape[1]
    rows = resid.shape[0] // pieces
    copies = [
        pltpu.make_async_copy(src.at[at], dst.at[at], sems.at[i, p])
        for p, at in enumerate(pl.ds(p * rows, rows) for p in range(pieces))
        for i, (src, dst) in enumerate(((resid, resid_hbm), (mod, mod_hbm)))
    ]
    for copy in copies:
        copy.start()
    for copy in copies:
        copy.wait()


def on_device(
    n_seq,
    n_head,
    video_rows,
    context,
    valid_length,
    timestep,
    query_weight,
    key_weight,
    value_weight,
    out_weight,
    query_gain,
    key_gain,
    time_weight,
    modulation,
):
    tok, width = video_rows.shape
    text = context.shape[0]
    depth, att = query_weight.shape
    cols = out_weight.shape[1]
    part_width = modulation.shape[1]
    ratio = n_seq // n_head
    n_chip = n_seq // 2
    quarter = tok // 4
    sizes = [quarter // 2] + [quarter] * 3 + [quarter // 2]
    cuts = [slice(sum(sizes[:c]), sum(sizes[: c + 1])) for c in range(len(sizes))]
    chunks = len(cuts)
    piece = out_weight.shape[0] // n_seq
    half = FREQ // 2
    freqs = np.exp(-np.log(10000.0) * np.arange(half) / half).astype(np.float32)[None, :]
    sliced = part_width % LANES != 0 or cols % LANES != 0
    extra = []
    if sliced:
        extra.append(
            lax.dynamic_slice_in_dim(
                video_rows, lax.axis_index("head") * part_width, part_width, 1
            )
        )
    out_bytes = tok * -(-part_width // LANES) * LANES * 2
    vmem = pl.BlockSpec(memory_space=pltpu.VMEM)
    hbm = pl.BlockSpec(memory_space=pltpu.HBM)
    dma = pltpu.SemaphoreType.DMA
    results = pl.pallas_call(
        functools.partial(body, n_seq, n_head, cuts, sliced),
        out_shape=[pltpu.VMEM((tok, part_width), BF16)] * 2,
        in_specs=[hbm] * 13 + [vmem] * len(extra),
        out_specs=[vmem] * 2,
        scratch_shapes=[
            pltpu.VMEM((tok, width), BF16),
            pltpu.VMEM((tok, width), BF16),
            pltpu.VMEM((text, width), BF16),
            pltpu.VMEM((n_chip, text, 2 * depth), BF16),
            pltpu.VMEM((n_seq * depth, att), BF16),
            pltpu.VMEM((2, depth, 2 * att), BF16),
            pltpu.VMEM((n_chip, text, att), F32),
            pltpu.VMEM((n_seq, text, att), F32),
            pltpu.VMEM((n_chip, text, att), BF16),
            pltpu.VMEM((n_seq, text, att), BF16),
            pltpu.VMEM((text, att), F32),
            pltpu.VMEM((2 * text, att), F32),
            pltpu.VMEM((n_seq, text, att), BF16),
            pltpu.VMEM((n_seq, text, att), BF16),
            pltpu.VMEM((n_seq, piece, cols), BF16),
            pltpu.VMEM((ratio, n_head, out_weight.shape[0], cols), BF16),
            pltpu.VMEM((n_head, tok, att), BF16),
            pltpu.VMEM((tok, att), F32),
            pltpu.VMEM((n_head, 1, tok), F32),
            pltpu.VMEM((n_head, 1, -(-2 * text // LANES) * LANES), F32),
            pltpu.VMEM((chunks, n_head, 1, -(-2 * max(sizes) // LANES) * LANES), F32),
            pltpu.VMEM((2, 8, part_width), F32),
            pltpu.VMEM(time_weight.shape, BF16),
            pltpu.VMEM((1, att), F32),
            pltpu.VMEM((1, att), F32),
            pltpu.VMEM((1, half), F32),
            pltpu.VMEM(modulation.shape, F32),
            pltpu.VMEM((tok, part_width), F32),
            pltpu.VMEM((1, 1), jnp.int32),
            pltpu.VMEM((1, 1), jnp.int32),
            dma((13,)),
            dma((12,)),
            dma((2, n_head - 1)),
            *[dma((n_chip - 1,))] * 2,
            *[dma((2, n_chip - 1)), dma((n_chip,))] * 2,
            dma((chunks, n_head - 1)),
            dma((chunks,)),
            dma((12,)),
        ],
        compiler_params=pltpu.CompilerParams(
            collective_id=0, has_side_effects=True, vmem_limit_bytes=VMEM_MOST - 2 * out_bytes
        ),
    )(
        valid_length[None, :],
        timestep[None, :],
        video_rows,
        context,
        query_weight,
        key_weight,
        value_weight,
        out_weight,
        query_gain[None, :],
        key_gain[None, :],
        freqs,
        time_weight,
        modulation,
        *extra,
    )
    return pl.pallas_call(
        put_out,
        out_shape=[jax.ShapeDtypeStruct((tok, part_width), BF16)] * 2,
        in_specs=[vmem] * 2,
        out_specs=[hbm] * 2,
        scratch_shapes=[dma((2, 4))],
        compiler_params=pltpu.CompilerParams(vmem_limit_bytes=4 * 1024 * 1024),
    )(*results)


def solution(mesh):
    in_specs = (
        P("seq", None),
        P("seq", None),
        P(),
        P(),
        P("seq", "head"),
        P("seq", "head"),
        P("seq", "head"),
        P("head", "seq"),
        P("head"),
        P("head"),
        P(None, None, "head"),
        P(None, "head"),
    )
    out_specs = (P("seq", "head"), P("seq", "head"))
    return jax.shard_map(
        functools.partial(on_device, mesh.shape["seq"], mesh.shape["head"]),
        mesh=mesh, in_specs=in_specs, out_specs=out_specs, check_vma=False,
    )
```
